32 devices in a mesh: facet: 8 (over z, y), freq: 4 (over x, core).
Axes of the slice: x: 2, y: 2, z: 4, core: 2. Of those that a mesh axis runs over, the one named last changes fastest.
Arguments:
- visibilities: bfloat16 [4, 2048, 2, 512], P('freq', 'facet'), may hold values from -6 to 6
- uvw: bfloat16 [4, 2048, 3, 512], P('freq', 'facet'), may hold values from -4 to 4
- facet_of: int32 [4, 2048, 1], P('freq', 'facet'), may hold values from 0 to 7; in each aligned block of 256 rows (0 to 255, 256 to 511, ..., all dimensions but the last counted through in order) at most 128 rows name the same one
- plane_of: int32 [4, 2048], P('freq', 'facet'), may hold values from 0 to 7
- cell_of: int32 [4, 2048], P('freq', 'facet'), may hold values from 0 to 1023
- kernels: bfloat16 [8, 2, 512, 256], replicated, may hold values from -0.25 to 0.25
- centers: float32 [8, 2], replicated, may hold values from -0.4 to 0.4
Outputs:
- images: float32 [8, 512, 512], P('facet', None, 'freq')
The draws below stay inside these ranges and needn't reach their ends.
Inputs may be any that keep to these rules, and one draw needn't show every extreme that they name: `facet_of`: the facet index k is held by index k of the facet axis. In each aligned block of 256 tiles of one group, no facet is named by more than 128 tiles, and in some blocks one facet is named by exactly 128.
All inputs are finite; a program needn't handle non-finite values.
Results may differ from the reference program's by a relative error of at most 0.0095.
Values may be sent and summed in bfloat16 or wider, within the bound.
No kernel may reach another device: no remote copies, remote signals or barrier semaphores. Data moves between devices by JAX's collectives and lax.ppermute only.
A program may use at most 128 MiB of HBM per device.

```python
import math
import jax
import jax.numpy as jnp
import numpy as np
from jax import lax

GRID = 512
PSIDE = 16
ROWS = 512
PLANES = 8
TILES_DEV = 256
GROUPS = 4
FACETS = 8
TILES = 2048
CAP = 128
PATCH = 256
CELLS = 1024


def plant(values, own_key, smallest, high):
    longest = values.shape.index(max(values.shape))
    spots = []
    for shift in (0, 1):
        where = [jax.random.randint(jax.random.fold_in(own_key, axis), (), 0, length) for axis, length in enumerate(values.shape)]
        where[longest] = (where[longest] + shift) % values.shape[longest]
        spots.append(tuple(where))
    return values.at[spots[0]].set(smallest).at[spots[1]].set(high)


def block_scale(own_key, shape, split, smallest, top_value):
    loudness, own = 1.0, jax.random.fold_in(own_key, 6)
    for position, shards_of in split:
        heights = jnp.exp(jax.random.uniform(jax.random.fold_in(own, position), (shards_of,), jnp.float32, smallest / len(split), top_value / len(split)))
        loudness = loudness * jnp.repeat(heights, shape[position] // shards_of).reshape([-1 if axis == position else 1 for axis in range(len(shape))])
    return loudness


def shared_out(stream_key, own, number, rows, amount, top, bound, lean):
    ranking = jax.random.permutation(stream_key, amount)
    packed, ordinary = shares(amount, rows * top, bound, lean, True), shares(amount, rows * top, bound, lean, False)
    places = jnp.arange(amount)

    def named(lengths, turn):
        used = int((lengths > 0).sum())
        fixed = max(1, used // 4)
        passed = fixed + (places - fixed + turn * (used - fixed)) % max(1, amount - fixed)
        return jnp.zeros((amount,), jnp.int32).at[ranking[jnp.where(places < fixed, places, passed)]].set(jnp.asarray(lengths, jnp.int32))

    lengths = jnp.where(number % 4 == 0, named(packed, number // 4), named(ordinary, number - number // 4 - 1))
    mixed = jax.random.permutation(jax.random.fold_in(own, 3), amount)
    giver, receiver = mixed[0:amount // 2 * 2:2], mixed[1:amount // 2 * 2:2]
    room = jnp.minimum(lengths[giver] - 1, bound - lengths[receiver]) // 2
    room = jnp.where((giver == ranking[0]) | (receiver == ranking[0]) | (lengths[receiver] == 0), 0, jnp.maximum(room, 0))
    passed = jax.random.randint(jax.random.fold_in(own, 4), (amount // 2,), 0, 1 << 20) % (room + 1)
    lengths = lengths.at[giver].add(-passed).at[receiver].add(passed)
    members = jnp.searchsorted(jnp.cumsum(lengths), jnp.arange(rows * top), side="right").astype(jnp.int32)
    listing = members.reshape(top, rows).T
    listing = listing[jax.random.permutation(jax.random.fold_in(own, 1), rows)]
    turn = jax.random.randint(jax.random.fold_in(own, 2), (rows, 1), 0, top)
    return jnp.take_along_axis(listing, (jnp.arange(top)[None, :] + turn) % top, axis=1)


def shares(count, total, most, skew, full):
    weights = [(1 << 20) // math.isqrt(standing ** skew) + 1 for standing in range(1, count + 1)]
    largest = most if full else min(most, max(-(-total // count), total * weights[0] // sum(weights)))
    least = 1 if total - largest >= count - 1 else 0
    holding, surplus = [largest] + [least] * (count - 1), total - largest - least * (count - 1)
    while surplus > 0:
        free = [i for i in range(1, count) if holding[i] < largest] or [i for i in range(1, count) if holding[i] < most]
        pool, budget = sum([weights[i] for i in free]), surplus
        for i in free:
            more = min(most - holding[i], max(1, budget * weights[i] // pool), surplus)
            holding[i] = holding[i] + more
            surplus = surplus - more
    return np.array(holding)


def scatter_about(key, extent, spread, bound, cuts=(), kind=jnp.bfloat16):
    array = jax.random.normal(key, extent, jnp.float32) * spread
    if len(cuts) > 0:
        array = block_scale(key, extent, cuts, -0.22, 0.18) * array
    return jnp.clip(array, min=-bound, max=bound).astype(kind)


def setup_inputs(seed: int = 0) -> dict:
    seeds = jax.random.split(jax.random.key(seed), 8)
    visibilities = scatter_about(seeds[0], (GROUPS, TILES, 2, ROWS), 1.0, 6.0, ((0, 4), (1, 8)))
    uvw = jnp.clip(jax.random.uniform(seeds[1], (GROUPS, TILES, 3, ROWS), jnp.float32, -4.0, 4.0) * block_scale(seeds[1], (GROUPS, TILES, 3, ROWS), ((0, 4), (1, 8)), -0.4, 0.0), -4.0, 4.0).astype(jnp.bfloat16)
    facet_of_keys = jax.random.split(jax.random.fold_in(seeds[2], 1), GROUPS * TILES // TILES_DEV)
    facet_of_turns = jax.random.permutation(jax.random.fold_in(seeds[2], 3), GROUPS * TILES // TILES_DEV)
    facet_of = jax.vmap(lambda own, number: shared_out(jax.random.fold_in(seeds[2], 2), own, number, TILES_DEV, FACETS, 1, CAP, 2))(facet_of_keys, facet_of_turns).reshape((GROUPS, TILES, 1))
    plane_of = plant(jax.random.randint(seeds[3], (GROUPS, TILES), 0, PLANES), jax.random.fold_in(seeds[3], 1), 0, PLANES - 1).astype(jnp.int32)
    cell_of = plant(jax.random.randint(seeds[4], (GROUPS, TILES), 0, CELLS), jax.random.fold_in(seeds[4], 1), 0, CELLS - 1).astype(jnp.int32)
    kernels = scatter_about(seeds[5], (PLANES, 2, ROWS, PATCH), ROWS ** -0.5, 0.25)
    centers = jnp.clip(jax.random.uniform(seeds[6], (FACETS, 2), jnp.float32, -0.4, 0.4), -0.4, 0.4)
    return {"visibilities": visibilities, "uvw": uvw, "facet_of": facet_of, "plane_of": plane_of, "cell_of": cell_of, "kernels": kernels, "centers": centers}


def dft_tables(length):
    indices = jnp.arange(length, dtype=jnp.int32)
    products_mod = indices[:, None] * indices[None, :] % length
    angle_table = products_mod.astype(jnp.float32) * (2.0 * jnp.pi / length)
    norm_scale = 1.0 / jnp.sqrt(jnp.float32(length))
    table_real = (jnp.cos(angle_table) * norm_scale).astype(jnp.bfloat16)
    table_imag = (jnp.sin(angle_table) * norm_scale).astype(jnp.bfloat16)
    return (table_real, table_imag)

def rotate_tiles(vis_pair, coords, sky_pos):
    l_coord = sky_pos[:, 0:1]
    m_coord = sky_pos[:, 1:2]
    w_term = jnp.sqrt(1.0 - l_coord * l_coord - m_coord * m_coord) - 1.0
    coords = coords.astype(jnp.float32)
    phase_angle = 2.0 * jnp.pi * (l_coord * coords[:, 0] + m_coord * coords[:, 1] + w_term * coords[:, 2])
    cosine = jnp.cos(phase_angle)
    sine_part = jnp.sin(phase_angle)
    real_part = vis_pair[:, 0].astype(jnp.float32)
    imag_part = vis_pair[:, 1].astype(jnp.float32)
    rot_real = (real_part * cosine + imag_part * sine_part).astype(jnp.bfloat16)
    rot_imag = (imag_part * cosine - real_part * sine_part).astype(jnp.bfloat16)
    return (rot_real, rot_imag)

def reference(visibilities, uvw, facet_of, plane_of, cell_of, kernels, centers):
    facet_count = centers.shape[0]
    row_count = visibilities.shape[3]
    nblocks = GRID // PSIDE
    ncells = nblocks * nblocks
    tile_block = 64
    table_real, table_imag = dft_tables(GRID)
    table_both = jnp.concatenate([table_real, table_imag], axis=1).astype(jnp.float32)
    kern_full = kernels.astype(jnp.float32)
    summed = jnp.zeros((facet_count, 2, GRID, GRID), jnp.float32)
    for group in range(visibilities.shape[0]):
        target = facet_of[group, :, 0]
        sky_rows = centers[target]
        rot_real, rot_imag = rotate_tiles(visibilities[group], uvw[group], sky_rows)

        def grid_block(pieces):
            block_real, block_imag, block_planes = pieces
            chosen = kern_full[block_planes]
            left_real = block_real.astype(jnp.float32)
            left_imag = block_imag.astype(jnp.float32)
            patch_real = jnp.einsum('tr,trq->tq', left_real, chosen[:, 0]) - jnp.einsum('tr,trq->tq', left_imag, chosen[:, 1])
            patch_imag = jnp.einsum('tr,trq->tq', left_real, chosen[:, 1]) + jnp.einsum('tr,trq->tq', left_imag, chosen[:, 0])
            return jnp.concatenate([patch_real, patch_imag], axis=1).astype(jnp.bfloat16)
        patches = lax.map(grid_block, (rot_real.reshape(-1, tile_block, row_count), rot_imag.reshape(-1, tile_block, row_count), plane_of[group].reshape(-1, tile_block)))
        patches = patches.reshape(-1, 2 * PSIDE * PSIDE)
        keys = (target * ncells + cell_of[group]).astype(jnp.int32)
        blocks = jax.ops.segment_sum(patches.astype(jnp.float32), keys, num_segments=facet_count * ncells).astype(jnp.bfloat16)
        grids = blocks.reshape(facet_count, nblocks, nblocks, 2, PSIDE, PSIDE)
        grids = grids.transpose(0, 3, 1, 4, 2, 5).reshape(facet_count, 2 * GRID, GRID)

        def half_transform(one_grid):
            product = jnp.dot(one_grid.astype(jnp.float32), table_both)
            half_real = product[:GRID, :GRID] - product[GRID:, GRID:]
            half_imag = product[:GRID, GRID:] + product[GRID:, :GRID]
            return jnp.stack([half_real, half_imag]).astype(jnp.bfloat16)
        partial_value = lax.map(half_transform, grids)
        partial_value = lax.optimization_barrier(partial_value)
        summed = summed + partial_value.astype(jnp.float32)
    halves = lax.optimization_barrier(summed.astype(jnp.bfloat16))

    def finish(one_half):
        right_side = jnp.concatenate([one_half[0], -one_half[1]], axis=0).astype(jnp.float32)
        return jnp.dot(table_both, right_side)
    return lax.map(finish, halves)
```

```python
import functools

import jax
import jax.numpy as jnp
import numpy as np
from jax import lax
from jax.experimental import pallas as pl
from jax.experimental.pallas import tpu as pltpu
from jax.sharding import PartitionSpec as P

GRID = 512
PSIDE = 16
NBLK = GRID // PSIDE
LANES = 128
SUBLANES = 8

SIN_POLY = (6.283185280261414, -41.34168066806301, 81.602480742862, -76.58128455932604, 39.76072207590882)
COS_POLY = (
    0.999999999779904,
    -19.739208548314995,
    64.93934655286789,
    -85.45356819388616,
    60.14395231405798,
    -24.98183599569851,
)


def horner(square, coefficients):
    value = jnp.full_like(square, coefficients[-1])
    for coefficient in coefficients[-2::-1]:
        value = value * square + coefficient
    return value


def cos_sin_turns(turns):
    halves = jnp.round(turns * 2.0)
    rest = turns - halves * 0.5
    half = halves * 0.5
    sign = 1.0 - 4.0 * (half - jnp.floor(half))
    square = rest * rest
    return (horner(square, COS_POLY) * sign, rest * horner(square, SIN_POLY) * sign)


def compiler_params(mebibytes):
    return pltpu.CompilerParams(vmem_limit_bytes=mebibytes << 20)


VMEM = pl.BlockSpec(memory_space=pltpu.VMEM)
SMEM = pl.BlockSpec(memory_space=pltpu.SMEM)
ANY = pl.BlockSpec(memory_space=pl.ANY)


def dft_tables(length):
    indices = jnp.arange(length, dtype=jnp.int32)
    products_mod = indices[:, None] * indices[None, :] % length
    angle_table = products_mod.astype(jnp.float32) * (2.0 * jnp.pi / length)
    norm_scale = 1.0 / jnp.sqrt(jnp.float32(length))
    table_real = (jnp.cos(angle_table) * norm_scale).astype(jnp.bfloat16)
    table_imag = (jnp.sin(angle_table) * norm_scale).astype(jnp.bfloat16)
    return (table_real, table_imag)


def rotate_tiles(vis_pair, coords, sky_pos):
    l_coord = sky_pos[:, 0:1]
    m_coord = sky_pos[:, 1:2]
    w_term = jnp.sqrt(1.0 - l_coord * l_coord - m_coord * m_coord) - 1.0
    coords = coords.astype(jnp.float32)
    phase_angle = (
        2.0 * jnp.pi * (l_coord * coords[:, 0] + m_coord * coords[:, 1] + w_term * coords[:, 2])
    )
    cosine = jnp.cos(phase_angle)
    sine_part = jnp.sin(phase_angle)
    real_part = vis_pair[:, 0].astype(jnp.float32)
    imag_part = vis_pair[:, 1].astype(jnp.float32)
    rot_real = (real_part * cosine + imag_part * sine_part).astype(jnp.bfloat16)
    rot_imag = (imag_part * cosine - real_part * sine_part).astype(jnp.bfloat16)
    return (rot_real, rot_imag)


def stack_kernels(kernels):
    kern_real = kernels[:, 0]
    kern_imag = kernels[:, 1]
    upper_rows = jnp.concatenate([kern_real, kern_imag], axis=2)
    lower_rows = jnp.concatenate([-kern_imag, kern_real], axis=2)
    stacked_rows = jnp.concatenate([upper_rows, lower_rows], axis=0)
    return stacked_rows.reshape(-1, stacked_rows.shape[2])


def grid_tiles(rot_real, rot_imag, planes, stacked, plane_count):
    plane_select = (planes[:, None] == jnp.arange(plane_count)[None, :]).astype(jnp.bfloat16)
    spread = jnp.concatenate(
        [
            rot_real[:, None, :] * plane_select[:, :, None],
            rot_imag[:, None, :] * plane_select[:, :, None],
        ],
        axis=1,
    )
    spread = spread.reshape(spread.shape[0], -1)
    return jnp.dot(spread, stacked, preferred_element_type=jnp.float32).astype(jnp.bfloat16)


def shards(visibilities, uvw, facet_of, plane_of, cell_of, kernels, centers):
    peer_count = lax.axis_size("facet")
    tile_count = visibilities.shape[1]
    capacity = 4 * tile_count // peer_count
    total_slots = peer_count * capacity
    vis_pair = visibilities[0]
    coords = uvw[0]
    target = facet_of[0, :, 0]
    planes = plane_of[0]
    tile_cells = cell_of[0]
    plane_count = kernels.shape[0]
    stacked = stack_kernels(kernels)
    dest_hits = (target[:, None] == jnp.arange(peer_count)[None, :]).astype(jnp.int32)
    before = jnp.cumsum(dest_hits, axis=0) - dest_hits
    within_rank = jnp.sum(before * dest_hits, axis=1)
    slot_index = target * capacity + within_rank
    chosen = (target[:, None] == jnp.arange(centers.shape[0])[None, :]).astype(jnp.float32)
    sky_rows = jnp.sum(chosen[:, :, None] * centers[None, :, :], axis=1)
    rot_real, rot_imag = rotate_tiles(vis_pair, coords, sky_rows)
    own_patches = grid_tiles(rot_real, rot_imag, planes, stacked, plane_count)
    patch_buffer = (
        jnp.zeros((total_slots, own_patches.shape[1]), jnp.bfloat16).at[slot_index].set(own_patches)
    )
    cell_buffer = jnp.zeros((total_slots,), jnp.int32).at[slot_index].set(tile_cells)
    patches, slot_cells = (
        lax.all_to_all(
            patch_buffer.reshape(peer_count, capacity, -1),
            "facet",
            split_axis=0,
            concat_axis=0,
            tiled=True,
        ),
        lax.all_to_all(
            cell_buffer.reshape(peer_count, capacity),
            "facet",
            split_axis=0,
            concat_axis=0,
            tiled=True,
        ),
    )
    patches = patches.reshape(-1, patches.shape[-1])
    slot_cells = slot_cells.reshape(-1)
    nblocks = GRID // PSIDE
    ncells = nblocks * nblocks
    placing = (slot_cells[None, :] == jnp.arange(ncells)[:, None]).astype(jnp.bfloat16)
    blocks = jnp.dot(placing, patches, preferred_element_type=jnp.float32).astype(jnp.bfloat16)
    uv_grid = (
        blocks.reshape(nblocks, nblocks, 2, PSIDE, PSIDE)
        .transpose(2, 0, 3, 1, 4)
        .reshape(2 * GRID, GRID)
    )
    table_real, table_imag = dft_tables(GRID)
    table_both = jnp.concatenate([table_real, table_imag], axis=1)
    product = jnp.dot(uv_grid, table_both, preferred_element_type=jnp.float32)
    half_real = product[:GRID, :GRID] - product[GRID:, GRID:]
    half_imag = product[:GRID, GRID:] + product[GRID:, :GRID]
    partial_value = jnp.stack([half_real, half_imag]).astype(jnp.bfloat16)
    summed = lax.psum_scatter(
        partial_value.astype(jnp.float32).astype(jnp.bfloat16),
        "freq",
        scatter_dimension=2,
        tiled=True,
    )
    right_side = jnp.concatenate([summed[0], -summed[1]], axis=0)
    facet_image = jnp.dot(table_both, right_side, preferred_element_type=jnp.float32)
    return facet_image[None]


def gather_kernel(peers, capacity, me_ref, centers_ref, facet_ref, plane_ref, cell_ref, vis_ref, uvw_ref, kern_ref, *rest):
    out_refs, (kern_buf, rows_buf, kern_sem) = rest[:peers], rest[peers:]
    planes, _, depth, cells = kern_ref.shape
    tiles = facet_ref.shape[1]
    copies = [pltpu.make_async_copy(kern_ref.at[p], kern_buf.at[p], kern_sem.at[p]) for p in range(planes)]
    for copy in copies:
        copy.start()
    facet = facet_ref[...]
    l_row = jnp.zeros(facet.shape, jnp.float32)
    m_row = jnp.zeros(facet.shape, jnp.float32)
    for f in range(peers):
        hit = facet == f
        l_row = jnp.where(hit, centers_ref[f, 0], l_row)
        m_row = jnp.where(hit, centers_ref[f, 1], m_row)
    d_row = jnp.sqrt(1.0 - l_row * l_row - m_row * m_row) - 1.0
    plane_row = plane_ref[...].astype(jnp.float32)
    zero_row = jnp.zeros_like(l_row)
    columns = jnp.concatenate([l_row, m_row, d_row, plane_row] + [zero_row] * 4, axis=0).T
    l_col, m_col, d_col, plane_col = (columns[:, i : i + 1] for i in range(4))

    u = uvw_ref[0].astype(jnp.float32)
    v = uvw_ref[1].astype(jnp.float32)
    w = uvw_ref[2].astype(jnp.float32)
    cosine, sine = cos_sin_turns(l_col * u + m_col * v + d_col * w)
    real = vis_ref[:, 0, :].astype(jnp.float32)
    imag = vis_ref[:, 1, :].astype(jnp.float32)
    rot_real = (real * cosine + imag * sine).astype(jnp.bfloat16)
    rot_imag = (imag * cosine - real * sine).astype(jnp.bfloat16)
    rows_buf[:tiles, :depth] = rot_real
    rows_buf[:tiles, depth:] = -rot_imag
    rows_buf[tiles:, :depth] = rot_imag
    rows_buf[tiles:, depth:] = rot_real

    relative = facet ^ me_ref[0]
    lanes = lax.broadcasted_iota(jnp.int32, (tiles, tiles), 1)
    earlier = (lax.broadcasted_iota(jnp.int32, (tiles, tiles), 0) < lanes).astype(jnp.float32).astype(jnp.bfloat16)
    hits = lax.broadcasted_iota(jnp.int32, (peers, tiles), 0) == relative
    before = jnp.dot(hits.astype(jnp.float32).astype(jnp.bfloat16), earlier, preferred_element_type=jnp.float32)
    rank = jnp.sum(jnp.where(hits, before, 0.0), axis=0, keepdims=True)
    slot = relative * capacity + rank.astype(jnp.int32)
    slots = peers * capacity
    placing = lax.broadcasted_iota(jnp.int32, (slots, tiles), 0) == slot
    placing = placing.astype(jnp.float32).astype(jnp.bfloat16)

    total = jnp.zeros((2 * tiles, cells), jnp.float32)
    plane_two = jnp.concatenate([plane_col, plane_col], axis=0)
    for p in range(planes):
        mask = (plane_two == float(p)).astype(jnp.float32).astype(jnp.bfloat16)
        copies[p].wait()
        total = total + jnp.dot(
            rows_buf[...] * mask, kern_buf[p].reshape(2 * depth, cells), preferred_element_type=jnp.float32
        )
    patches = jnp.concatenate([total[:tiles], total[tiles:]], axis=1).astype(jnp.bfloat16)
    placed = jnp.dot(placing, patches, preferred_element_type=jnp.float32).astype(jnp.bfloat16)
    cell = cell_ref[...].astype(jnp.float32)
    block_u = jnp.floor(cell * (1.0 / NBLK))
    block_v = cell - block_u * NBLK
    pair = jnp.concatenate([block_u, block_v] + [zero_row] * (SUBLANES - 2), axis=0).astype(jnp.bfloat16)
    pair = lax.dot_general(pair, placing, (((1,), (1,)), ((), ())), preferred_element_type=jnp.float32)
    pair = pair.astype(jnp.bfloat16)
    for s in range(peers):
        rows = slice(s * capacity, (s + 1) * capacity)
        for j in range(2 * cells // LANES):
            out_refs[s][j * capacity : (j + 1) * capacity, :] = placed[rows, j * LANES : (j + 1) * LANES]
        out_refs[s][2 * cells // LANES * capacity :, :] = pair[:, rows]


def image_kernel(peers, groups, capacity, me_ref, table_ref, *rest):
    in_refs, out_refs = rest[:peers], rest[peers : peers + groups]
    phases_buf, patch_buf, table_buf = rest[peers + groups :]
    cells = PSIDE * PSIDE
    slots = peers * capacity
    share = cells // groups
    half_tiles = cells // LANES
    for s in range(peers):
        rows = slice(s * capacity, (s + 1) * capacity)
        below = slice(slots + s * capacity, slots + (s + 1) * capacity)
        for j in range(half_tiles):
            left = slice(j * LANES, (j + 1) * LANES)
            right = slice(cells + j * LANES, cells + (j + 1) * LANES)
            real = in_refs[s][j * capacity : (j + 1) * capacity, :]
            imag = in_refs[s][(half_tiles + j) * capacity : (half_tiles + j + 1) * capacity, :]
            patch_buf[rows, left] = real
            patch_buf[rows, right] = imag
            patch_buf[below, left] = -imag
            patch_buf[below, right] = real
    for s in range(groups):
        start = pl.multiple_of((me_ref[0] ^ s) * share, share)
        table_buf[s * share : (s + 1) * share, :] = table_ref[pl.ds(start, share), :]

    first = 2 * half_tiles * capacity
    block_u = jnp.concatenate([ref[first : first + SUBLANES, :][0:1].astype(jnp.float32) for ref in in_refs], axis=1)
    block_v = jnp.concatenate([ref[first : first + SUBLANES, :][1:2].astype(jnp.float32) for ref in in_refs], axis=1)
    index = lax.broadcasted_iota(jnp.int32, (NBLK, slots), 0).astype(jnp.float32)
    cos_u, sin_u = cos_sin_turns(index * block_u * (1.0 / NBLK))
    cos_v, sin_v = cos_sin_turns(index * block_v * (1.0 / NBLK))

    lane = lax.broadcasted_iota(jnp.int32, (NBLK, cells), 1)
    row = lax.broadcasted_iota(jnp.int32, (NBLK, cells), 0)
    patch_u, patch_v = lane // PSIDE, lane % PSIDE
    twid_u = cos_sin_turns((row * patch_u).astype(jnp.float32) * (1.0 / GRID))
    twid_v = cos_sin_turns((row * patch_v).astype(jnp.float32) * (1.0 / GRID))

    per_chunk = 8
    for chunk in range(NBLK // per_chunk):
        for i in range(per_chunk):
            j = chunk * per_chunk + i
            cu, su = cos_u[j : j + 1], sin_u[j : j + 1]
            rows = slice(i * NBLK, (i + 1) * NBLK)
            buf = phases_buf.at[chunk % 2]
            buf[rows, :slots] = (cu * cos_v - su * sin_v).astype(jnp.bfloat16)
            buf[rows, slots:] = (cu * sin_v + su * cos_v).astype(jnp.bfloat16)
        spectrum = jnp.dot(phases_buf[chunk % 2], patch_buf[...], preferred_element_type=jnp.float32)
        turned = []
        for i in range(per_chunk):
            j = chunk * per_chunk + i
            rows = slice(i * NBLK, (i + 1) * NBLK)
            real, imag = spectrum[rows, :cells], spectrum[rows, cells:]
            tr = twid_u[0][j : j + 1] * twid_v[0] - twid_u[1][j : j + 1] * twid_v[1]
            ti = twid_u[0][j : j + 1] * twid_v[1] + twid_u[1][j : j + 1] * twid_v[0]
            turned.append(jnp.concatenate([real * tr - imag * ti, real * ti + imag * tr], axis=1).astype(jnp.bfloat16))
        turned = jnp.concatenate(turned, axis=0)
        image = lax.dot_general(
            table_buf[...], turned, (((1,), (1,)), ((), ())), preferred_element_type=jnp.float32
        ).astype(jnp.bfloat16)
        width = per_chunk * NBLK
        for s in range(groups):
            out_refs[s][:, chunk * width : (chunk + 1) * width] = image[s * share : (s + 1) * share]


def finish_kernel(groups, *refs):
    in_refs, out_ref = refs[:groups], refs[groups]
    columns = PSIDE // groups
    per_tile = LANES // NBLK
    lane = lax.broadcasted_iota(jnp.int32, (PSIDE, LANES), 1) // NBLK
    for tile in range(NBLK // per_tile):
        lanes = slice(tile * LANES, (tile + 1) * LANES)
        total = in_refs[0][:, lanes].astype(jnp.float32)
        for ref in in_refs[1:]:
            total = total + ref[:, lanes].astype(jnp.float32)
        for i in range(per_tile):
            value = jnp.zeros((PSIDE, LANES), jnp.float32)
            for kq in range(columns):
                piece = total[kq * PSIDE : (kq + 1) * PSIDE]
                shift = (kq - i) * NBLK % LANES
                piece = pltpu.roll(piece, shift, 1) if shift else piece
                value = jnp.where(lane == kq, piece, value)
            out_ref[pl.ds(tile * per_tile + i, PSIDE, stride=NBLK), :] = value


def patch_table(groups):
    index = np.arange(PSIDE)
    kq, jq = (a.reshape(-1, 1) for a in np.meshgrid(index, index, indexing="ij"))
    pu, pv = (a.reshape(1, -1) for a in np.meshgrid(index, index, indexing="ij"))
    angle = 2.0 * np.pi * ((pu * jq + pv * kq) % PSIDE) / PSIDE
    return np.concatenate([np.cos(angle), -np.sin(angle)], axis=1) / GRID


def swap(piece, axis, distance):
    count = lax.axis_size(axis)
    return lax.ppermute(piece, axis, [(i, i ^ distance) for i in range(count)])


def packed_shards(visibilities, uvw, facet_of, plane_of, cell_of, kernels, centers):
    peers, groups = lax.axis_size("facet"), lax.axis_size("freq")
    tiles = visibilities.shape[1]
    capacity = 4 * tiles // peers
    planes, _, depth, cells = kernels.shape
    payload = jax.ShapeDtypeStruct((2 * cells // LANES * capacity + SUBLANES, LANES), jnp.bfloat16)
    facet_index = lax.axis_index("facet").reshape(1).astype(jnp.int32)
    group_index = lax.axis_index("freq").reshape(1).astype(jnp.int32)
    pieces = pl.pallas_call(
        functools.partial(gather_kernel, peers, capacity),
        out_shape=[payload] * peers,
        in_specs=[SMEM, SMEM, VMEM, VMEM, VMEM, VMEM, VMEM, ANY],
        out_specs=[VMEM] * peers,
        scratch_shapes=[
            pltpu.VMEM(kernels.shape, jnp.bfloat16),
            pltpu.VMEM((2 * tiles, 2 * depth), jnp.bfloat16),
            pltpu.SemaphoreType.DMA((planes,)),
        ],
        compiler_params=compiler_params(40),
        name="gather",
    )(
        facet_index,
        centers,
        facet_of.reshape(1, tiles),
        plane_of,
        cell_of,
        visibilities[0],
        uvw[0].transpose(1, 0, 2),
        kernels,
    )
    received = [pieces[0]] + [swap(pieces[s], "facet", s) for s in range(1, peers)]
    share = cells // groups
    image = jax.ShapeDtypeStruct((share, NBLK * NBLK), jnp.bfloat16)
    slots = peers * capacity
    images = pl.pallas_call(
        functools.partial(image_kernel, peers, groups, capacity),
        out_shape=[image] * groups,
        in_specs=[SMEM] + [VMEM] * (1 + peers),
        out_specs=[VMEM] * groups,
        scratch_shapes=[
            pltpu.VMEM((2, 8 * NBLK, 2 * slots), jnp.bfloat16),
            pltpu.VMEM((2 * slots, 2 * cells), jnp.bfloat16),
            pltpu.VMEM((cells, 2 * cells), jnp.bfloat16),
        ],
        compiler_params=compiler_params(40),
        name="image",
    )(group_index, jnp.asarray(patch_table(groups), jnp.bfloat16), *received)
    summed = [images[0]] + [swap(images[s], "freq", s) for s in range(1, groups)]
    facet_image = pl.pallas_call(
        functools.partial(finish_kernel, groups),
        out_shape=jax.ShapeDtypeStruct((GRID, GRID // groups), jnp.float32),
        in_specs=[VMEM] * groups,
        out_specs=VMEM,
        compiler_params=compiler_params(16),
        name="finish",
    )(*summed)
    return facet_image[None]


def solution(mesh):
    in_specs = (
        P("freq", "facet", None, None),
        P("freq", "facet", None, None),
        P("freq", "facet", None),
        P("freq", "facet"),
        P("freq", "facet"),
        P(),
        P(),
    )
    out_specs = P("facet", None, "freq")

    def body(*args):
        peers, groups = lax.axis_size("facet"), lax.axis_size("freq")
        capacity = 4 * args[0].shape[1] // peers
        powers = peers & (peers - 1) == 0 and groups & (groups - 1) == 0
        packed = capacity % LANES == 0 and powers and GRID // groups == LANES
        return (packed_shards if packed else shards)(*args)

    return jax.shard_map(body, mesh=mesh, in_specs=in_specs, out_specs=out_specs, check_vma=False)
```

```python
import functools

import jax
import jax.numpy as jnp
import numpy as np
from jax import lax
from jax.experimental import pallas as pl
from jax.experimental.pallas import tpu as pltpu
from jax.sharding import PartitionSpec as P

GRID = 512
PSIDE = 16
NBLK = GRID // PSIDE
LANES = 128
SUBLANES = 8

SIN_POLY = (4.442882919124345, -7.30824568650904, 3.6063542184326933, -0.8461116503732697, 0.10982451642490525)
COS_POLY = (1.4142134962552284, -6.978850948563788, 5.73946037690675, -1.8835579059841707, 0.3106880275217573)


def horner(square, coefficients):
    value = coefficients[-1] * square + coefficients[-2]
    for coefficient in coefficients[-3::-1]:
        value = value * square + coefficient
    return value


def cos_sin_turns(turns):
    rest = turns - jnp.round(turns)
    square = rest * rest
    sine = rest * horner(square, SIN_POLY)
    return (1.0 - sine * sine, sine * horner(square, COS_POLY))


def compiler_params(mebibytes):
    return pltpu.CompilerParams(vmem_limit_bytes=mebibytes << 20)


VMEM = pl.BlockSpec(memory_space=pltpu.VMEM)
HBM = pl.BlockSpec(memory_space=pltpu.HBM)


def dft_tables(length):
    indices = jnp.arange(length, dtype=jnp.int32)
    products_mod = indices[:, None] * indices[None, :] % length
    angle_table = products_mod.astype(jnp.float32) * (2.0 * jnp.pi / length)
    norm_scale = 1.0 / jnp.sqrt(jnp.float32(length))
    table_real = (jnp.cos(angle_table) * norm_scale).astype(jnp.bfloat16)
    table_imag = (jnp.sin(angle_table) * norm_scale).astype(jnp.bfloat16)
    return (table_real, table_imag)


def rotate_tiles(vis_pair, coords, sky_pos):
    l_coord = sky_pos[:, 0:1]
    m_coord = sky_pos[:, 1:2]
    w_term = jnp.sqrt(1.0 - l_coord * l_coord - m_coord * m_coord) - 1.0
    coords = coords.astype(jnp.float32)
    phase_angle = (
        2.0 * jnp.pi * (l_coord * coords[:, 0] + m_coord * coords[:, 1] + w_term * coords[:, 2])
    )
    cosine = jnp.cos(phase_angle)
    sine_part = jnp.sin(phase_angle)
    real_part = vis_pair[:, 0].astype(jnp.float32)
    imag_part = vis_pair[:, 1].astype(jnp.float32)
    rot_real = (real_part * cosine + imag_part * sine_part).astype(jnp.bfloat16)
    rot_imag = (imag_part * cosine - real_part * sine_part).astype(jnp.bfloat16)
    return (rot_real, rot_imag)


def stack_kernels(kernels):
    kern_real = kernels[:, 0]
    kern_imag = kernels[:, 1]
    upper_rows = jnp.concatenate([kern_real, kern_imag], axis=2)
    lower_rows = jnp.concatenate([-kern_imag, kern_real], axis=2)
    stacked_rows = jnp.concatenate([upper_rows, lower_rows], axis=0)
    return stacked_rows.reshape(-1, stacked_rows.shape[2])


def grid_tiles(rot_real, rot_imag, planes, stacked, plane_count):
    plane_select = (planes[:, None] == jnp.arange(plane_count)[None, :]).astype(jnp.bfloat16)
    spread = jnp.concatenate(
        [
            rot_real[:, None, :] * plane_select[:, :, None],
            rot_imag[:, None, :] * plane_select[:, :, None],
        ],
        axis=1,
    )
    spread = spread.reshape(spread.shape[0], -1)
    return jnp.dot(spread, stacked, preferred_element_type=jnp.float32).astype(jnp.bfloat16)


def shards(visibilities, uvw, facet_of, plane_of, cell_of, kernels, centers):
    peer_count = lax.axis_size("facet")
    tile_count = visibilities.shape[1]
    capacity = 4 * tile_count // peer_count
    total_slots = peer_count * capacity
    vis_pair = visibilities[0]
    coords = uvw[0]
    target = facet_of[0, :, 0]
    planes = plane_of[0]
    tile_cells = cell_of[0]
    plane_count = kernels.shape[0]
    stacked = stack_kernels(kernels)
    dest_hits = (target[:, None] == jnp.arange(peer_count)[None, :]).astype(jnp.int32)
    before = jnp.cumsum(dest_hits, axis=0) - dest_hits
    within_rank = jnp.sum(before * dest_hits, axis=1)
    slot_index = target * capacity + within_rank
    chosen = (target[:, None] == jnp.arange(centers.shape[0])[None, :]).astype(jnp.float32)
    sky_rows = jnp.sum(chosen[:, :, None] * centers[None, :, :], axis=1)
    rot_real, rot_imag = rotate_tiles(vis_pair, coords, sky_rows)
    own_patches = grid_tiles(rot_real, rot_imag, planes, stacked, plane_count)
    patch_buffer = (
        jnp.zeros((total_slots, own_patches.shape[1]), jnp.bfloat16).at[slot_index].set(own_patches)
    )
    cell_buffer = jnp.zeros((total_slots,), jnp.int32).at[slot_index].set(tile_cells)
    patches, slot_cells = (
        lax.all_to_all(
            patch_buffer.reshape(peer_count, capacity, -1),
            "facet",
            split_axis=0,
            concat_axis=0,
            tiled=True,
        ),
        lax.all_to_all(
            cell_buffer.reshape(peer_count, capacity),
            "facet",
            split_axis=0,
            concat_axis=0,
            tiled=True,
        ),
    )
    patches = patches.reshape(-1, patches.shape[-1])
    slot_cells = slot_cells.reshape(-1)
    nblocks = GRID // PSIDE
    ncells = nblocks * nblocks
    placing = (slot_cells[None, :] == jnp.arange(ncells)[:, None]).astype(jnp.bfloat16)
    blocks = jnp.dot(placing, patches, preferred_element_type=jnp.float32).astype(jnp.bfloat16)
    uv_grid = (
        blocks.reshape(nblocks, nblocks, 2, PSIDE, PSIDE)
        .transpose(2, 0, 3, 1, 4)
        .reshape(2 * GRID, GRID)
    )
    table_real, table_imag = dft_tables(GRID)
    table_both = jnp.concatenate([table_real, table_imag], axis=1)
    product = jnp.dot(uv_grid, table_both, preferred_element_type=jnp.float32)
    half_real = product[:GRID, :GRID] - product[GRID:, GRID:]
    half_imag = product[:GRID, GRID:] + product[GRID:, :GRID]
    partial_value = jnp.stack([half_real, half_imag]).astype(jnp.bfloat16)
    summed = lax.psum_scatter(
        partial_value.astype(jnp.float32).astype(jnp.bfloat16),
        "freq",
        scatter_dimension=2,
        tiled=True,
    )
    right_side = jnp.concatenate([summed[0], -summed[1]], axis=0)
    facet_image = jnp.dot(table_both, right_side, preferred_element_type=jnp.float32)
    return facet_image[None]


def gather_kernel(peers, capacity, centers_hbm, facet_hbm, plane_hbm, cell_hbm, vis_hbm, uvw_hbm, kern_hbm, *rest):
    out_refs = rest[:peers]
    centers_ref, facet_ref, plane_ref, cell_ref, vis_ref, uvw_ref, kern_ref, parts_ref, rows_ref, sems = rest[peers:]
    planes, _, depth, cells = kern_ref.shape
    tiles = facet_ref.shape[1]
    half = tiles // 2
    groups_of_lanes = depth // LANES
    small = [
        pltpu.make_async_copy(source, target, sems.at[i])
        for i, (source, target) in enumerate(
            (
                (centers_hbm, centers_ref),
                (facet_hbm, facet_ref),
                (plane_hbm, plane_ref),
                (vis_hbm, vis_ref),
                (uvw_hbm, uvw_ref),
                (cell_hbm, cell_ref),
            )
        )
    ]
    large = [
        pltpu.make_async_copy(kern_hbm.at[p], kern_ref.at[p], sems.at[len(small) + p]) for p in range(planes)
    ]
    for copy in small + large:
        copy.start()
    for copy in small[:3]:
        copy.wait()
    facet = facet_ref[...]
    l_row = jnp.zeros(facet.shape, jnp.float32)
    m_row = jnp.zeros(facet.shape, jnp.float32)
    for f in range(peers):
        hit = facet == f
        l_row = jnp.where(hit, centers_ref[0:1, f : f + 1], l_row)
        m_row = jnp.where(hit, centers_ref[1:2, f : f + 1], m_row)
    d_row = jnp.sqrt(1.0 - l_row * l_row - m_row * m_row) - 1.0
    plane_row = plane_ref[...].astype(jnp.float32)
    zero_row = jnp.zeros_like(l_row)
    columns = jnp.concatenate([l_row, m_row, d_row, plane_row] + [zero_row] * 4, axis=0).T

    relative = facet ^ lax.axis_index("facet")
    lanes = lax.broadcasted_iota(jnp.int32, (tiles, tiles), 1)
    earlier = (lax.broadcasted_iota(jnp.int32, (tiles, tiles), 0) < lanes).astype(jnp.float32).astype(jnp.bfloat16)
    hits = lax.broadcasted_iota(jnp.int32, (peers, tiles), 0) == relative
    before = jnp.dot(hits.astype(jnp.float32).astype(jnp.bfloat16), earlier, preferred_element_type=jnp.float32)
    rank = jnp.sum(jnp.where(hits, before, 0.0), axis=0, keepdims=True)
    slot = relative * capacity + rank.astype(jnp.int32)
    slots = peers * capacity

    for copy in small[3:]:
        copy.wait()
    parts_ref[...] = vis_ref[...].astype(jnp.float32)
    patches = []
    for h in range(2):
        tile_rows = slice(h * half, (h + 1) * half)
        l_col, m_col, d_col, plane_col = (
            jnp.broadcast_to(columns[tile_rows, i : i + 1], (half, LANES)) for i in range(4)
        )
        for j in range(groups_of_lanes):
            lane = slice(j * LANES, (j + 1) * LANES)
            u, v, w = (uvw_ref[i, tile_rows, lane].astype(jnp.float32) for i in range(3))
            cosine, sine = cos_sin_turns(l_col * u + m_col * v + d_col * w)
            first = 2 * (h * half * groups_of_lanes + j)
            real = parts_ref[pl.ds(first, half, stride=2 * groups_of_lanes), :]
            imag = parts_ref[pl.ds(first + 1, half, stride=2 * groups_of_lanes), :]
            rot_real = (real * cosine + imag * sine).astype(jnp.bfloat16)
            rot_imag = (imag * cosine - real * sine).astype(jnp.bfloat16)
            right = slice(depth + j * LANES, depth + (j + 1) * LANES)
            rows_ref[h, :half, lane] = rot_real
            rows_ref[h, :half, right] = -rot_imag
            rows_ref[h, half:, lane] = rot_imag
            rows_ref[h, half:, right] = rot_real
        total = None
        for p in range(planes):
            mask = (plane_col[:, 0:1] == float(p)).astype(jnp.float32).astype(jnp.bfloat16)
            mask = jnp.concatenate([mask, mask], axis=0)
            if h == 0:
                large[p].wait()
            product = jnp.dot(
                rows_ref[h] * mask, kern_ref[p].reshape(2 * depth, cells), preferred_element_type=jnp.float32
            )
            total = product if total is None else total + product
        patches.append(jnp.concatenate([total[:half], total[half:]], axis=1).astype(jnp.bfloat16))
    patches = jnp.concatenate(patches, axis=0)
    placing = lax.broadcasted_iota(jnp.int32, (slots, tiles), 0) == slot
    placing = placing.astype(jnp.float32).astype(jnp.bfloat16)
    placed = jnp.dot(placing, patches, preferred_element_type=jnp.float32).astype(jnp.bfloat16)
    cell = cell_ref[...].astype(jnp.float32)
    block_u = jnp.floor(cell * (1.0 / NBLK))
    block_v = cell - block_u * NBLK
    pair = jnp.concatenate([block_u, block_v] + [zero_row] * (SUBLANES - 2), axis=0).astype(jnp.bfloat16)
    pair = lax.dot_general(pair, placing, (((1,), (1,)), ((), ())), preferred_element_type=jnp.float32)
    pair = pair.astype(jnp.bfloat16)
    for s in range(peers):
        rows = slice(s * capacity, (s + 1) * capacity)
        for j in range(2 * cells // LANES):
            out_refs[s][j * capacity : (j + 1) * capacity, :] = placed[rows, j * LANES : (j + 1) * LANES]
        out_refs[s][2 * cells // LANES * capacity :, :] = pair[:, rows]


def image_kernel(peers, groups, capacity, table_ref, *rest):
    in_refs, out_refs = rest[:peers], rest[peers : peers + groups]
    phases_buf, patch_buf, table_buf = rest[peers + groups :]
    cells = PSIDE * PSIDE
    slots = peers * capacity
    share = cells // groups
    half_tiles = cells // LANES
    for s in range(peers):
        rows = slice(s * capacity, (s + 1) * capacity)
        below = slice(slots + s * capacity, slots + (s + 1) * capacity)
        for j in range(half_tiles):
            left = slice(j * LANES, (j + 1) * LANES)
            right = slice(cells + j * LANES, cells + (j + 1) * LANES)
            real = in_refs[s][j * capacity : (j + 1) * capacity, :]
            imag = in_refs[s][(half_tiles + j) * capacity : (half_tiles + j + 1) * capacity, :]
            patch_buf[rows, left] = real
            patch_buf[rows, right] = imag
            patch_buf[below, left] = -imag
            patch_buf[below, right] = real
    for s in range(groups):
        start = pl.multiple_of((lax.axis_index("freq") ^ s) * share, share)
        table_buf[s * share : (s + 1) * share, :] = table_ref[pl.ds(start, share), :]

    first = 2 * half_tiles * capacity
    block_u = jnp.concatenate([ref[first : first + SUBLANES, :][0:1].astype(jnp.float32) for ref in in_refs], axis=1)
    block_v = jnp.concatenate([ref[first : first + SUBLANES, :][1:2].astype(jnp.float32) for ref in in_refs], axis=1)
    index = lax.broadcasted_iota(jnp.int32, (NBLK, slots), 0).astype(jnp.float32)
    cos_u, sin_u = cos_sin_turns(index * block_u * (1.0 / NBLK))
    cos_v, sin_v = cos_sin_turns(index * block_v * (1.0 / NBLK))

    lane = lax.broadcasted_iota(jnp.int32, (NBLK, cells), 1)
    row = lax.broadcasted_iota(jnp.int32, (NBLK, cells), 0)
    patch_u, patch_v = lane // PSIDE, lane % PSIDE
    twid_u = cos_sin_turns((row * patch_u).astype(jnp.float32) * (1.0 / GRID))
    twid_v = cos_sin_turns((row * patch_v).astype(jnp.float32) * (1.0 / GRID))

    per_chunk = 8
    for chunk in range(NBLK // per_chunk):
        for i in range(per_chunk):
            j = chunk * per_chunk + i
            cu, su = cos_u[j : j + 1], sin_u[j : j + 1]
            rows = slice(i * NBLK, (i + 1) * NBLK)
            buf = phases_buf.at[chunk % 2]
            buf[rows, :slots] = (cu * cos_v - su * sin_v).astype(jnp.bfloat16)
            buf[rows, slots:] = (cu * sin_v + su * cos_v).astype(jnp.bfloat16)
        spectrum = jnp.dot(phases_buf[chunk % 2], patch_buf[...], preferred_element_type=jnp.float32)
        turned = []
        for i in range(per_chunk):
            j = chunk * per_chunk + i
            rows = slice(i * NBLK, (i + 1) * NBLK)
            real, imag = spectrum[rows, :cells], spectrum[rows, cells:]
            tr = twid_u[0][j : j + 1] * twid_v[0] - twid_u[1][j : j + 1] * twid_v[1]
            ti = twid_u[0][j : j + 1] * twid_v[1] + twid_u[1][j : j + 1] * twid_v[0]
            turned.append(jnp.concatenate([real * tr - imag * ti, real * ti + imag * tr], axis=1).astype(jnp.bfloat16))
        turned = jnp.concatenate(turned, axis=0)
        image = lax.dot_general(
            table_buf[...], turned, (((1,), (1,)), ((), ())), preferred_element_type=jnp.float32
        ).astype(jnp.bfloat16)
        width = per_chunk * NBLK
        for s in range(groups):
            out_refs[s][:, chunk * width : (chunk + 1) * width] = image[s * share : (s + 1) * share]


def finish_kernel(groups, *refs):
    in_refs, out_ref = refs[:groups], refs[groups]
    columns = PSIDE // groups
    per_tile = LANES // NBLK
    lane = lax.broadcasted_iota(jnp.int32, (PSIDE, LANES), 1) // NBLK
    for tile in range(NBLK // per_tile):
        lanes = slice(tile * LANES, (tile + 1) * LANES)
        total = in_refs[0][:, lanes].astype(jnp.float32)
        for ref in in_refs[1:]:
            total = total + ref[:, lanes].astype(jnp.float32)
        for i in range(per_tile):
            value = jnp.zeros((PSIDE, LANES), jnp.float32)
            for kq in range(columns):
                piece = total[kq * PSIDE : (kq + 1) * PSIDE]
                shift = (kq - i) * NBLK % LANES
                piece = pltpu.roll(piece, shift, 1) if shift else piece
                value = jnp.where(lane == kq, piece, value)
            out_ref[pl.ds(tile * per_tile + i, PSIDE, stride=NBLK), :] = value


def patch_table(groups):
    index = np.arange(PSIDE)
    kq, jq = (a.reshape(-1, 1) for a in np.meshgrid(index, index, indexing="ij"))
    pu, pv = (a.reshape(1, -1) for a in np.meshgrid(index, index, indexing="ij"))
    angle = 2.0 * np.pi * ((pu * jq + pv * kq) % PSIDE) / PSIDE
    return np.concatenate([np.cos(angle), -np.sin(angle)], axis=1) / GRID


def swap(piece, axis, distance):
    count = lax.axis_size(axis)
    return lax.ppermute(piece, axis, [(i, i ^ distance) for i in range(count)])


def packed_shards(visibilities, uvw, facet_of, plane_of, cell_of, kernels, centers):
    peers, groups = lax.axis_size("facet"), lax.axis_size("freq")
    tiles = visibilities.shape[1]
    capacity = 4 * tiles // peers
    planes, _, depth, cells = kernels.shape
    payload = jax.ShapeDtypeStruct((2 * cells // LANES * capacity + SUBLANES, LANES), jnp.bfloat16)
    lanes = depth // LANES
    vis_rows = visibilities[0].reshape(tiles, 2, lanes, LANES).transpose(0, 2, 1, 3).reshape(-1, LANES)
    operands = (
        centers.T,
        facet_of.reshape(1, tiles),
        plane_of,
        cell_of,
        vis_rows,
        uvw[0].transpose(1, 0, 2),
        kernels,
    )
    pieces = pl.pallas_call(
        functools.partial(gather_kernel, peers, capacity),
        out_shape=[payload] * peers,
        in_specs=[HBM] * len(operands),
        out_specs=[VMEM] * peers,
        scratch_shapes=[pltpu.VMEM(operand.shape, operand.dtype) for operand in operands]
        + [
            pltpu.VMEM(vis_rows.shape, jnp.float32),
            pltpu.VMEM((2, tiles, 2 * depth), jnp.bfloat16),
            pltpu.SemaphoreType.DMA((len(operands) - 1 + planes,)),
        ],
        compiler_params=compiler_params(40),
        name="gather",
    )(*(pltpu.with_memory_space_constraint(operand, pltpu.HBM) for operand in operands))
    received = [pieces[0]] + [swap(pieces[s], "facet", s) for s in range(1, peers)]
    share = cells // groups
    image = jax.ShapeDtypeStruct((share, NBLK * NBLK), jnp.bfloat16)
    slots = peers * capacity
    images = pl.pallas_call(
        functools.partial(image_kernel, peers, groups, capacity),
        out_shape=[image] * groups,
        in_specs=[VMEM] * (1 + peers),
        out_specs=[VMEM] * groups,
        scratch_shapes=[
            pltpu.VMEM((2, 8 * NBLK, 2 * slots), jnp.bfloat16),
            pltpu.VMEM((2 * slots, 2 * cells), jnp.bfloat16),
            pltpu.VMEM((cells, 2 * cells), jnp.bfloat16),
        ],
        compiler_params=compiler_params(40),
        name="image",
    )(jnp.asarray(patch_table(groups), jnp.bfloat16), *received)
    summed = [images[0]] + [swap(images[s], "freq", s) for s in range(1, groups)]
    facet_image = pl.pallas_call(
        functools.partial(finish_kernel, groups),
        out_shape=jax.ShapeDtypeStruct((GRID, GRID // groups), jnp.float32),
        in_specs=[VMEM] * groups,
        out_specs=VMEM,
        compiler_params=compiler_params(16),
        name="finish",
    )(*summed)
    return facet_image[None]


def solution(mesh):
    in_specs = (
        P("freq", "facet", None, None),
        P("freq", "facet", None, None),
        P("freq", "facet", None),
        P("freq", "facet"),
        P("freq", "facet"),
        P(),
        P(),
    )
    out_specs = P("facet", None, "freq")

    def body(*args):
        peers, groups = lax.axis_size("facet"), lax.axis_size("freq")
        capacity = 4 * args[0].shape[1] // peers
        powers = peers & (peers - 1) == 0 and groups & (groups - 1) == 0
        packed = capacity % LANES == 0 and powers and GRID // groups == LANES
        return (packed_shards if packed else shards)(*args)

    return jax.shard_map(body, mesh=mesh, in_specs=in_specs, out_specs=out_specs, check_vma=False)
```

```python
import functools

import jax
import jax.numpy as jnp
import numpy as np
from jax import lax
from jax.experimental import pallas as pl
from jax.experimental.pallas import tpu as pltpu
from jax.sharding import PartitionSpec as P


GRID = 512
PSIDE = 16
NBLK = GRID // PSIDE
LANES = 128
SUBLANES = 8

SIN_POLY = (4.442882919124345, -7.30824568650904, 3.6063542184326933, -0.8461116503732697, 0.10982451642490525)
COS_POLY = (1.4142134962552284, -6.978850948563788, 5.73946037690675, -1.8835579059841707, 0.3106880275217573)


def horner(square, coefficients):
    value = coefficients[-1] * square + coefficients[-2]
    for coefficient in coefficients[-3::-1]:
        value = value * square + coefficient
    return value


def cos_sin_turns(turns):
    rest = turns - jnp.round(turns)
    square = rest * rest
    sine = rest * horner(square, SIN_POLY)
    return (1.0 - sine * sine, sine * horner(square, COS_POLY))


def compiler_params(mebibytes):
    return pltpu.CompilerParams(vmem_limit_bytes=mebibytes << 20)


VMEM = pl.BlockSpec(memory_space=pltpu.VMEM)
HBM = pl.BlockSpec(memory_space=pltpu.HBM)


def dft_tables(length):
    indices = jnp.arange(length, dtype=jnp.int32)
    products_mod = indices[:, None] * indices[None, :] % length
    angle_table = products_mod.astype(jnp.float32) * (2.0 * jnp.pi / length)
    norm_scale = 1.0 / jnp.sqrt(jnp.float32(length))
    table_real = (jnp.cos(angle_table) * norm_scale).astype(jnp.bfloat16)
    table_imag = (jnp.sin(angle_table) * norm_scale).astype(jnp.bfloat16)
    return (table_real, table_imag)


def rotate_tiles(vis_pair, coords, sky_pos):
    l_coord = sky_pos[:, 0:1]
    m_coord = sky_pos[:, 1:2]
    w_term = jnp.sqrt(1.0 - l_coord * l_coord - m_coord * m_coord) - 1.0
    coords = coords.astype(jnp.float32)
    phase_angle = (
        2.0 * jnp.pi * (l_coord * coords[:, 0] + m_coord * coords[:, 1] + w_term * coords[:, 2])
    )
    cosine = jnp.cos(phase_angle)
    sine_part = jnp.sin(phase_angle)
    real_part = vis_pair[:, 0].astype(jnp.float32)
    imag_part = vis_pair[:, 1].astype(jnp.float32)
    rot_real = (real_part * cosine + imag_part * sine_part).astype(jnp.bfloat16)
    rot_imag = (imag_part * cosine - real_part * sine_part).astype(jnp.bfloat16)
    return (rot_real, rot_imag)


def stack_kernels(kernels):
    kern_real = kernels[:, 0]
    kern_imag = kernels[:, 1]
    upper_rows = jnp.concatenate([kern_real, kern_imag], axis=2)
    lower_rows = jnp.concatenate([-kern_imag, kern_real], axis=2)
    stacked_rows = jnp.concatenate([upper_rows, lower_rows], axis=0)
    return stacked_rows.reshape(-1, stacked_rows.shape[2])


def grid_tiles(rot_real, rot_imag, planes, stacked, plane_count):
    plane_select = (planes[:, None] == jnp.arange(plane_count)[None, :]).astype(jnp.bfloat16)
    spread = jnp.concatenate(
        [
            rot_real[:, None, :] * plane_select[:, :, None],
            rot_imag[:, None, :] * plane_select[:, :, None],
        ],
        axis=1,
    )
    spread = spread.reshape(spread.shape[0], -1)
    return jnp.dot(spread, stacked, preferred_element_type=jnp.float32).astype(jnp.bfloat16)


def shards(visibilities, uvw, facet_of, plane_of, cell_of, kernels, centers):
    peer_count = lax.axis_size("facet")
    tile_count = visibilities.shape[1]
    capacity = 4 * tile_count // peer_count
    total_slots = peer_count * capacity
    vis_pair = visibilities[0]
    coords = uvw[0]
    target = facet_of[0, :, 0]
    planes = plane_of[0]
    tile_cells = cell_of[0]
    plane_count = kernels.shape[0]
    stacked = stack_kernels(kernels)
    dest_hits = (target[:, None] == jnp.arange(peer_count)[None, :]).astype(jnp.int32)
    before = jnp.cumsum(dest_hits, axis=0) - dest_hits
    within_rank = jnp.sum(before * dest_hits, axis=1)
    slot_index = target * capacity + within_rank
    chosen = (target[:, None] == jnp.arange(centers.shape[0])[None, :]).astype(jnp.float32)
    sky_rows = jnp.sum(chosen[:, :, None] * centers[None, :, :], axis=1)
    rot_real, rot_imag = rotate_tiles(vis_pair, coords, sky_rows)
    own_patches = grid_tiles(rot_real, rot_imag, planes, stacked, plane_count)
    patch_buffer = (
        jnp.zeros((total_slots, own_patches.shape[1]), jnp.bfloat16).at[slot_index].set(own_patches)
    )
    cell_buffer = jnp.zeros((total_slots,), jnp.int32).at[slot_index].set(tile_cells)
    patches, slot_cells = (
        lax.all_to_all(
            patch_buffer.reshape(peer_count, capacity, -1),
            "facet",
            split_axis=0,
            concat_axis=0,
            tiled=True,
        ),
        lax.all_to_all(
            cell_buffer.reshape(peer_count, capacity),
            "facet",
            split_axis=0,
            concat_axis=0,
            tiled=True,
        ),
    )
    patches = patches.reshape(-1, patches.shape[-1])
    slot_cells = slot_cells.reshape(-1)
    nblocks = GRID // PSIDE
    ncells = nblocks * nblocks
    placing = (slot_cells[None, :] == jnp.arange(ncells)[:, None]).astype(jnp.bfloat16)
    blocks = jnp.dot(placing, patches, preferred_element_type=jnp.float32).astype(jnp.bfloat16)
    uv_grid = (
        blocks.reshape(nblocks, nblocks, 2, PSIDE, PSIDE)
        .transpose(2, 0, 3, 1, 4)
        .reshape(2 * GRID, GRID)
    )
    table_real, table_imag = dft_tables(GRID)
    table_both = jnp.concatenate([table_real, table_imag], axis=1)
    product = jnp.dot(uv_grid, table_both, preferred_element_type=jnp.float32)
    half_real = product[:GRID, :GRID] - product[GRID:, GRID:]
    half_imag = product[:GRID, GRID:] + product[GRID:, :GRID]
    partial_value = jnp.stack([half_real, half_imag]).astype(jnp.bfloat16)
    summed = lax.psum_scatter(
        partial_value.astype(jnp.float32).astype(jnp.bfloat16),
        "freq",
        scatter_dimension=2,
        tiled=True,
    )
    right_side = jnp.concatenate([summed[0], -summed[1]], axis=0)
    facet_image = jnp.dot(table_both, right_side, preferred_element_type=jnp.float32)
    return facet_image[None]


def gather_kernel(peers, capacity, centers_hbm, facet_hbm, plane_hbm, cell_hbm, vis_hbm, uvw_hbm, kern_hbm, *rest):
    out_refs = rest[:peers]
    centers_ref, facet_ref, plane_ref, cell_ref, vis_ref, uvw_ref, kern_ref, parts_ref, rows_ref, sems = rest[peers:]
    planes, _, depth, cells = kern_ref.shape
    tiles = facet_ref.shape[1]
    half = tiles // 2
    groups_of_lanes = depth // LANES
    rows_of = [slice(h * half, (h + 1) * half) for h in range(2)]
    vis_rows = vis_ref.shape[0] // 2
    transfers = [(centers_hbm, centers_ref), (facet_hbm, facet_ref), (plane_hbm, plane_ref)]
    for h in range(2):
        part = slice(h * vis_rows, (h + 1) * vis_rows)
        transfers += [(vis_hbm.at[part], vis_ref.at[part]), (uvw_hbm.at[:, rows_of[h]], uvw_ref.at[:, rows_of[h]])]
    transfers += [(cell_hbm, cell_ref)] + [(kern_hbm.at[p], kern_ref.at[p]) for p in range(planes)]
    copies = [pltpu.make_async_copy(source, target, sems.at[i]) for i, (source, target) in enumerate(transfers)]
    for copy in copies:
        copy.start()
    for copy in copies[:3]:
        copy.wait()
    facet = facet_ref[...]
    l_row = jnp.zeros(facet.shape, jnp.float32)
    m_row = jnp.zeros(facet.shape, jnp.float32)
    for f in range(peers):
        hit = facet == f
        l_row = jnp.where(hit, centers_ref[0:1, f : f + 1], l_row)
        m_row = jnp.where(hit, centers_ref[1:2, f : f + 1], m_row)
    d_row = jnp.sqrt(1.0 - l_row * l_row - m_row * m_row) - 1.0
    plane_row = plane_ref[...].astype(jnp.float32)
    zero_row = jnp.zeros_like(l_row)
    columns = jnp.concatenate([l_row, m_row, d_row, plane_row] + [zero_row] * 4, axis=0).T

    relative = facet ^ lax.axis_index("facet")
    lanes = lax.broadcasted_iota(jnp.int32, (tiles, tiles), 1)
    earlier = (lax.broadcasted_iota(jnp.int32, (tiles, tiles), 0) < lanes).astype(jnp.float32).astype(jnp.bfloat16)
    hits = lax.broadcasted_iota(jnp.int32, (peers, tiles), 0) == relative
    before = jnp.dot(hits.astype(jnp.float32).astype(jnp.bfloat16), earlier, preferred_element_type=jnp.float32)
    rank = jnp.sum(jnp.where(hits, before, 0.0), axis=0, keepdims=True)
    slot = relative * capacity + rank.astype(jnp.int32)
    slots = peers * capacity

    patches = []
    for h in range(2):
        tile_rows = rows_of[h]
        for copy in copies[3:5] if h == 0 else copies[5:]:
            copy.wait()
        part = slice(h * vis_rows, (h + 1) * vis_rows)
        parts_ref[part] = vis_ref[part].astype(jnp.float32)
        l_col, m_col, d_col = (jnp.broadcast_to(columns[tile_rows, i : i + 1], (half, LANES)) for i in range(3))
        for j in range(groups_of_lanes):
            lane = slice(j * LANES, (j + 1) * LANES)
            u, v, w = (uvw_ref[i, tile_rows, lane].astype(jnp.float32) for i in range(3))
            cosine, sine = cos_sin_turns(l_col * u + m_col * v + d_col * w)
            first = 2 * (h * half * groups_of_lanes + j)
            real = parts_ref[pl.ds(first, half, stride=2 * groups_of_lanes), :]
            imag = parts_ref[pl.ds(first + 1, half, stride=2 * groups_of_lanes), :]
            rot_real = (real * cosine + imag * sine).astype(jnp.bfloat16)
            rot_imag = (imag * cosine - real * sine).astype(jnp.bfloat16)
            right = slice(depth + j * LANES, depth + (j + 1) * LANES)
            rows_ref[h, :half, lane] = rot_real
            rows_ref[h, :half, right] = -rot_imag
            rows_ref[h, half:, lane] = rot_imag
            rows_ref[h, half:, right] = rot_real
    for h in range(2):
        plane_two = jnp.concatenate([columns[rows_of[h], 3:4]] * 2, axis=0)
        total = None
        for p in range(planes):
            mask = (plane_two == float(p)).astype(jnp.float32).astype(jnp.bfloat16)
            product = jnp.dot(
                rows_ref[h] * mask, kern_ref[p].reshape(2 * depth, cells), preferred_element_type=jnp.float32
            )
            total = product if total is None else total + product
        patches.append(jnp.concatenate([total[:half], total[half:]], axis=1).astype(jnp.bfloat16))
    patches = jnp.concatenate(patches, axis=0)
    placing = lax.broadcasted_iota(jnp.int32, (slots, tiles), 0) == slot
    placing = placing.astype(jnp.float32).astype(jnp.bfloat16)
    placed = jnp.dot(placing, patches, preferred_element_type=jnp.float32).astype(jnp.bfloat16)
    cell = cell_ref[...].astype(jnp.float32)
    block_u = jnp.floor(cell * (1.0 / NBLK))
    block_v = cell - block_u * NBLK
    pair = jnp.concatenate([block_u, block_v] + [zero_row] * (SUBLANES - 2), axis=0).astype(jnp.bfloat16)
    pair = lax.dot_general(pair, placing, (((1,), (1,)), ((), ())), preferred_element_type=jnp.float32)
    pair = pair.astype(jnp.bfloat16)
    for s in range(peers):
        rows = slice(s * capacity, (s + 1) * capacity)
        for j in range(2 * cells // LANES):
            out_refs[s][j * capacity : (j + 1) * capacity, :] = placed[rows, j * LANES : (j + 1) * LANES]
        out_refs[s][2 * cells // LANES * capacity :, :] = pair[:, rows]


def load_patches(in_refs, capacity, patch_buf):
    cells = PSIDE * PSIDE
    slots = len(in_refs) * capacity
    half_tiles = cells // LANES
    for s, ref in enumerate(in_refs):
        rows = slice(s * capacity, (s + 1) * capacity)
        below = slice(slots + s * capacity, slots + (s + 1) * capacity)
        for j in range(half_tiles):
            left = slice(j * LANES, (j + 1) * LANES)
            right = slice(cells + j * LANES, cells + (j + 1) * LANES)
            real = ref[j * capacity : (j + 1) * capacity, :]
            imag = ref[(half_tiles + j) * capacity : (half_tiles + j + 1) * capacity, :]
            patch_buf[rows, left] = real
            patch_buf[rows, right] = imag
            patch_buf[below, left] = -imag
            patch_buf[below, right] = real


def cell_phases(in_refs, capacity):
    first = 2 * PSIDE * PSIDE // LANES * capacity
    slots = len(in_refs) * capacity
    blocks = [ref[first : first + SUBLANES, :].astype(jnp.float32) for ref in in_refs]
    index = lax.broadcasted_iota(jnp.int32, (NBLK, slots), 0).astype(jnp.float32) * (1.0 / NBLK)
    return [
        part
        for row in range(2)
        for part in cos_sin_turns(index * jnp.concatenate([block[row : row + 1] for block in blocks], axis=1))
    ]


def fill_phases(buf, rows_of, phases):
    cos_u, sin_u, cos_v, sin_v = phases
    slots = cos_v.shape[1]
    for i, j in enumerate(rows_of):
        cu, su = cos_u[j : j + 1], sin_u[j : j + 1]
        rows = slice(i * NBLK, (i + 1) * NBLK)
        buf[rows, :slots] = (cu * cos_v - su * sin_v).astype(jnp.bfloat16)
        buf[rows, slots:] = (cu * sin_v + su * cos_v).astype(jnp.bfloat16)


PER_CHUNK = 8


def spectrum_kernel(near, capacity, *rest):
    in_refs, out_ref, (phases_buf, patch_buf) = rest[:near], rest[near], rest[near + 1 :]
    load_patches(in_refs, capacity, patch_buf)
    phases = cell_phases(in_refs, capacity)
    width = PER_CHUNK * NBLK
    for chunk in range(NBLK // PER_CHUNK):
        buf = phases_buf.at[chunk % 2]
        fill_phases(buf, range(chunk * PER_CHUNK, (chunk + 1) * PER_CHUNK), phases)
        out_ref[chunk * width : (chunk + 1) * width, :] = jnp.dot(
            buf[...], patch_buf[...], preferred_element_type=jnp.float32
        )


def image_kernel(far, groups, capacity, table_ref, near_ref, *rest):
    in_refs, out_refs = rest[:far], rest[far : far + groups]
    phases_buf, patch_buf, table_buf = rest[far + groups :]
    cells = PSIDE * PSIDE
    share = cells // groups
    load_patches(in_refs, capacity, patch_buf)
    for s in range(groups):
        start = pl.multiple_of((lax.axis_index("freq") ^ s) * share, share)
        table_buf[s * share : (s + 1) * share, :] = table_ref[pl.ds(start, share), :]
    phases = cell_phases(in_refs, capacity)

    lane = lax.broadcasted_iota(jnp.int32, (NBLK, cells), 1)
    row = lax.broadcasted_iota(jnp.int32, (NBLK, cells), 0)
    patch_u, patch_v = lane // PSIDE, lane % PSIDE
    twid_u = cos_sin_turns((row * patch_u).astype(jnp.float32) * (1.0 / GRID))
    twid_v = cos_sin_turns((row * patch_v).astype(jnp.float32) * (1.0 / GRID))

    width = PER_CHUNK * NBLK
    for chunk in range(NBLK // PER_CHUNK):
        buf = phases_buf.at[chunk % 2]
        fill_phases(buf, range(chunk * PER_CHUNK, (chunk + 1) * PER_CHUNK), phases)
        here = slice(chunk * width, (chunk + 1) * width)
        spectrum = near_ref[here, :] + jnp.dot(buf[...], patch_buf[...], preferred_element_type=jnp.float32)
        turned = []
        for i in range(PER_CHUNK):
            j = chunk * PER_CHUNK + i
            rows = slice(i * NBLK, (i + 1) * NBLK)
            real, imag = spectrum[rows, :cells], spectrum[rows, cells:]
            tr = twid_u[0][j : j + 1] * twid_v[0] - twid_u[1][j : j + 1] * twid_v[1]
            ti = twid_u[0][j : j + 1] * twid_v[1] + twid_u[1][j : j + 1] * twid_v[0]
            turned.append(jnp.concatenate([real * tr - imag * ti, real * ti + imag * tr], axis=1).astype(jnp.bfloat16))
        turned = jnp.concatenate(turned, axis=0)
        image = lax.dot_general(
            table_buf[...], turned, (((1,), (1,)), ((), ())), preferred_element_type=jnp.float32
        ).astype(jnp.bfloat16)
        for s in range(groups):
            out_refs[s][:, here] = image[s * share : (s + 1) * share]


def finish_kernel(groups, *refs):
    in_refs, out_ref = refs[:groups], refs[groups]
    columns = PSIDE // groups
    per_tile = LANES // NBLK
    lane = lax.broadcasted_iota(jnp.int32, (PSIDE, LANES), 1) // NBLK
    for tile in range(NBLK // per_tile):
        lanes = slice(tile * LANES, (tile + 1) * LANES)
        total = in_refs[0][:, lanes].astype(jnp.float32)
        for ref in in_refs[1:]:
            total = total + ref[:, lanes].astype(jnp.float32)
        for i in range(per_tile):
            value = jnp.zeros((PSIDE, LANES), jnp.float32)
            for kq in range(columns):
                piece = total[kq * PSIDE : (kq + 1) * PSIDE]
                shift = (kq - i) * NBLK % LANES
                piece = pltpu.roll(piece, shift, 1) if shift else piece
                value = jnp.where(lane == kq, piece, value)
            out_ref[pl.ds(tile * per_tile + i, PSIDE, stride=NBLK), :] = value


def patch_table(groups):
    index = np.arange(PSIDE)
    kq, jq = (a.reshape(-1, 1) for a in np.meshgrid(index, index, indexing="ij"))
    pu, pv = (a.reshape(1, -1) for a in np.meshgrid(index, index, indexing="ij"))
    angle = 2.0 * np.pi * ((pu * jq + pv * kq) % PSIDE) / PSIDE
    return np.concatenate([np.cos(angle), -np.sin(angle)], axis=1) / GRID


def swap(piece, axis, distance):
    count = lax.axis_size(axis)
    return lax.ppermute(piece, axis, [(i, i ^ distance) for i in range(count)])


def packed_shards(visibilities, uvw, facet_of, plane_of, cell_of, kernels, centers):
    peers, groups = lax.axis_size("facet"), lax.axis_size("freq")
    tiles = visibilities.shape[1]
    capacity = 4 * tiles // peers
    planes, _, depth, cells = kernels.shape
    payload = jax.ShapeDtypeStruct((2 * cells // LANES * capacity + SUBLANES, LANES), jnp.bfloat16)
    lanes = depth // LANES
    vis_rows = visibilities[0].reshape(tiles, 2, lanes, LANES).transpose(0, 2, 1, 3).reshape(-1, LANES)
    operands = (
        centers.T,
        facet_of.reshape(1, tiles),
        plane_of,
        cell_of,
        vis_rows,
        uvw[0].transpose(1, 0, 2),
        kernels,
    )
    pieces = pl.pallas_call(
        functools.partial(gather_kernel, peers, capacity),
        out_shape=[payload] * peers,
        in_specs=[HBM] * len(operands),
        out_specs=[VMEM] * peers,
        scratch_shapes=[pltpu.VMEM(operand.shape, operand.dtype) for operand in operands]
        + [
            pltpu.VMEM(vis_rows.shape, jnp.float32),
            pltpu.VMEM((2, tiles, 2 * depth), jnp.bfloat16),
            pltpu.SemaphoreType.DMA((len(operands) + 1 + planes,)),
        ],
        compiler_params=compiler_params(40),
        name="gather",
    )(*(pltpu.with_memory_space_constraint(operand, pltpu.HBM) for operand in operands))
    received = [pieces[0]] + [swap(pieces[s], "facet", s) for s in range(1, peers)]
    share = cells // groups
    near = peers // 2
    slots = near * capacity
    buffers = [
        pltpu.VMEM((2, PER_CHUNK * NBLK, 2 * slots), jnp.bfloat16),
        pltpu.VMEM((2 * slots, 2 * cells), jnp.bfloat16),
    ]
    points = NBLK * NBLK
    cost = pl.CostEstimate(flops=2 * points * 4 * slots * cells, bytes_accessed=4 << 20, transcendentals=0)
    spectrum = pl.pallas_call(
        functools.partial(spectrum_kernel, near, capacity),
        out_shape=jax.ShapeDtypeStruct((points, 2 * cells), jnp.float32),
        in_specs=[VMEM] * near,
        out_specs=VMEM,
        scratch_shapes=buffers,
        compiler_params=compiler_params(40),
        cost_estimate=cost,
        name="spectrum",
    )(*received[:near])
    image = jax.ShapeDtypeStruct((share, points), jnp.bfloat16)
    images = pl.pallas_call(
        functools.partial(image_kernel, peers - near, groups, capacity),
        out_shape=[image] * groups,
        in_specs=[VMEM] * (2 + peers - near),
        out_specs=[VMEM] * groups,
        scratch_shapes=buffers + [pltpu.VMEM((cells, 2 * cells), jnp.bfloat16)],
        compiler_params=compiler_params(40),
        cost_estimate=cost,
        name="image",
    )(jnp.asarray(patch_table(groups), jnp.bfloat16), spectrum, *received[near:])
    summed = [images[0]] + [swap(images[s], "freq", s) for s in range(1, groups)]
    facet_image = pl.pallas_call(
        functools.partial(finish_kernel, groups),
        out_shape=jax.ShapeDtypeStruct((GRID, GRID // groups), jnp.float32),
        in_specs=[VMEM] * groups,
        out_specs=VMEM,
        compiler_params=compiler_params(16),
        name="finish",
    )(*summed)
    return facet_image[None]


def solution(mesh):
    in_specs = (
        P("freq", "facet", None, None),
        P("freq", "facet", None, None),
        P("freq", "facet", None),
        P("freq", "facet"),
        P("freq", "facet"),
        P(),
        P(),
    )
    out_specs = P("facet", None, "freq")

    def body(*args):
        peers, groups = lax.axis_size("facet"), lax.axis_size("freq")
        capacity = 4 * args[0].shape[1] // peers
        powers = peers & (peers - 1) == 0 and groups & (groups - 1) == 0
        packed = capacity % LANES == 0 and powers and GRID // groups == LANES
        return (packed_shards if packed else shards)(*args)

    return jax.shard_map(body, mesh=mesh, in_specs=in_specs, out_specs=out_specs, check_vma=False)
```

```python
import functools

import jax
import jax.numpy as jnp
import numpy as np
from jax import lax
from jax.experimental import pallas as pl
from jax.experimental.pallas import tpu as pltpu
from jax.sharding import PartitionSpec as P


GRID = 512
PSIDE = 16
NBLK = GRID // PSIDE
LANES = 128
SUBLANES = 8

SIN_POLY = (4.442882919124345, -7.30824568650904, 3.6063542184326933, -0.8461116503732697, 0.10982451642490525)
COS_POLY = (1.4142134962552284, -6.978850948563788, 5.73946037690675, -1.8835579059841707, 0.3106880275217573)


def horner(square, coefficients):
    value = coefficients[-1] * square + coefficients[-2]
    for coefficient in coefficients[-3::-1]:
        value = value * square + coefficient
    return value


def cos_sin_turns(turns):
    rest = turns - jnp.round(turns)
    square = rest * rest
    sine = rest * horner(square, SIN_POLY)
    return (1.0 - sine * sine, sine * horner(square, COS_POLY))


def compiler_params(mebibytes):
    return pltpu.CompilerParams(vmem_limit_bytes=mebibytes << 20)


VMEM = pl.BlockSpec(memory_space=pltpu.VMEM)
HBM = pl.BlockSpec(memory_space=pltpu.HBM)


def dft_tables(length):
    indices = jnp.arange(length, dtype=jnp.int32)
    products_mod = indices[:, None] * indices[None, :] % length
    angle_table = products_mod.astype(jnp.float32) * (2.0 * jnp.pi / length)
    norm_scale = 1.0 / jnp.sqrt(jnp.float32(length))
    table_real = (jnp.cos(angle_table) * norm_scale).astype(jnp.bfloat16)
    table_imag = (jnp.sin(angle_table) * norm_scale).astype(jnp.bfloat16)
    return (table_real, table_imag)


def rotate_tiles(vis_pair, coords, sky_pos):
    l_coord = sky_pos[:, 0:1]
    m_coord = sky_pos[:, 1:2]
    w_term = jnp.sqrt(1.0 - l_coord * l_coord - m_coord * m_coord) - 1.0
    coords = coords.astype(jnp.float32)
    phase_angle = (
        2.0 * jnp.pi * (l_coord * coords[:, 0] + m_coord * coords[:, 1] + w_term * coords[:, 2])
    )
    cosine = jnp.cos(phase_angle)
    sine_part = jnp.sin(phase_angle)
    real_part = vis_pair[:, 0].astype(jnp.float32)
    imag_part = vis_pair[:, 1].astype(jnp.float32)
    rot_real = (real_part * cosine + imag_part * sine_part).astype(jnp.bfloat16)
    rot_imag = (imag_part * cosine - real_part * sine_part).astype(jnp.bfloat16)
    return (rot_real, rot_imag)


def stack_kernels(kernels):
    kern_real = kernels[:, 0]
    kern_imag = kernels[:, 1]
    upper_rows = jnp.concatenate([kern_real, kern_imag], axis=2)
    lower_rows = jnp.concatenate([-kern_imag, kern_real], axis=2)
    stacked_rows = jnp.concatenate([upper_rows, lower_rows], axis=0)
    return stacked_rows.reshape(-1, stacked_rows.shape[2])


def grid_tiles(rot_real, rot_imag, planes, stacked, plane_count):
    plane_select = (planes[:, None] == jnp.arange(plane_count)[None, :]).astype(jnp.bfloat16)
    spread = jnp.concatenate(
        [
            rot_real[:, None, :] * plane_select[:, :, None],
            rot_imag[:, None, :] * plane_select[:, :, None],
        ],
        axis=1,
    )
    spread = spread.reshape(spread.shape[0], -1)
    return jnp.dot(spread, stacked, preferred_element_type=jnp.float32).astype(jnp.bfloat16)


def shards(visibilities, uvw, facet_of, plane_of, cell_of, kernels, centers):
    peer_count = lax.axis_size("facet")
    tile_count = visibilities.shape[1]
    capacity = 4 * tile_count // peer_count
    total_slots = peer_count * capacity
    vis_pair = visibilities[0]
    coords = uvw[0]
    target = facet_of[0, :, 0]
    planes = plane_of[0]
    tile_cells = cell_of[0]
    plane_count = kernels.shape[0]
    stacked = stack_kernels(kernels)
    dest_hits = (target[:, None] == jnp.arange(peer_count)[None, :]).astype(jnp.int32)
    before = jnp.cumsum(dest_hits, axis=0) - dest_hits
    within_rank = jnp.sum(before * dest_hits, axis=1)
    slot_index = target * capacity + within_rank
    chosen = (target[:, None] == jnp.arange(centers.shape[0])[None, :]).astype(jnp.float32)
    sky_rows = jnp.sum(chosen[:, :, None] * centers[None, :, :], axis=1)
    rot_real, rot_imag = rotate_tiles(vis_pair, coords, sky_rows)
    own_patches = grid_tiles(rot_real, rot_imag, planes, stacked, plane_count)
    patch_buffer = (
        jnp.zeros((total_slots, own_patches.shape[1]), jnp.bfloat16).at[slot_index].set(own_patches)
    )
    cell_buffer = jnp.zeros((total_slots,), jnp.int32).at[slot_index].set(tile_cells)
    patches, slot_cells = (
        lax.all_to_all(
            patch_buffer.reshape(peer_count, capacity, -1),
            "facet",
            split_axis=0,
            concat_axis=0,
            tiled=True,
        ),
        lax.all_to_all(
            cell_buffer.reshape(peer_count, capacity),
            "facet",
            split_axis=0,
            concat_axis=0,
            tiled=True,
        ),
    )
    patches = patches.reshape(-1, patches.shape[-1])
    slot_cells = slot_cells.reshape(-1)
    nblocks = GRID // PSIDE
    ncells = nblocks * nblocks
    placing = (slot_cells[None, :] == jnp.arange(ncells)[:, None]).astype(jnp.bfloat16)
    blocks = jnp.dot(placing, patches, preferred_element_type=jnp.float32).astype(jnp.bfloat16)
    uv_grid = (
        blocks.reshape(nblocks, nblocks, 2, PSIDE, PSIDE)
        .transpose(2, 0, 3, 1, 4)
        .reshape(2 * GRID, GRID)
    )
    table_real, table_imag = dft_tables(GRID)
    table_both = jnp.concatenate([table_real, table_imag], axis=1)
    product = jnp.dot(uv_grid, table_both, preferred_element_type=jnp.float32)
    half_real = product[:GRID, :GRID] - product[GRID:, GRID:]
    half_imag = product[:GRID, GRID:] + product[GRID:, :GRID]
    partial_value = jnp.stack([half_real, half_imag]).astype(jnp.bfloat16)
    summed = lax.psum_scatter(
        partial_value.astype(jnp.float32).astype(jnp.bfloat16),
        "freq",
        scatter_dimension=2,
        tiled=True,
    )
    right_side = jnp.concatenate([summed[0], -summed[1]], axis=0)
    facet_image = jnp.dot(table_both, right_side, preferred_element_type=jnp.float32)
    return facet_image[None]


def gather_kernel(peers, sizes, centers_hbm, facet_hbm, plane_hbm, cell_hbm, vis_hbm, uvw_hbm, kern_hbm, *rest):
    out_refs = rest[: len(sizes)]
    centers_ref, facet_ref, plane_ref, cell_ref, vis_ref, uvw_ref, kern_ref, parts_ref, rows_ref, sems = rest[len(sizes) :]
    planes, _, depth, cells = kern_ref.shape
    tiles = facet_ref.shape[1]
    half = tiles // 2
    groups_of_lanes = depth // LANES
    rows_of = [slice(h * half, (h + 1) * half) for h in range(2)]
    vis_rows = vis_ref.shape[0] // 2
    transfers = [(centers_hbm, centers_ref), (facet_hbm, facet_ref), (plane_hbm, plane_ref)]
    for h in range(2):
        part = slice(h * vis_rows, (h + 1) * vis_rows)
        transfers += [(vis_hbm.at[part], vis_ref.at[part]), (uvw_hbm.at[:, rows_of[h]], uvw_ref.at[:, rows_of[h]])]
    transfers += [(cell_hbm, cell_ref)] + [(kern_hbm.at[p], kern_ref.at[p]) for p in range(planes)]
    copies = [pltpu.make_async_copy(source, target, sems.at[i]) for i, (source, target) in enumerate(transfers)]
    for copy in copies:
        copy.start()
    for copy in copies[:3]:
        copy.wait()
    facet = facet_ref[...]
    l_row = jnp.zeros(facet.shape, jnp.float32)
    m_row = jnp.zeros(facet.shape, jnp.float32)
    for f in range(peers):
        hit = facet == f
        l_row = jnp.where(hit, centers_ref[0:1, f : f + 1], l_row)
        m_row = jnp.where(hit, centers_ref[1:2, f : f + 1], m_row)
    d_row = jnp.sqrt(1.0 - l_row * l_row - m_row * m_row) - 1.0
    plane_row = plane_ref[...].astype(jnp.float32)
    zero_row = jnp.zeros_like(l_row)
    columns = jnp.concatenate([l_row, m_row, d_row, plane_row] + [zero_row] * 4, axis=0).T

    near, capacity, few, slots = peers // 2, sizes[0], sizes[peers // 2], sum(sizes)
    relative = facet ^ lax.axis_index("facet")
    lanes = lax.broadcasted_iota(jnp.int32, (tiles, tiles), 1)
    earlier = (lax.broadcasted_iota(jnp.int32, (tiles, tiles), 0) < lanes).astype(jnp.float32).astype(jnp.bfloat16)
    facets = lax.broadcasted_iota(jnp.int32, (peers, tiles), 0)
    hits = facets == relative
    before = jnp.dot(hits.astype(jnp.float32).astype(jnp.bfloat16), earlier, preferred_element_type=jnp.float32)
    rank = jnp.sum(jnp.where(hits, before, 0.0), axis=0, keepdims=True).astype(jnp.int32)
    passed = jnp.where(facets >= near, jnp.maximum(before - few, 0.0), 0.0)
    passed = jnp.sum(passed, axis=0, keepdims=True).astype(jnp.int32)
    direct = near * capacity + (relative - near) * few + rank
    slot = jnp.where(rank < few, direct, near * (capacity + few) + passed)
    slot = jnp.where(relative < near, relative * capacity + rank, slot)

    patches = []
    for h in range(2):
        tile_rows = rows_of[h]
        for copy in copies[3:5] if h == 0 else copies[5:]:
            copy.wait()
        part = slice(h * vis_rows, (h + 1) * vis_rows)
        parts_ref[part] = vis_ref[part].astype(jnp.float32)
        l_col, m_col, d_col = (jnp.broadcast_to(columns[tile_rows, i : i + 1], (half, LANES)) for i in range(3))
        for j in range(groups_of_lanes):
            lane = slice(j * LANES, (j + 1) * LANES)
            u, v, w = (uvw_ref[i, tile_rows, lane].astype(jnp.float32) for i in range(3))
            cosine, sine = cos_sin_turns(l_col * u + m_col * v + d_col * w)
            first = 2 * (h * half * groups_of_lanes + j)
            real = parts_ref[pl.ds(first, half, stride=2 * groups_of_lanes), :]
            imag = parts_ref[pl.ds(first + 1, half, stride=2 * groups_of_lanes), :]
            rot_real = (real * cosine + imag * sine).astype(jnp.bfloat16)
            rot_imag = (imag * cosine - real * sine).astype(jnp.bfloat16)
            right = slice(depth + j * LANES, depth + (j + 1) * LANES)
            rows_ref[h, :half, lane] = rot_real
            rows_ref[h, :half, right] = -rot_imag
            rows_ref[h, half:, lane] = rot_imag
            rows_ref[h, half:, right] = rot_real
    for h in range(2):
        plane_two = jnp.concatenate([columns[rows_of[h], 3:4]] * 2, axis=0)
        total = None
        for p in range(planes):
            mask = (plane_two == float(p)).astype(jnp.float32).astype(jnp.bfloat16)
            product = jnp.dot(
                rows_ref[h] * mask, kern_ref[p].reshape(2 * depth, cells), preferred_element_type=jnp.float32
            )
            total = product if total is None else total + product
        patches.append(jnp.concatenate([total[:half], total[half:]], axis=1).astype(jnp.bfloat16))
    patches = jnp.concatenate(patches, axis=0)
    placing = lax.broadcasted_iota(jnp.int32, (slots, tiles), 0) == slot
    placing = placing.astype(jnp.float32).astype(jnp.bfloat16)
    placed = jnp.dot(placing, patches, preferred_element_type=jnp.float32).astype(jnp.bfloat16)
    cell = cell_ref[...].astype(jnp.float32)
    block_u = jnp.floor(cell * (1.0 / NBLK))
    block_v = cell - block_u * NBLK
    labels = [block_u, block_v, facet.astype(jnp.float32)] + [zero_row] * (SUBLANES - 3)
    labels = jnp.concatenate(labels, axis=0).astype(jnp.bfloat16)
    labels = lax.dot_general(labels, placing, (((1,), (1,)), ((), ())), preferred_element_type=jnp.float32)
    lane = lax.broadcasted_iota(jnp.int32, (SUBLANES, LANES), 1)
    start = 0
    for ref, size in zip(out_refs, sizes):
        for j in range(2 * cells // LANES):
            ref[j * size : (j + 1) * size, :] = placed[start : start + size, j * LANES : (j + 1) * LANES]
        tile = start // LANES * LANES
        inside = (lane >= start - tile) & (lane < start - tile + size)
        ref[2 * cells // LANES * size :, :] = jnp.where(inside, labels[:, tile : tile + LANES], 0.0).astype(jnp.bfloat16)
        start += size


def load_patches(in_refs, sizes, patch_buf):
    cells = PSIDE * PSIDE
    half_tiles = cells // LANES
    start = 0
    for ref, size in zip(in_refs, sizes):
        rows = slice(start, start + size)
        below = slice(sum(sizes) + start, sum(sizes) + start + size)
        for j in range(half_tiles):
            left = slice(j * LANES, (j + 1) * LANES)
            right = slice(cells + j * LANES, cells + (j + 1) * LANES)
            real = ref[j * size : (j + 1) * size, :]
            imag = ref[(half_tiles + j) * size : (half_tiles + j + 1) * size, :]
            patch_buf[rows, left] = real
            patch_buf[rows, right] = imag
            patch_buf[below, left] = -imag
            patch_buf[below, right] = real
        start += size


def cell_phases(in_refs, sizes, direct):
    labels, start = [], 0
    for ref, size in zip(in_refs, sizes):
        here = ref[2 * PSIDE * PSIDE // LANES * size :, :].astype(jnp.float32)
        if start % LANES:
            labels[-1] = labels[-1] + here
        else:
            labels.append(here)
        start += size
    labels = jnp.concatenate(labels, axis=1)
    lane = lax.broadcasted_iota(jnp.int32, (1, start), 1)
    mine = labels[2:3] == lax.axis_index("facet").astype(jnp.float32)
    mine = jnp.where(mine | (lane < sum(sizes[:direct])), 1.0, 0.0)
    index = lax.broadcasted_iota(jnp.int32, (NBLK, start), 0).astype(jnp.float32) * (1.0 / NBLK)
    cos_u, sin_u = cos_sin_turns(index * labels[0:1])
    return (cos_u * mine, sin_u * mine) + cos_sin_turns(index * labels[1:2])


def fill_phases(buf, rows_of, phases):
    cos_u, sin_u, cos_v, sin_v = phases
    slots = cos_v.shape[1]
    for i, j in enumerate(rows_of):
        cu, su = cos_u[j : j + 1], sin_u[j : j + 1]
        rows = slice(i * NBLK, (i + 1) * NBLK)
        buf[rows, :slots] = (cu * cos_v - su * sin_v).astype(jnp.bfloat16)
        buf[rows, slots:] = (cu * sin_v + su * cos_v).astype(jnp.bfloat16)


PER_CHUNK = 8


def spectrum_kernel(sizes, direct, *rest):
    count = len(sizes)
    in_refs, out_ref, (phases_buf, patch_buf) = rest[:count], rest[count], rest[count + 1 :]
    load_patches(in_refs, sizes, patch_buf)
    phases = cell_phases(in_refs, sizes, direct)
    width = PER_CHUNK * NBLK
    for chunk in range(NBLK // PER_CHUNK):
        buf = phases_buf.at[chunk % 2]
        fill_phases(buf, range(chunk * PER_CHUNK, (chunk + 1) * PER_CHUNK), phases)
        out_ref[chunk * width : (chunk + 1) * width, :] = jnp.dot(
            buf[...], patch_buf[...], preferred_element_type=jnp.float32
        )


def image_kernel(sizes, direct, groups, table_ref, early_ref, *rest):
    count = len(sizes)
    in_refs, out_refs = rest[:count], rest[count : count + groups]
    phases_buf, patch_buf, table_buf = rest[count + groups :]
    cells = PSIDE * PSIDE
    share = cells // groups
    load_patches(in_refs, sizes, patch_buf)
    for s in range(groups):
        start = pl.multiple_of((lax.axis_index("freq") ^ s) * share, share)
        table_buf[s * share : (s + 1) * share, :] = table_ref[pl.ds(start, share), :]
    phases = cell_phases(in_refs, sizes, direct)

    lane = lax.broadcasted_iota(jnp.int32, (NBLK, cells), 1)
    row = lax.broadcasted_iota(jnp.int32, (NBLK, cells), 0)
    patch_u, patch_v = lane // PSIDE, lane % PSIDE
    twid_u = cos_sin_turns((row * patch_u).astype(jnp.float32) * (1.0 / GRID))
    twid_v = cos_sin_turns((row * patch_v).astype(jnp.float32) * (1.0 / GRID))

    width = PER_CHUNK * NBLK
    for chunk in range(NBLK // PER_CHUNK):
        buf = phases_buf.at[chunk % 2]
        fill_phases(buf, range(chunk * PER_CHUNK, (chunk + 1) * PER_CHUNK), phases)
        here = slice(chunk * width, (chunk + 1) * width)
        spectrum = early_ref[here, :] + jnp.dot(buf[...], patch_buf[...], preferred_element_type=jnp.float32)
        turned = []
        for i in range(PER_CHUNK):
            j = chunk * PER_CHUNK + i
            rows = slice(i * NBLK, (i + 1) * NBLK)
            real, imag = spectrum[rows, :cells], spectrum[rows, cells:]
            tr = twid_u[0][j : j + 1] * twid_v[0] - twid_u[1][j : j + 1] * twid_v[1]
            ti = twid_u[0][j : j + 1] * twid_v[1] + twid_u[1][j : j + 1] * twid_v[0]
            turned.append(jnp.concatenate([real * tr - imag * ti, real * ti + imag * tr], axis=1).astype(jnp.bfloat16))
        turned = jnp.concatenate(turned, axis=0)
        image = lax.dot_general(
            table_buf[...], turned, (((1,), (1,)), ((), ())), preferred_element_type=jnp.float32
        ).astype(jnp.bfloat16)
        for s in range(groups):
            out_refs[s][:, here] = image[s * share : (s + 1) * share]


def finish_kernel(groups, *refs):
    in_refs, out_ref = refs[:groups], refs[groups]
    columns = PSIDE // groups
    per_tile = LANES // NBLK
    lane = lax.broadcasted_iota(jnp.int32, (PSIDE, LANES), 1) // NBLK
    for tile in range(NBLK // per_tile):
        lanes = slice(tile * LANES, (tile + 1) * LANES)
        total = in_refs[0][:, lanes].astype(jnp.float32)
        for ref in in_refs[1:]:
            total = total + ref[:, lanes].astype(jnp.float32)
        for i in range(per_tile):
            value = jnp.zeros((PSIDE, LANES), jnp.float32)
            for kq in range(columns):
                piece = total[kq * PSIDE : (kq + 1) * PSIDE]
                shift = (kq - i) * NBLK % LANES
                piece = pltpu.roll(piece, shift, 1) if shift else piece
                value = jnp.where(lane == kq, piece, value)
            out_ref[pl.ds(tile * per_tile + i, PSIDE, stride=NBLK), :] = value


def patch_table():
    index = np.arange(PSIDE)
    kq, jq = (a.reshape(-1, 1) for a in np.meshgrid(index, index, indexing="ij"))
    pu, pv = (a.reshape(1, -1) for a in np.meshgrid(index, index, indexing="ij"))
    angle = 2.0 * np.pi * ((pu * jq + pv * kq) % PSIDE) / PSIDE
    return np.concatenate([np.cos(angle), -np.sin(angle)], axis=1) / GRID


def swap(piece, axis, distance):
    count = lax.axis_size(axis)
    return lax.ppermute(piece, axis, [(i, i ^ distance) for i in range(count)])


def packed_shards(visibilities, uvw, facet_of, plane_of, cell_of, kernels, centers):
    peers, groups = lax.axis_size("facet"), lax.axis_size("freq")
    tiles = visibilities.shape[1]
    capacity = 4 * tiles // peers
    planes, _, depth, cells = kernels.shape
    near = peers // 2
    sizes = [capacity] * near + [capacity // 2] * near + [tiles // 2]
    payloads = [jax.ShapeDtypeStruct((2 * cells // LANES * size + SUBLANES, LANES), jnp.bfloat16) for size in sizes]
    lanes = depth // LANES
    vis_rows = visibilities[0].reshape(tiles, 2, lanes, LANES).transpose(0, 2, 1, 3).reshape(-1, LANES)
    operands = (
        centers.T,
        facet_of.reshape(1, tiles),
        plane_of,
        cell_of,
        vis_rows,
        uvw[0].transpose(1, 0, 2),
        kernels,
    )
    pieces = pl.pallas_call(
        functools.partial(gather_kernel, peers, sizes),
        out_shape=payloads,
        in_specs=[HBM] * len(operands),
        out_specs=[VMEM] * len(sizes),
        scratch_shapes=[pltpu.VMEM(operand.shape, operand.dtype) for operand in operands]
        + [
            pltpu.VMEM(vis_rows.shape, jnp.float32),
            pltpu.VMEM((2, tiles, 2 * depth), jnp.bfloat16),
            pltpu.SemaphoreType.DMA((len(operands) + 1 + planes,)),
        ],
        compiler_params=compiler_params(40),
        name="gather",
    )(*(pltpu.with_memory_space_constraint(operand, pltpu.HBM) for operand in operands))
    overflow = [swap(pieces[peers], "facet", near)]
    received = [pieces[0]] + [swap(pieces[s], "facet", s) for s in range(1, peers)]
    overflow += [swap(overflow[0], "facet", s) for s in range(1, near)]
    early, late = received[:near] + overflow[:1], received[near:] + overflow[1:]
    early_sizes, late_sizes = sizes[:near] + sizes[peers:], sizes[near:peers] + sizes[peers:] * (near - 1)
    share = cells // groups
    points = NBLK * NBLK

    def buffers_and_cost(slots):
        buffers = [
            pltpu.VMEM((2, PER_CHUNK * NBLK, 2 * slots), jnp.bfloat16),
            pltpu.VMEM((2 * slots, 2 * cells), jnp.bfloat16),
        ]
        return buffers, pl.CostEstimate(flops=8 * points * slots * cells, bytes_accessed=4 << 20, transcendentals=0)

    buffers, cost = buffers_and_cost(sum(early_sizes))
    spectrum = pl.pallas_call(
        functools.partial(spectrum_kernel, early_sizes, near),
        out_shape=jax.ShapeDtypeStruct((points, 2 * cells), jnp.float32),
        in_specs=[VMEM] * len(early),
        out_specs=VMEM,
        scratch_shapes=buffers,
        compiler_params=compiler_params(40),
        cost_estimate=cost,
        name="spectrum",
    )(*early)
    buffers, cost = buffers_and_cost(sum(late_sizes))
    image = jax.ShapeDtypeStruct((share, points), jnp.bfloat16)
    images = pl.pallas_call(
        functools.partial(image_kernel, late_sizes, near, groups),
        out_shape=[image] * groups,
        in_specs=[VMEM] * (2 + len(late)),
        out_specs=[VMEM] * groups,
        scratch_shapes=buffers + [pltpu.VMEM((cells, 2 * cells), jnp.bfloat16)],
        compiler_params=compiler_params(40),
        cost_estimate=cost,
        name="image",
    )(jnp.asarray(patch_table(), jnp.bfloat16), spectrum, *late)
    summed = [images[0]] + [swap(images[s], "freq", s) for s in range(1, groups)]
    facet_image = pl.pallas_call(
        functools.partial(finish_kernel, groups),
        out_shape=jax.ShapeDtypeStruct((GRID, GRID // groups), jnp.float32),
        in_specs=[VMEM] * groups,
        out_specs=VMEM,
        compiler_params=compiler_params(16),
        name="finish",
    )(*summed)
    return facet_image[None]


def solution(mesh):
    in_specs = (
        P("freq", "facet", None, None),
        P("freq", "facet", None, None),
        P("freq", "facet", None),
        P("freq", "facet"),
        P("freq", "facet"),
        P(),
        P(),
    )
    out_specs = P("facet", None, "freq")

    def body(*args):
        peers, groups = lax.axis_size("facet"), lax.axis_size("freq")
        capacity = 4 * args[0].shape[1] // peers
        powers = peers & (peers - 1) == 0 and groups & (groups - 1) == 0
        packed = capacity == LANES and powers and GRID // groups == LANES
        return (packed_shards if packed else shards)(*args)

    return jax.shard_map(body, mesh=mesh, in_specs=in_specs, out_specs=out_specs, check_vma=False)
```

```python
import functools

import jax
import jax.numpy as jnp
import numpy as np
from jax import lax
from jax.experimental import pallas as pl
from jax.experimental.pallas import tpu as pltpu
from jax.sharding import PartitionSpec as P


GRID = 512
PSIDE = 16
NBLK = GRID // PSIDE
LANES = 128
SUBLANES = 8

SIN_POLY = (4.442882919124345, -7.30824568650904, 3.6063542184326933, -0.8461116503732697, 0.10982451642490525)
COS_POLY = (1.4142134962552284, -6.978850948563788, 5.73946037690675, -1.8835579059841707, 0.3106880275217573)


def horner(square, coefficients):
    value = coefficients[-1] * square + coefficients[-2]
    for coefficient in coefficients[-3::-1]:
        value = value * square + coefficient
    return value


def cos_sin_turns(turns):
    rest = turns - jnp.round(turns)
    square = rest * rest
    sine = rest * horner(square, SIN_POLY)
    return (1.0 - sine * sine, sine * horner(square, COS_POLY))


def compiler_params(mebibytes):
    return pltpu.CompilerParams(vmem_limit_bytes=mebibytes << 20)


VMEM = pl.BlockSpec(memory_space=pltpu.VMEM)
HBM = pl.BlockSpec(memory_space=pltpu.HBM)


def dft_tables(length):
    indices = jnp.arange(length, dtype=jnp.int32)
    products_mod = indices[:, None] * indices[None, :] % length
    angle_table = products_mod.astype(jnp.float32) * (2.0 * jnp.pi / length)
    norm_scale = 1.0 / jnp.sqrt(jnp.float32(length))
    table_real = (jnp.cos(angle_table) * norm_scale).astype(jnp.bfloat16)
    table_imag = (jnp.sin(angle_table) * norm_scale).astype(jnp.bfloat16)
    return (table_real, table_imag)


def rotate_tiles(vis_pair, coords, sky_pos):
    l_coord = sky_pos[:, 0:1]
    m_coord = sky_pos[:, 1:2]
    w_term = jnp.sqrt(1.0 - l_coord * l_coord - m_coord * m_coord) - 1.0
    coords = coords.astype(jnp.float32)
    phase_angle = (
        2.0 * jnp.pi * (l_coord * coords[:, 0] + m_coord * coords[:, 1] + w_term * coords[:, 2])
    )
    cosine = jnp.cos(phase_angle)
    sine_part = jnp.sin(phase_angle)
    real_part = vis_pair[:, 0].astype(jnp.float32)
    imag_part = vis_pair[:, 1].astype(jnp.float32)
    rot_real = (real_part * cosine + imag_part * sine_part).astype(jnp.bfloat16)
    rot_imag = (imag_part * cosine - real_part * sine_part).astype(jnp.bfloat16)
    return (rot_real, rot_imag)


def stack_kernels(kernels):
    kern_real = kernels[:, 0]
    kern_imag = kernels[:, 1]
    upper_rows = jnp.concatenate([kern_real, kern_imag], axis=2)
    lower_rows = jnp.concatenate([-kern_imag, kern_real], axis=2)
    stacked_rows = jnp.concatenate([upper_rows, lower_rows], axis=0)
    return stacked_rows.reshape(-1, stacked_rows.shape[2])


def grid_tiles(rot_real, rot_imag, planes, stacked, plane_count):
    plane_select = (planes[:, None] == jnp.arange(plane_count)[None, :]).astype(jnp.bfloat16)
    spread = jnp.concatenate(
        [
            rot_real[:, None, :] * plane_select[:, :, None],
            rot_imag[:, None, :] * plane_select[:, :, None],
        ],
        axis=1,
    )
    spread = spread.reshape(spread.shape[0], -1)
    return jnp.dot(spread, stacked, preferred_element_type=jnp.float32).astype(jnp.bfloat16)


def shards(visibilities, uvw, facet_of, plane_of, cell_of, kernels, centers):
    peer_count = lax.axis_size("facet")
    tile_count = visibilities.shape[1]
    capacity = 4 * tile_count // peer_count
    total_slots = peer_count * capacity
    vis_pair = visibilities[0]
    coords = uvw[0]
    target = facet_of[0, :, 0]
    planes = plane_of[0]
    tile_cells = cell_of[0]
    plane_count = kernels.shape[0]
    stacked = stack_kernels(kernels)
    dest_hits = (target[:, None] == jnp.arange(peer_count)[None, :]).astype(jnp.int32)
    before = jnp.cumsum(dest_hits, axis=0) - dest_hits
    within_rank = jnp.sum(before * dest_hits, axis=1)
    slot_index = target * capacity + within_rank
    chosen = (target[:, None] == jnp.arange(centers.shape[0])[None, :]).astype(jnp.float32)
    sky_rows = jnp.sum(chosen[:, :, None] * centers[None, :, :], axis=1)
    rot_real, rot_imag = rotate_tiles(vis_pair, coords, sky_rows)
    own_patches = grid_tiles(rot_real, rot_imag, planes, stacked, plane_count)
    patch_buffer = (
        jnp.zeros((total_slots, own_patches.shape[1]), jnp.bfloat16).at[slot_index].set(own_patches)
    )
    cell_buffer = jnp.zeros((total_slots,), jnp.int32).at[slot_index].set(tile_cells)
    patches, slot_cells = (
        lax.all_to_all(
            patch_buffer.reshape(peer_count, capacity, -1),
            "facet",
            split_axis=0,
            concat_axis=0,
            tiled=True,
        ),
        lax.all_to_all(
            cell_buffer.reshape(peer_count, capacity),
            "facet",
            split_axis=0,
            concat_axis=0,
            tiled=True,
        ),
    )
    patches = patches.reshape(-1, patches.shape[-1])
    slot_cells = slot_cells.reshape(-1)
    nblocks = GRID // PSIDE
    ncells = nblocks * nblocks
    placing = (slot_cells[None, :] == jnp.arange(ncells)[:, None]).astype(jnp.bfloat16)
    blocks = jnp.dot(placing, patches, preferred_element_type=jnp.float32).astype(jnp.bfloat16)
    uv_grid = (
        blocks.reshape(nblocks, nblocks, 2, PSIDE, PSIDE)
        .transpose(2, 0, 3, 1, 4)
        .reshape(2 * GRID, GRID)
    )
    table_real, table_imag = dft_tables(GRID)
    table_both = jnp.concatenate([table_real, table_imag], axis=1)
    product = jnp.dot(uv_grid, table_both, preferred_element_type=jnp.float32)
    half_real = product[:GRID, :GRID] - product[GRID:, GRID:]
    half_imag = product[:GRID, GRID:] + product[GRID:, :GRID]
    partial_value = jnp.stack([half_real, half_imag]).astype(jnp.bfloat16)
    summed = lax.psum_scatter(
        partial_value.astype(jnp.float32).astype(jnp.bfloat16),
        "freq",
        scatter_dimension=2,
        tiled=True,
    )
    right_side = jnp.concatenate([summed[0], -summed[1]], axis=0)
    facet_image = jnp.dot(table_both, right_side, preferred_element_type=jnp.float32)
    return facet_image[None]


def gather_kernel(peers, sizes, centers_hbm, facet_hbm, plane_hbm, cell_hbm, vis_hbm, uvw_hbm, kern_hbm, *rest):
    out_refs = rest[: len(sizes)]
    centers_ref, facet_ref, plane_ref, cell_ref, vis_ref, uvw_ref, kern_ref, parts_ref, rows_ref, sems = rest[len(sizes) :]
    planes, _, depth, cells = kern_ref.shape
    tiles = facet_ref.shape[1]
    half = tiles // 2
    groups_of_lanes = depth // LANES
    rows_of = [slice(h * half, (h + 1) * half) for h in range(2)]
    vis_rows = vis_ref.shape[0] // 2
    transfers = [(centers_hbm, centers_ref), (facet_hbm, facet_ref), (plane_hbm, plane_ref)]
    for h in range(2):
        part = slice(h * vis_rows, (h + 1) * vis_rows)
        transfers += [(vis_hbm.at[part], vis_ref.at[part]), (uvw_hbm.at[:, rows_of[h]], uvw_ref.at[:, rows_of[h]])]
    transfers += [(cell_hbm, cell_ref)] + [(kern_hbm.at[p], kern_ref.at[p]) for p in range(planes)]
    copies = [pltpu.make_async_copy(source, target, sems.at[i]) for i, (source, target) in enumerate(transfers)]
    for copy in copies:
        copy.start()
    for copy in copies[:3]:
        copy.wait()
    facet = facet_ref[...]
    l_row = jnp.zeros(facet.shape, jnp.float32)
    m_row = jnp.zeros(facet.shape, jnp.float32)
    for f in range(peers):
        hit = facet == f
        l_row = jnp.where(hit, centers_ref[0:1, f : f + 1], l_row)
        m_row = jnp.where(hit, centers_ref[1:2, f : f + 1], m_row)
    d_row = jnp.sqrt(1.0 - l_row * l_row - m_row * m_row) - 1.0
    plane_row = plane_ref[...].astype(jnp.float32)
    zero_row = jnp.zeros_like(l_row)
    columns = jnp.concatenate([l_row, m_row, d_row, plane_row] + [zero_row] * 4, axis=0).T

    near, capacity, few, slots = peers // 2, sizes[0], sizes[peers // 2], LANES * len(sizes)
    relative = facet ^ lax.axis_index("facet")
    lanes = lax.broadcasted_iota(jnp.int32, (tiles, tiles), 1)
    earlier = (lax.broadcasted_iota(jnp.int32, (tiles, tiles), 0) < lanes).astype(jnp.float32).astype(jnp.bfloat16)
    facets = lax.broadcasted_iota(jnp.int32, (peers, tiles), 0)
    hits = facets == relative
    before = jnp.dot(hits.astype(jnp.float32).astype(jnp.bfloat16), earlier, preferred_element_type=jnp.float32)
    rank = jnp.sum(jnp.where(hits, before, 0.0), axis=0, keepdims=True).astype(jnp.int32)
    passed = jnp.where(facets >= near, jnp.maximum(before - few, 0.0), 0.0)
    passed = jnp.sum(passed, axis=0, keepdims=True).astype(jnp.int32)
    slot = jnp.where((relative < near) | (rank < few), relative * capacity + rank, peers * capacity + passed)

    patches = []
    for h in range(2):
        tile_rows = rows_of[h]
        for copy in copies[3:5] if h == 0 else copies[5:]:
            copy.wait()
        part = slice(h * vis_rows, (h + 1) * vis_rows)
        parts_ref[part] = vis_ref[part].astype(jnp.float32)
        l_col, m_col, d_col = (jnp.broadcast_to(columns[tile_rows, i : i + 1], (half, LANES)) for i in range(3))
        for j in range(groups_of_lanes):
            lane = slice(j * LANES, (j + 1) * LANES)
            u, v, w = (uvw_ref[i, tile_rows, lane].astype(jnp.float32) for i in range(3))
            cosine, sine = cos_sin_turns(l_col * u + m_col * v + d_col * w)
            first = 2 * (h * half * groups_of_lanes + j)
            real = parts_ref[pl.ds(first, half, stride=2 * groups_of_lanes), :]
            imag = parts_ref[pl.ds(first + 1, half, stride=2 * groups_of_lanes), :]
            rot_real = (real * cosine + imag * sine).astype(jnp.bfloat16)
            rot_imag = (imag * cosine - real * sine).astype(jnp.bfloat16)
            right = slice(depth + j * LANES, depth + (j + 1) * LANES)
            rows_ref[h, :half, lane] = rot_real
            rows_ref[h, :half, right] = -rot_imag
            rows_ref[h, half:, lane] = rot_imag
            rows_ref[h, half:, right] = rot_real
    for h in range(2):
        plane_two = jnp.concatenate([columns[rows_of[h], 3:4]] * 2, axis=0)
        total = None
        for p in range(planes):
            mask = (plane_two == float(p)).astype(jnp.float32).astype(jnp.bfloat16)
            product = jnp.dot(
                rows_ref[h] * mask, kern_ref[p].reshape(2 * depth, cells), preferred_element_type=jnp.float32
            )
            total = product if total is None else total + product
        patches.append(jnp.concatenate([total[:half], total[half:]], axis=1).astype(jnp.bfloat16))
    patches = jnp.concatenate(patches, axis=0)
    placing = lax.broadcasted_iota(jnp.int32, (slots, tiles), 0) == slot
    placing = placing.astype(jnp.float32).astype(jnp.bfloat16)
    placed = jnp.dot(placing, patches, preferred_element_type=jnp.float32).astype(jnp.bfloat16)
    cell = cell_ref[...].astype(jnp.float32)
    block_u = jnp.floor(cell * (1.0 / NBLK))
    block_v = cell - block_u * NBLK
    labels = [block_u, block_v, facet.astype(jnp.float32)] + [zero_row] * (SUBLANES - 3)
    labels = jnp.concatenate(labels, axis=0).astype(jnp.bfloat16)
    labels = lax.dot_general(labels, placing, (((1,), (1,)), ((), ())), preferred_element_type=jnp.float32)
    labels = labels.astype(jnp.bfloat16)
    for i, (ref, size) in enumerate(zip(out_refs, sizes)):
        start = i * LANES
        for j in range(2 * cells // LANES):
            ref[j * size : (j + 1) * size, :] = placed[start : start + size, j * LANES : (j + 1) * LANES]
        ref[2 * cells // LANES * size :, :] = labels[:, start : start + LANES]


def padded(sizes):
    return -(-sum(sizes) // LANES) * LANES


def load_patches(in_refs, sizes, patch_buf):
    cells = PSIDE * PSIDE
    half_tiles = cells // LANES
    slots = padded(sizes)
    start = 0
    for ref, size in zip(in_refs, sizes):
        rows = slice(start, start + size)
        below = slice(slots + start, slots + start + size)
        for j in range(half_tiles):
            left = slice(j * LANES, (j + 1) * LANES)
            right = slice(cells + j * LANES, cells + (j + 1) * LANES)
            real = ref[j * size : (j + 1) * size, :]
            imag = ref[(half_tiles + j) * size : (half_tiles + j + 1) * size, :]
            patch_buf[rows, left] = real
            patch_buf[rows, right] = imag
            patch_buf[below, left] = -imag
            patch_buf[below, right] = real
        start += size
    if start < slots:
        for first in (0, slots):
            patch_buf[first + start : first + slots, :] = jnp.zeros((slots - start, 2 * cells), jnp.bfloat16)


def cell_phases(in_refs, sizes, direct):
    slots = padded(sizes)
    labels = [jnp.zeros((SUBLANES, LANES), jnp.float32) for _ in range(slots // LANES)]
    lane = lax.broadcasted_iota(jnp.int32, (SUBLANES, LANES), 1)
    start = 0
    for ref, size in zip(in_refs, sizes):
        here = ref[2 * PSIDE * PSIDE // LANES * size :, :].astype(jnp.float32)
        tile, shift = divmod(start, LANES)
        if shift:
            here = pltpu.roll(here, shift, 1)
            if shift + size > LANES:
                labels[tile + 1] = jnp.where(lane < shift, here, 0.0)
            here = jnp.where(lane >= shift, here, 0.0)
        labels[tile] = labels[tile] + here
        start += size
    labels = jnp.concatenate(labels, axis=1)
    lane = lax.broadcasted_iota(jnp.int32, (1, slots), 1)
    mine = labels[2:3] == lax.axis_index("facet").astype(jnp.float32)
    mine = jnp.where(mine | (lane < sum(sizes[:direct])), 1.0, 0.0)
    index = lax.broadcasted_iota(jnp.int32, (NBLK, slots), 0).astype(jnp.float32) * (1.0 / NBLK)
    cos_u, sin_u = cos_sin_turns(index * labels[0:1])
    return (cos_u * mine, sin_u * mine) + cos_sin_turns(index * labels[1:2])


def fill_phases(buf, rows_of, phases):
    cos_u, sin_u, cos_v, sin_v = phases
    slots = cos_v.shape[1]
    for i, j in enumerate(rows_of):
        cu, su = cos_u[j : j + 1], sin_u[j : j + 1]
        rows = slice(i * NBLK, (i + 1) * NBLK)
        buf[rows, :slots] = (cu * cos_v - su * sin_v).astype(jnp.bfloat16)
        buf[rows, slots:] = (cu * sin_v + su * cos_v).astype(jnp.bfloat16)


PER_CHUNK = 8


def spectrum_kernel(sizes, direct, *rest):
    count = len(sizes)
    in_refs, (out_ref, turn_ref, phases_buf, patch_buf) = rest[:count], rest[count:]
    load_patches(in_refs, sizes, patch_buf)
    phases = cell_phases(in_refs, sizes, direct)
    width = PER_CHUNK * NBLK
    for chunk in range(NBLK // PER_CHUNK):
        buf = phases_buf.at[chunk % 2]
        fill_phases(buf, range(chunk * PER_CHUNK, (chunk + 1) * PER_CHUNK), phases)
        out_ref[chunk * width : (chunk + 1) * width, :] = jnp.dot(
            buf[...], patch_buf[...], preferred_element_type=jnp.float32
        )

    cells = PSIDE * PSIDE
    lane = lax.broadcasted_iota(jnp.int32, (NBLK, cells), 1)
    row = lax.broadcasted_iota(jnp.int32, (NBLK, cells), 0)
    cos_u, sin_u = cos_sin_turns((row * (lane // PSIDE)).astype(jnp.float32) * (1.0 / GRID))
    cos_v, sin_v = cos_sin_turns((row * (lane % PSIDE)).astype(jnp.float32) * (1.0 / GRID))
    for j in range(NBLK):
        rows = slice(j * NBLK, (j + 1) * NBLK)
        cu, su = cos_u[j : j + 1], sin_u[j : j + 1]
        turn_ref[rows, :cells] = cu * cos_v - su * sin_v
        turn_ref[rows, cells:] = cu * sin_v + su * cos_v


def image_kernel(sizes, direct, groups, table_ref, early_ref, turn_ref, *rest):
    count = len(sizes)
    in_refs, out_refs = rest[:count], rest[count : count + groups]
    phases_buf, patch_buf, table_buf = rest[count + groups :]
    cells = PSIDE * PSIDE
    share = cells // groups
    load_patches(in_refs, sizes, patch_buf)
    for s in range(groups):
        start = pl.multiple_of((lax.axis_index("freq") ^ s) * share, share)
        table_buf[s * share : (s + 1) * share, :] = table_ref[pl.ds(start, share), :]
    phases = cell_phases(in_refs, sizes, direct)

    width = PER_CHUNK * NBLK
    for chunk in range(NBLK // PER_CHUNK):
        buf = phases_buf.at[chunk % 2]
        fill_phases(buf, range(chunk * PER_CHUNK, (chunk + 1) * PER_CHUNK), phases)
        here = slice(chunk * width, (chunk + 1) * width)
        spectrum = early_ref[here, :] + jnp.dot(buf[...], patch_buf[...], preferred_element_type=jnp.float32)
        real, imag = spectrum[:, :cells], spectrum[:, cells:]
        cosine, sine = turn_ref[here, :cells], turn_ref[here, cells:]
        turned = jnp.concatenate([real * cosine - imag * sine, real * sine + imag * cosine], axis=1).astype(jnp.bfloat16)
        image = lax.dot_general(
            table_buf[...], turned, (((1,), (1,)), ((), ())), preferred_element_type=jnp.float32
        ).astype(jnp.bfloat16)
        for s in range(groups):
            out_refs[s][:, here] = image[s * share : (s + 1) * share]


def finish_kernel(groups, *refs):
    in_refs, out_ref = refs[:groups], refs[groups]
    columns = PSIDE // groups
    per_tile = LANES // NBLK
    lane = lax.broadcasted_iota(jnp.int32, (PSIDE, LANES), 1) // NBLK
    for tile in range(NBLK // per_tile):
        lanes = slice(tile * LANES, (tile + 1) * LANES)
        total = in_refs[0][:, lanes].astype(jnp.float32)
        for ref in in_refs[1:]:
            total = total + ref[:, lanes].astype(jnp.float32)
        for i in range(per_tile):
            value = jnp.zeros((PSIDE, LANES), jnp.float32)
            for kq in range(columns):
                piece = total[kq * PSIDE : (kq + 1) * PSIDE]
                shift = (kq - i) * NBLK % LANES
                piece = pltpu.roll(piece, shift, 1) if shift else piece
                value = jnp.where(lane == kq, piece, value)
            out_ref[pl.ds(tile * per_tile + i, PSIDE, stride=NBLK), :] = value


def patch_table():
    index = np.arange(PSIDE)
    kq, jq = (a.reshape(-1, 1) for a in np.meshgrid(index, index, indexing="ij"))
    pu, pv = (a.reshape(1, -1) for a in np.meshgrid(index, index, indexing="ij"))
    angle = 2.0 * np.pi * ((pu * jq + pv * kq) % PSIDE) / PSIDE
    return np.concatenate([np.cos(angle), -np.sin(angle)], axis=1) / GRID


def swap(piece, axis, distance):
    count = lax.axis_size(axis)
    return lax.ppermute(piece, axis, [(i, i ^ distance) for i in range(count)])


def overflow_slots(tiles, capacity, few, facets):
    full = min(facets, tiles // capacity)
    most = full * (capacity - few)
    if full < facets:
        most += max(0, tiles - full * capacity - few)
    return -(-most // 16) * 16


def packed_shards(visibilities, uvw, facet_of, plane_of, cell_of, kernels, centers):
    peers, groups = lax.axis_size("facet"), lax.axis_size("freq")
    tiles = visibilities.shape[1]
    capacity = 4 * tiles // peers
    planes, _, depth, cells = kernels.shape
    near = peers // 2
    few = 5 * capacity // 8
    sizes = [capacity] * near + [few] * near + [overflow_slots(tiles, capacity, few, near)]
    payloads = [jax.ShapeDtypeStruct((2 * cells // LANES * size + SUBLANES, LANES), jnp.bfloat16) for size in sizes]
    lanes = depth // LANES
    vis_rows = visibilities[0].reshape(tiles, 2, lanes, LANES).transpose(0, 2, 1, 3).reshape(-1, LANES)
    operands = (
        centers.T,
        facet_of.reshape(1, tiles),
        plane_of,
        cell_of,
        vis_rows,
        uvw[0].transpose(1, 0, 2),
        kernels,
    )
    pieces = pl.pallas_call(
        functools.partial(gather_kernel, peers, sizes),
        out_shape=payloads,
        in_specs=[HBM] * len(operands),
        out_specs=[VMEM] * len(sizes),
        scratch_shapes=[pltpu.VMEM(operand.shape, operand.dtype) for operand in operands]
        + [
            pltpu.VMEM(vis_rows.shape, jnp.float32),
            pltpu.VMEM((2, tiles, 2 * depth), jnp.bfloat16),
            pltpu.SemaphoreType.DMA((len(operands) + 1 + planes,)),
        ],
        compiler_params=compiler_params(40),
        name="gather",
    )(*(pltpu.with_memory_space_constraint(operand, pltpu.HBM) for operand in operands))
    overflow = [swap(pieces[peers], "facet", near)]
    received = [pieces[0]] + [swap(pieces[s], "facet", s) for s in range(1, peers)]
    overflow += [swap(overflow[0], "facet", s) for s in range(1, near)]
    early, late = received[:near] + overflow[:1], received[near:] + overflow[1:]
    early_sizes, late_sizes = sizes[:near] + sizes[peers:], sizes[near:peers] + sizes[peers:] * (near - 1)
    share = cells // groups
    points = NBLK * NBLK

    def buffers_and_cost(slots):
        buffers = [
            pltpu.VMEM((2, PER_CHUNK * NBLK, 2 * slots), jnp.bfloat16),
            pltpu.VMEM((2 * slots, 2 * cells), jnp.bfloat16),
        ]
        return buffers, pl.CostEstimate(flops=8 * points * slots * cells, bytes_accessed=4 << 20, transcendentals=0)

    buffers, cost = buffers_and_cost(padded(early_sizes))
    spectrum, turns = pl.pallas_call(
        functools.partial(spectrum_kernel, early_sizes, near),
        out_shape=[jax.ShapeDtypeStruct((points, 2 * cells), jnp.float32)] * 2,
        in_specs=[VMEM] * len(early),
        out_specs=[VMEM] * 2,
        scratch_shapes=buffers,
        compiler_params=compiler_params(40),
        cost_estimate=cost,
        name="spectrum",
    )(*early)
    buffers, cost = buffers_and_cost(padded(late_sizes))
    image = jax.ShapeDtypeStruct((share, points), jnp.bfloat16)
    images = pl.pallas_call(
        functools.partial(image_kernel, late_sizes, near, groups),
        out_shape=[image] * groups,
        in_specs=[VMEM] * (3 + len(late)),
        out_specs=[VMEM] * groups,
        scratch_shapes=buffers + [pltpu.VMEM((cells, 2 * cells), jnp.bfloat16)],
        compiler_params=compiler_params(40),
        cost_estimate=cost,
        name="image",
    )(jnp.asarray(patch_table(), jnp.bfloat16), spectrum, turns, *late)
    summed = [images[0]] + [swap(images[s], "freq", s) for s in range(1, groups)]
    facet_image = pl.pallas_call(
        functools.partial(finish_kernel, groups),
        out_shape=jax.ShapeDtypeStruct((GRID, GRID // groups), jnp.float32),
        in_specs=[VMEM] * groups,
        out_specs=VMEM,
        compiler_params=compiler_params(16),
        name="finish",
    )(*summed)
    return facet_image[None]


def solution(mesh):
    in_specs = (
        P("freq", "facet", None, None),
        P("freq", "facet", None, None),
        P("freq", "facet", None),
        P("freq", "facet"),
        P("freq", "facet"),
        P(),
        P(),
    )
    out_specs = P("facet", None, "freq")

    def body(*args):
        peers, groups = lax.axis_size("facet"), lax.axis_size("freq")
        capacity = 4 * args[0].shape[1] // peers
        powers = peers & (peers - 1) == 0 and groups & (groups - 1) == 0
        packed = capacity == LANES and powers and GRID // groups == LANES
        return (packed_shards if packed else shards)(*args)

    return jax.shard_map(body, mesh=mesh, in_specs=in_specs, out_specs=out_specs, check_vma=False)
```

```python
import functools

import jax
import jax.numpy as jnp
import numpy as np
from jax import lax
from jax.experimental import pallas as pl
from jax.experimental.pallas import tpu as pltpu
from jax.sharding import PartitionSpec as P


GRID = 512
PSIDE = 16
NBLK = GRID // PSIDE
LANES = 128
SUBLANES = 8

SIN_POLY = (4.442882919124345, -7.30824568650904, 3.6063542184326933, -0.8461116503732697, 0.10982451642490525)
COS_POLY = (1.4142134962552284, -6.978850948563788, 5.73946037690675, -1.8835579059841707, 0.3106880275217573)


def horner(square, coefficients):
    value = coefficients[-1] * square + coefficients[-2]
    for coefficient in coefficients[-3::-1]:
        value = value * square + coefficient
    return value


def cos_sin_turns(turns):
    rest = turns - jnp.round(turns)
    square = rest * rest
    sine = rest * horner(square, SIN_POLY)
    return (1.0 - sine * sine, sine * horner(square, COS_POLY))


def compiler_params(mebibytes):
    return pltpu.CompilerParams(vmem_limit_bytes=mebibytes << 20)


VMEM = pl.BlockSpec(memory_space=pltpu.VMEM)
HBM = pl.BlockSpec(memory_space=pltpu.HBM)


def dft_tables(length):
    indices = jnp.arange(length, dtype=jnp.int32)
    products_mod = indices[:, None] * indices[None, :] % length
    angle_table = products_mod.astype(jnp.float32) * (2.0 * jnp.pi / length)
    norm_scale = 1.0 / jnp.sqrt(jnp.float32(length))
    table_real = (jnp.cos(angle_table) * norm_scale).astype(jnp.bfloat16)
    table_imag = (jnp.sin(angle_table) * norm_scale).astype(jnp.bfloat16)
    return (table_real, table_imag)


def rotate_tiles(vis_pair, coords, sky_pos):
    l_coord = sky_pos[:, 0:1]
    m_coord = sky_pos[:, 1:2]
    w_term = jnp.sqrt(1.0 - l_coord * l_coord - m_coord * m_coord) - 1.0
    coords = coords.astype(jnp.float32)
    phase_angle = (
        2.0 * jnp.pi * (l_coord * coords[:, 0] + m_coord * coords[:, 1] + w_term * coords[:, 2])
    )
    cosine = jnp.cos(phase_angle)
    sine_part = jnp.sin(phase_angle)
    real_part = vis_pair[:, 0].astype(jnp.float32)
    imag_part = vis_pair[:, 1].astype(jnp.float32)
    rot_real = (real_part * cosine + imag_part * sine_part).astype(jnp.bfloat16)
    rot_imag = (imag_part * cosine - real_part * sine_part).astype(jnp.bfloat16)
    return (rot_real, rot_imag)


def stack_kernels(kernels):
    kern_real = kernels[:, 0]
    kern_imag = kernels[:, 1]
    upper_rows = jnp.concatenate([kern_real, kern_imag], axis=2)
    lower_rows = jnp.concatenate([-kern_imag, kern_real], axis=2)
    stacked_rows = jnp.concatenate([upper_rows, lower_rows], axis=0)
    return stacked_rows.reshape(-1, stacked_rows.shape[2])


def grid_tiles(rot_real, rot_imag, planes, stacked, plane_count):
    plane_select = (planes[:, None] == jnp.arange(plane_count)[None, :]).astype(jnp.bfloat16)
    spread = jnp.concatenate(
        [
            rot_real[:, None, :] * plane_select[:, :, None],
            rot_imag[:, None, :] * plane_select[:, :, None],
        ],
        axis=1,
    )
    spread = spread.reshape(spread.shape[0], -1)
    return jnp.dot(spread, stacked, preferred_element_type=jnp.float32).astype(jnp.bfloat16)


def shards(visibilities, uvw, facet_of, plane_of, cell_of, kernels, centers):
    peer_count = lax.axis_size("facet")
    tile_count = visibilities.shape[1]
    capacity = 4 * tile_count // peer_count
    total_slots = peer_count * capacity
    vis_pair = visibilities[0]
    coords = uvw[0]
    target = facet_of[0, :, 0]
    planes = plane_of[0]
    tile_cells = cell_of[0]
    plane_count = kernels.shape[0]
    stacked = stack_kernels(kernels)
    dest_hits = (target[:, None] == jnp.arange(peer_count)[None, :]).astype(jnp.int32)
    before = jnp.cumsum(dest_hits, axis=0) - dest_hits
    within_rank = jnp.sum(before * dest_hits, axis=1)
    slot_index = target * capacity + within_rank
    chosen = (target[:, None] == jnp.arange(centers.shape[0])[None, :]).astype(jnp.float32)
    sky_rows = jnp.sum(chosen[:, :, None] * centers[None, :, :], axis=1)
    rot_real, rot_imag = rotate_tiles(vis_pair, coords, sky_rows)
    own_patches = grid_tiles(rot_real, rot_imag, planes, stacked, plane_count)
    patch_buffer = (
        jnp.zeros((total_slots, own_patches.shape[1]), jnp.bfloat16).at[slot_index].set(own_patches)
    )
    cell_buffer = jnp.zeros((total_slots,), jnp.int32).at[slot_index].set(tile_cells)
    patches, slot_cells = (
        lax.all_to_all(
            patch_buffer.reshape(peer_count, capacity, -1),
            "facet",
            split_axis=0,
            concat_axis=0,
            tiled=True,
        ),
        lax.all_to_all(
            cell_buffer.reshape(peer_count, capacity),
            "facet",
            split_axis=0,
            concat_axis=0,
            tiled=True,
        ),
    )
    patches = patches.reshape(-1, patches.shape[-1])
    slot_cells = slot_cells.reshape(-1)
    nblocks = GRID // PSIDE
    ncells = nblocks * nblocks
    placing = (slot_cells[None, :] == jnp.arange(ncells)[:, None]).astype(jnp.bfloat16)
    blocks = jnp.dot(placing, patches, preferred_element_type=jnp.float32).astype(jnp.bfloat16)
    uv_grid = (
        blocks.reshape(nblocks, nblocks, 2, PSIDE, PSIDE)
        .transpose(2, 0, 3, 1, 4)
        .reshape(2 * GRID, GRID)
    )
    table_real, table_imag = dft_tables(GRID)
    table_both = jnp.concatenate([table_real, table_imag], axis=1)
    product = jnp.dot(uv_grid, table_both, preferred_element_type=jnp.float32)
    half_real = product[:GRID, :GRID] - product[GRID:, GRID:]
    half_imag = product[:GRID, GRID:] + product[GRID:, :GRID]
    partial_value = jnp.stack([half_real, half_imag]).astype(jnp.bfloat16)
    summed = lax.psum_scatter(
        partial_value.astype(jnp.float32).astype(jnp.bfloat16),
        "freq",
        scatter_dimension=2,
        tiled=True,
    )
    right_side = jnp.concatenate([summed[0], -summed[1]], axis=0)
    facet_image = jnp.dot(table_both, right_side, preferred_element_type=jnp.float32)
    return facet_image[None]


def gather_kernel(peers, sizes, centers_hbm, facet_hbm, plane_hbm, cell_hbm, vis_hbm, uvw_hbm, kern_hbm, *rest):
    out_refs = rest[: len(sizes)]
    centers_ref, facet_ref, plane_ref, cell_ref, vis_ref, uvw_ref, kern_ref, parts_ref, rows_ref, sems = rest[len(sizes) :]
    planes, _, depth, cells = kern_ref.shape
    tiles = facet_ref.shape[1]
    half = tiles // 2
    groups_of_lanes = depth // LANES
    rows_of = [slice(h * half, (h + 1) * half) for h in range(2)]
    vis_rows = vis_ref.shape[0] // 2
    transfers = [(centers_hbm, centers_ref), (facet_hbm, facet_ref), (plane_hbm, plane_ref)]
    for h in range(2):
        part = slice(h * vis_rows, (h + 1) * vis_rows)
        transfers += [(vis_hbm.at[part], vis_ref.at[part]), (uvw_hbm.at[:, rows_of[h]], uvw_ref.at[:, rows_of[h]])]
    transfers += [(cell_hbm, cell_ref)] + [(kern_hbm.at[p], kern_ref.at[p]) for p in range(planes)]
    copies = [pltpu.make_async_copy(source, target, sems.at[i]) for i, (source, target) in enumerate(transfers)]
    for copy in copies:
        copy.start()
    for copy in copies[:3]:
        copy.wait()
    facet = facet_ref[...]
    l_row = jnp.zeros(facet.shape, jnp.float32)
    m_row = jnp.zeros(facet.shape, jnp.float32)
    for f in range(peers):
        hit = facet == f
        l_row = jnp.where(hit, centers_ref[0:1, f : f + 1], l_row)
        m_row = jnp.where(hit, centers_ref[1:2, f : f + 1], m_row)
    d_row = jnp.sqrt(1.0 - l_row * l_row - m_row * m_row) - 1.0
    plane_row = plane_ref[...].astype(jnp.float32)
    zero_row = jnp.zeros_like(l_row)
    columns = jnp.concatenate([l_row, m_row, d_row, plane_row] + [zero_row] * 4, axis=0).T

    near, capacity, few, slots = peers // 2, sizes[0], sizes[peers // 2], LANES * len(sizes)
    relative = facet ^ lax.axis_index("facet")
    lanes = lax.broadcasted_iota(jnp.int32, (tiles, tiles), 1)
    earlier = (lax.broadcasted_iota(jnp.int32, (tiles, tiles), 0) < lanes).astype(jnp.float32).astype(jnp.bfloat16)
    facets = lax.broadcasted_iota(jnp.int32, (peers, tiles), 0)
    hits = facets == relative
    before = jnp.dot(hits.astype(jnp.float32).astype(jnp.bfloat16), earlier, preferred_element_type=jnp.float32)
    rank = jnp.sum(jnp.where(hits, before, 0.0), axis=0, keepdims=True).astype(jnp.int32)
    passed = jnp.where(facets >= near, jnp.maximum(before - few, 0.0), 0.0)
    passed = jnp.sum(passed, axis=0, keepdims=True).astype(jnp.int32)
    slot = jnp.where((relative < near) | (rank < few), relative * capacity + rank, peers * capacity + passed)

    patches = []
    for h in range(2):
        tile_rows = rows_of[h]
        for copy in copies[3:5] if h == 0 else copies[5:]:
            copy.wait()
        part = slice(h * vis_rows, (h + 1) * vis_rows)
        parts_ref[part] = vis_ref[part].astype(jnp.float32)
        l_col, m_col, d_col = (jnp.broadcast_to(columns[tile_rows, i : i + 1], (half, LANES)) for i in range(3))
        for j in range(groups_of_lanes):
            lane = slice(j * LANES, (j + 1) * LANES)
            u, v, w = (uvw_ref[i, tile_rows, lane].astype(jnp.float32) for i in range(3))
            cosine, sine = cos_sin_turns(l_col * u + m_col * v + d_col * w)
            first = 2 * (h * half * groups_of_lanes + j)
            real = parts_ref[pl.ds(first, half, stride=2 * groups_of_lanes), :]
            imag = parts_ref[pl.ds(first + 1, half, stride=2 * groups_of_lanes), :]
            rot_real = (real * cosine + imag * sine).astype(jnp.bfloat16)
            rot_imag = (imag * cosine - real * sine).astype(jnp.bfloat16)
            right = slice(depth + j * LANES, depth + (j + 1) * LANES)
            rows_ref[h, :half, lane] = rot_real
            rows_ref[h, :half, right] = -rot_imag
            rows_ref[h, half:, lane] = rot_imag
            rows_ref[h, half:, right] = rot_real
    for h in range(2):
        plane_two = jnp.concatenate([columns[rows_of[h], 3:4]] * 2, axis=0)
        total = None
        for p in range(planes):
            mask = (plane_two == float(p)).astype(jnp.float32).astype(jnp.bfloat16)
            product = jnp.dot(
                rows_ref[h] * mask, kern_ref[p].reshape(2 * depth, cells), preferred_element_type=jnp.float32
            )
            total = product if total is None else total + product
        patches.append(jnp.concatenate([total[:half], total[half:]], axis=1).astype(jnp.bfloat16))
    patches = jnp.concatenate(patches, axis=0)
    placing = lax.broadcasted_iota(jnp.int32, (slots, tiles), 0) == slot
    placing = placing.astype(jnp.float32).astype(jnp.bfloat16)
    placed = jnp.dot(placing, patches, preferred_element_type=jnp.float32).astype(jnp.bfloat16)
    cell = cell_ref[...].astype(jnp.float32)
    block_u = jnp.floor(cell * (1.0 / NBLK))
    block_v = cell - block_u * NBLK
    labels = [block_u, block_v, facet.astype(jnp.float32)] + [zero_row] * (SUBLANES - 3)
    labels = jnp.concatenate(labels, axis=0).astype(jnp.bfloat16)
    labels = lax.dot_general(labels, placing, (((1,), (1,)), ((), ())), preferred_element_type=jnp.float32)
    labels = labels.astype(jnp.bfloat16)
    for i, (ref, size) in enumerate(zip(out_refs, sizes)):
        start = i * LANES
        for j in range(2 * cells // LANES):
            ref[j * size : (j + 1) * size, :] = placed[start : start + size, j * LANES : (j + 1) * LANES]
        ref[2 * cells // LANES * size :, :] = labels[:, start : start + LANES]


def padded(sizes):
    return -(-sum(sizes) // LANES) * LANES


def load_patches(in_refs, sizes, patch_buf):
    cells = PSIDE * PSIDE
    half_tiles = cells // LANES
    slots = padded(sizes)
    start = 0
    for ref, size in zip(in_refs, sizes):
        rows = slice(start, start + size)
        below = slice(slots + start, slots + start + size)
        for j in range(half_tiles):
            left = slice(j * LANES, (j + 1) * LANES)
            right = slice(cells + j * LANES, cells + (j + 1) * LANES)
            real = ref[j * size : (j + 1) * size, :]
            imag = ref[(half_tiles + j) * size : (half_tiles + j + 1) * size, :]
            patch_buf[rows, left] = real
            patch_buf[rows, right] = imag
            patch_buf[below, left] = -imag
            patch_buf[below, right] = real
        start += size
    if start < slots:
        for first in (0, slots):
            patch_buf[first + start : first + slots, :] = jnp.zeros((slots - start, 2 * cells), jnp.bfloat16)


def cell_phases(in_refs, sizes, direct):
    slots = padded(sizes)
    labels = [jnp.zeros((SUBLANES, LANES), jnp.float32) for _ in range(slots // LANES)]
    lane = lax.broadcasted_iota(jnp.int32, (SUBLANES, LANES), 1)
    start = 0
    for ref, size in zip(in_refs, sizes):
        here = ref[2 * PSIDE * PSIDE // LANES * size :, :].astype(jnp.float32)
        tile, shift = divmod(start, LANES)
        if shift:
            here = pltpu.roll(here, shift, 1)
            if shift + size > LANES:
                labels[tile + 1] = jnp.where(lane < shift, here, 0.0)
            here = jnp.where(lane >= shift, here, 0.0)
        labels[tile] = labels[tile] + here
        start += size
    labels = jnp.concatenate(labels, axis=1)
    lane = lax.broadcasted_iota(jnp.int32, (1, slots), 1)
    mine = labels[2:3] == lax.axis_index("facet").astype(jnp.float32)
    mine = jnp.where(mine | (lane < sum(sizes[:direct])), 1.0, 0.0)
    index = lax.broadcasted_iota(jnp.int32, (NBLK, slots), 0).astype(jnp.float32) * (1.0 / NBLK)
    cos_u, sin_u = cos_sin_turns(index * labels[0:1])
    return (cos_u * mine, sin_u * mine) + cos_sin_turns(index * labels[1:2])


def fill_phases(buf, rows_of, phases):
    cos_u, sin_u, cos_v, sin_v = phases
    slots = cos_v.shape[1]
    for i, j in enumerate(rows_of):
        cu, su = cos_u[j : j + 1], sin_u[j : j + 1]
        rows = slice(i * NBLK, (i + 1) * NBLK)
        buf[rows, :slots] = (cu * cos_v - su * sin_v).astype(jnp.bfloat16)
        buf[rows, slots:] = (cu * sin_v + su * cos_v).astype(jnp.bfloat16)


PER_CHUNK = 8
IMAGE_PARTS = 2


def spectrum_kernel(sizes, direct, *rest):
    count = len(sizes)
    in_refs, (out_ref, turn_ref, phases_buf, patch_buf) = rest[:count], rest[count:]
    load_patches(in_refs, sizes, patch_buf)
    phases = cell_phases(in_refs, sizes, direct)
    width = PER_CHUNK * NBLK
    for chunk in range(NBLK // PER_CHUNK):
        buf = phases_buf.at[chunk % 2]
        fill_phases(buf, range(chunk * PER_CHUNK, (chunk + 1) * PER_CHUNK), phases)
        out_ref[chunk * width : (chunk + 1) * width, :] = jnp.dot(
            buf[...], patch_buf[...], preferred_element_type=jnp.float32
        )

    cells = PSIDE * PSIDE
    lane = lax.broadcasted_iota(jnp.int32, (NBLK, cells), 1)
    row = lax.broadcasted_iota(jnp.int32, (NBLK, cells), 0)
    cos_u, sin_u = cos_sin_turns((row * (lane // PSIDE)).astype(jnp.float32) * (1.0 / GRID))
    cos_v, sin_v = cos_sin_turns((row * (lane % PSIDE)).astype(jnp.float32) * (1.0 / GRID))
    for j in range(NBLK):
        rows = slice(j * NBLK, (j + 1) * NBLK)
        cu, su = cos_u[j : j + 1], sin_u[j : j + 1]
        turn_ref[rows, :cells] = cu * cos_v - su * sin_v
        turn_ref[rows, cells:] = cu * sin_v + su * cos_v


def image_kernel(sizes, direct, groups, chunks, table_ref, early_ref, turn_ref, *rest):
    count = len(sizes)
    in_refs, out_refs = rest[:count], rest[count : count + groups]
    phases_buf, patch_buf, table_buf = rest[count + groups :]
    cells = PSIDE * PSIDE
    share = cells // groups
    load_patches(in_refs, sizes, patch_buf)
    for s in range(groups):
        start = pl.multiple_of((lax.axis_index("freq") ^ s) * share, share)
        table_buf[s * share : (s + 1) * share, :] = table_ref[pl.ds(start, share), :]
    phases = cell_phases(in_refs, sizes, direct)

    width = PER_CHUNK * NBLK
    for i, chunk in enumerate(chunks):
        buf = phases_buf.at[chunk % 2]
        fill_phases(buf, range(chunk * PER_CHUNK, (chunk + 1) * PER_CHUNK), phases)
        here = slice(chunk * width, (chunk + 1) * width)
        spectrum = early_ref[here, :] + jnp.dot(buf[...], patch_buf[...], preferred_element_type=jnp.float32)
        real, imag = spectrum[:, :cells], spectrum[:, cells:]
        cosine, sine = turn_ref[here, :cells], turn_ref[here, cells:]
        turned = jnp.concatenate([real * cosine - imag * sine, real * sine + imag * cosine], axis=1).astype(jnp.bfloat16)
        image = lax.dot_general(
            table_buf[...], turned, (((1,), (1,)), ((), ())), preferred_element_type=jnp.float32
        ).astype(jnp.bfloat16)
        for s in range(groups):
            out_refs[s][:, i * width : (i + 1) * width] = image[s * share : (s + 1) * share]


def finish_kernel(groups, parts, *refs):
    out_ref = refs[-1]
    columns = PSIDE // groups
    per_tile = LANES // NBLK
    lane = lax.broadcasted_iota(jnp.int32, (PSIDE, LANES), 1) // NBLK
    for tile in range(NBLK // per_tile):
        part, place = divmod(tile, NBLK // per_tile // parts)
        in_refs = refs[part * groups : (part + 1) * groups]
        lanes = slice(place * LANES, (place + 1) * LANES)
        total = in_refs[0][:, lanes].astype(jnp.float32)
        for ref in in_refs[1:]:
            total = total + ref[:, lanes].astype(jnp.float32)
        for i in range(per_tile):
            value = jnp.zeros((PSIDE, LANES), jnp.float32)
            for kq in range(columns):
                piece = total[kq * PSIDE : (kq + 1) * PSIDE]
                shift = (kq - i) * NBLK % LANES
                piece = pltpu.roll(piece, shift, 1) if shift else piece
                value = jnp.where(lane == kq, piece, value)
            out_ref[pl.ds(tile * per_tile + i, PSIDE, stride=NBLK), :] = value


def patch_table():
    index = np.arange(PSIDE)
    kq, jq = (a.reshape(-1, 1) for a in np.meshgrid(index, index, indexing="ij"))
    pu, pv = (a.reshape(1, -1) for a in np.meshgrid(index, index, indexing="ij"))
    angle = 2.0 * np.pi * ((pu * jq + pv * kq) % PSIDE) / PSIDE
    return np.concatenate([np.cos(angle), -np.sin(angle)], axis=1) / GRID


def swap(piece, axis, distance):
    count = lax.axis_size(axis)
    return lax.ppermute(piece, axis, [(i, i ^ distance) for i in range(count)])


def overflow_slots(tiles, capacity, few, facets):
    full = min(facets, tiles // capacity)
    most = full * (capacity - few)
    if full < facets:
        most += max(0, tiles - full * capacity - few)
    return -(-most // 16) * 16


def packed_shards(visibilities, uvw, facet_of, plane_of, cell_of, kernels, centers):
    peers, groups = lax.axis_size("facet"), lax.axis_size("freq")
    tiles = visibilities.shape[1]
    capacity = 4 * tiles // peers
    planes, _, depth, cells = kernels.shape
    near = peers // 2
    few = 5 * capacity // 8
    sizes = [capacity] * near + [few] * near + [overflow_slots(tiles, capacity, few, near)]
    payloads = [jax.ShapeDtypeStruct((2 * cells // LANES * size + SUBLANES, LANES), jnp.bfloat16) for size in sizes]
    lanes = depth // LANES
    vis_rows = visibilities[0].reshape(tiles, 2, lanes, LANES).transpose(0, 2, 1, 3).reshape(-1, LANES)
    operands = (
        centers.T,
        facet_of.reshape(1, tiles),
        plane_of,
        cell_of,
        vis_rows,
        uvw[0].transpose(1, 0, 2),
        kernels,
    )
    pieces = pl.pallas_call(
        functools.partial(gather_kernel, peers, sizes),
        out_shape=payloads,
        in_specs=[HBM] * len(operands),
        out_specs=[VMEM] * len(sizes),
        scratch_shapes=[pltpu.VMEM(operand.shape, operand.dtype) for operand in operands]
        + [
            pltpu.VMEM(vis_rows.shape, jnp.float32),
            pltpu.VMEM((2, tiles, 2 * depth), jnp.bfloat16),
            pltpu.SemaphoreType.DMA((len(operands) + 1 + planes,)),
        ],
        compiler_params=compiler_params(40),
        name="gather",
    )(*(pltpu.with_memory_space_constraint(operand, pltpu.HBM) for operand in operands))
    overflow = [swap(pieces[peers], "facet", near)]
    received = [pieces[0]] + [swap(pieces[s], "facet", s) for s in range(1, peers)]
    overflow += [swap(overflow[0], "facet", s) for s in range(1, near)]
    early, late = received[:near] + overflow[:1], received[near:] + overflow[1:]
    early_sizes, late_sizes = sizes[:near] + sizes[peers:], sizes[near:peers] + sizes[peers:] * (near - 1)
    share = cells // groups
    points = NBLK * NBLK

    def buffers_and_cost(slots):
        buffers = [
            pltpu.VMEM((2, PER_CHUNK * NBLK, 2 * slots), jnp.bfloat16),
            pltpu.VMEM((2 * slots, 2 * cells), jnp.bfloat16),
        ]
        return buffers, pl.CostEstimate(flops=8 * points * slots * cells, bytes_accessed=4 << 20, transcendentals=0)

    buffers, cost = buffers_and_cost(padded(early_sizes))
    spectrum, turns = pl.pallas_call(
        functools.partial(spectrum_kernel, early_sizes, near),
        out_shape=[jax.ShapeDtypeStruct((points, 2 * cells), jnp.float32)] * 2,
        in_specs=[VMEM] * len(early),
        out_specs=[VMEM] * 2,
        scratch_shapes=buffers,
        compiler_params=compiler_params(40),
        cost_estimate=cost,
        name="spectrum",
    )(*early)
    buffers, cost = buffers_and_cost(padded(late_sizes))
    parts = IMAGE_PARTS
    chunks = NBLK // PER_CHUNK // parts
    image = jax.ShapeDtypeStruct((share, points // parts), jnp.bfloat16)
    table = jnp.asarray(patch_table(), jnp.bfloat16)
    summed = []
    for part in range(parts):
        images = pl.pallas_call(
            functools.partial(image_kernel, late_sizes, near, groups, range(part * chunks, (part + 1) * chunks)),
            out_shape=[image] * groups,
            in_specs=[VMEM] * (3 + len(late)),
            out_specs=[VMEM] * groups,
            scratch_shapes=buffers + [pltpu.VMEM((cells, 2 * cells), jnp.bfloat16)],
            compiler_params=compiler_params(40),
            cost_estimate=cost,
        )(table, spectrum, turns, *late)
        summed += [images[0]] + [swap(images[s], "freq", s) for s in range(1, groups)]
    facet_image = pl.pallas_call(
        functools.partial(finish_kernel, groups, parts),
        out_shape=jax.ShapeDtypeStruct((GRID, GRID // groups), jnp.float32),
        in_specs=[VMEM] * len(summed),
        out_specs=VMEM,
        compiler_params=compiler_params(16),
        name="finish",
    )(*summed)
    return facet_image[None]


def solution(mesh):
    in_specs = (
        P("freq", "facet", None, None),
        P("freq", "facet", None, None),
        P("freq", "facet", None),
        P("freq", "facet"),
        P("freq", "facet"),
        P(),
        P(),
    )
    out_specs = P("facet", None, "freq")

    def body(*args):
        peers, groups = lax.axis_size("facet"), lax.axis_size("freq")
        capacity = 4 * args[0].shape[1] // peers
        powers = peers & (peers - 1) == 0 and groups & (groups - 1) == 0
        packed = capacity == LANES and powers and GRID // groups == LANES
        return (packed_shards if packed else shards)(*args)

    return jax.shard_map(body, mesh=mesh, in_specs=in_specs, out_specs=out_specs, check_vma=False)
```

```python
import functools

import jax
import jax.numpy as jnp
import numpy as np
from jax import lax
from jax.experimental import pallas as pl
from jax.experimental.pallas import tpu as pltpu
from jax.sharding import PartitionSpec as P


GRID = 512
PSIDE = 16
NBLK = GRID // PSIDE
LANES = 128
SUBLANES = 8

SIN_POLY = (4.442882919124345, -7.30824568650904, 3.6063542184326933, -0.8461116503732697, 0.10982451642490525)
COS_POLY = (1.4142134962552284, -6.978850948563788, 5.73946037690675, -1.8835579059841707, 0.3106880275217573)


def horner(square, coefficients):
    value = coefficients[-1] * square + coefficients[-2]
    for coefficient in coefficients[-3::-1]:
        value = value * square + coefficient
    return value


def cos_sin_turns(turns):
    rest = turns - jnp.round(turns)
    square = rest * rest
    sine = rest * horner(square, SIN_POLY)
    return (1.0 - sine * sine, sine * horner(square, COS_POLY))


def compiler_params(mebibytes):
    return pltpu.CompilerParams(vmem_limit_bytes=mebibytes << 20)


VMEM = pl.BlockSpec(memory_space=pltpu.VMEM)
HBM = pl.BlockSpec(memory_space=pltpu.HBM)


def dft_tables(length):
    indices = jnp.arange(length, dtype=jnp.int32)
    products_mod = indices[:, None] * indices[None, :] % length
    angle_table = products_mod.astype(jnp.float32) * (2.0 * jnp.pi / length)
    norm_scale = 1.0 / jnp.sqrt(jnp.float32(length))
    table_real = (jnp.cos(angle_table) * norm_scale).astype(jnp.bfloat16)
    table_imag = (jnp.sin(angle_table) * norm_scale).astype(jnp.bfloat16)
    return (table_real, table_imag)


def rotate_tiles(vis_pair, coords, sky_pos):
    l_coord = sky_pos[:, 0:1]
    m_coord = sky_pos[:, 1:2]
    w_term = jnp.sqrt(1.0 - l_coord * l_coord - m_coord * m_coord) - 1.0
    coords = coords.astype(jnp.float32)
    phase_angle = (
        2.0 * jnp.pi * (l_coord * coords[:, 0] + m_coord * coords[:, 1] + w_term * coords[:, 2])
    )
    cosine = jnp.cos(phase_angle)
    sine_part = jnp.sin(phase_angle)
    real_part = vis_pair[:, 0].astype(jnp.float32)
    imag_part = vis_pair[:, 1].astype(jnp.float32)
    rot_real = (real_part * cosine + imag_part * sine_part).astype(jnp.bfloat16)
    rot_imag = (imag_part * cosine - real_part * sine_part).astype(jnp.bfloat16)
    return (rot_real, rot_imag)


def stack_kernels(kernels):
    kern_real = kernels[:, 0]
    kern_imag = kernels[:, 1]
    upper_rows = jnp.concatenate([kern_real, kern_imag], axis=2)
    lower_rows = jnp.concatenate([-kern_imag, kern_real], axis=2)
    stacked_rows = jnp.concatenate([upper_rows, lower_rows], axis=0)
    return stacked_rows.reshape(-1, stacked_rows.shape[2])


def grid_tiles(rot_real, rot_imag, planes, stacked, plane_count):
    plane_select = (planes[:, None] == jnp.arange(plane_count)[None, :]).astype(jnp.bfloat16)
    spread = jnp.concatenate(
        [
            rot_real[:, None, :] * plane_select[:, :, None],
            rot_imag[:, None, :] * plane_select[:, :, None],
        ],
        axis=1,
    )
    spread = spread.reshape(spread.shape[0], -1)
    return jnp.dot(spread, stacked, preferred_element_type=jnp.float32).astype(jnp.bfloat16)


def shards(visibilities, uvw, facet_of, plane_of, cell_of, kernels, centers):
    peer_count = lax.axis_size("facet")
    tile_count = visibilities.shape[1]
    capacity = 4 * tile_count // peer_count
    total_slots = peer_count * capacity
    vis_pair = visibilities[0]
    coords = uvw[0]
    target = facet_of[0, :, 0]
    planes = plane_of[0]
    tile_cells = cell_of[0]
    plane_count = kernels.shape[0]
    stacked = stack_kernels(kernels)
    dest_hits = (target[:, None] == jnp.arange(peer_count)[None, :]).astype(jnp.int32)
    before = jnp.cumsum(dest_hits, axis=0) - dest_hits
    within_rank = jnp.sum(before * dest_hits, axis=1)
    slot_index = target * capacity + within_rank
    chosen = (target[:, None] == jnp.arange(centers.shape[0])[None, :]).astype(jnp.float32)
    sky_rows = jnp.sum(chosen[:, :, None] * centers[None, :, :], axis=1)
    rot_real, rot_imag = rotate_tiles(vis_pair, coords, sky_rows)
    own_patches = grid_tiles(rot_real, rot_imag, planes, stacked, plane_count)
    patch_buffer = (
        jnp.zeros((total_slots, own_patches.shape[1]), jnp.bfloat16).at[slot_index].set(own_patches)
    )
    cell_buffer = jnp.zeros((total_slots,), jnp.int32).at[slot_index].set(tile_cells)
    patches, slot_cells = (
        lax.all_to_all(
            patch_buffer.reshape(peer_count, capacity, -1),
            "facet",
            split_axis=0,
            concat_axis=0,
            tiled=True,
        ),
        lax.all_to_all(
            cell_buffer.reshape(peer_count, capacity),
            "facet",
            split_axis=0,
            concat_axis=0,
            tiled=True,
        ),
    )
    patches = patches.reshape(-1, patches.shape[-1])
    slot_cells = slot_cells.reshape(-1)
    nblocks = GRID // PSIDE
    ncells = nblocks * nblocks
    placing = (slot_cells[None, :] == jnp.arange(ncells)[:, None]).astype(jnp.bfloat16)
    blocks = jnp.dot(placing, patches, preferred_element_type=jnp.float32).astype(jnp.bfloat16)
    uv_grid = (
        blocks.reshape(nblocks, nblocks, 2, PSIDE, PSIDE)
        .transpose(2, 0, 3, 1, 4)
        .reshape(2 * GRID, GRID)
    )
    table_real, table_imag = dft_tables(GRID)
    table_both = jnp.concatenate([table_real, table_imag], axis=1)
    product = jnp.dot(uv_grid, table_both, preferred_element_type=jnp.float32)
    half_real = product[:GRID, :GRID] - product[GRID:, GRID:]
    half_imag = product[:GRID, GRID:] + product[GRID:, :GRID]
    partial_value = jnp.stack([half_real, half_imag]).astype(jnp.bfloat16)
    summed = lax.psum_scatter(
        partial_value.astype(jnp.float32).astype(jnp.bfloat16),
        "freq",
        scatter_dimension=2,
        tiled=True,
    )
    right_side = jnp.concatenate([summed[0], -summed[1]], axis=0)
    facet_image = jnp.dot(table_both, right_side, preferred_element_type=jnp.float32)
    return facet_image[None]


def gather_kernel(peers, sizes, centers_hbm, facet_hbm, plane_hbm, cell_hbm, vis_hbm, uvw_hbm, kern_hbm, *rest):
    out_refs = rest[: len(sizes)]
    (centers_ref, facet_ref, plane_ref, cell_ref, vis_ref, uvw_ref, kern_ref, parts_ref, rows_ref, placing_ref, sems) = rest[
        len(sizes) :
    ]
    planes, _, depth, cells = kern_ref.shape
    tiles = facet_ref.shape[1]
    half = tiles // 2
    groups_of_lanes = depth // LANES
    rows_of = [slice(h * half, (h + 1) * half) for h in range(2)]
    vis_rows = vis_ref.shape[0] // 2
    transfers = [(centers_hbm, centers_ref), (facet_hbm, facet_ref), (plane_hbm, plane_ref), (cell_hbm, cell_ref)]
    for h in range(2):
        part = slice(h * vis_rows, (h + 1) * vis_rows)
        transfers += [(vis_hbm.at[part], vis_ref.at[part]), (uvw_hbm.at[:, rows_of[h]], uvw_ref.at[:, rows_of[h]])]
    transfers += [(kern_hbm.at[p], kern_ref.at[p]) for p in range(planes)]
    copies = [pltpu.make_async_copy(source, target, sems.at[i]) for i, (source, target) in enumerate(transfers)]
    for copy in copies:
        copy.start()
    for copy in copies[:4]:
        copy.wait()
    facet = facet_ref[...]
    l_row = jnp.zeros(facet.shape, jnp.float32)
    m_row = jnp.zeros(facet.shape, jnp.float32)
    for f in range(peers):
        hit = facet == f
        l_row = jnp.where(hit, centers_ref[0:1, f : f + 1], l_row)
        m_row = jnp.where(hit, centers_ref[1:2, f : f + 1], m_row)
    d_row = jnp.sqrt(1.0 - l_row * l_row - m_row * m_row) - 1.0
    plane_row = plane_ref[...].astype(jnp.float32)
    zero_row = jnp.zeros_like(l_row)
    columns = jnp.concatenate([l_row, m_row, d_row, plane_row] + [zero_row] * 4, axis=0).T

    near, capacity, few, slots = peers // 2, sizes[0], sizes[peers // 2], LANES * len(sizes)
    relative = facet ^ lax.axis_index("facet")
    lanes = lax.broadcasted_iota(jnp.int32, (tiles, tiles), 1)
    earlier = (lax.broadcasted_iota(jnp.int32, (tiles, tiles), 0) < lanes).astype(jnp.float32).astype(jnp.bfloat16)
    facets = lax.broadcasted_iota(jnp.int32, (peers, tiles), 0)
    hits = facets == relative
    before = jnp.dot(hits.astype(jnp.float32).astype(jnp.bfloat16), earlier, preferred_element_type=jnp.float32)
    rank = jnp.sum(jnp.where(hits, before, 0.0), axis=0, keepdims=True).astype(jnp.int32)
    passed = jnp.where(facets >= near, jnp.maximum(before - few, 0.0), 0.0)
    passed = jnp.sum(passed, axis=0, keepdims=True).astype(jnp.int32)
    slot = jnp.where((relative < near) | (rank < few), relative * capacity + rank, peers * capacity + passed)

    placing = lax.broadcasted_iota(jnp.int32, (slots, tiles), 0) == slot
    placing = placing.astype(jnp.float32).astype(jnp.bfloat16)
    placing_ref[...] = placing
    cell = cell_ref[...].astype(jnp.float32)
    block_u = jnp.floor(cell * (1.0 / NBLK))
    block_v = cell - block_u * NBLK
    labels = [block_u, block_v, facet.astype(jnp.float32)] + [zero_row] * (SUBLANES - 3)
    labels = jnp.concatenate(labels, axis=0).astype(jnp.bfloat16)
    labels = lax.dot_general(labels, placing, (((1,), (1,)), ((), ())), preferred_element_type=jnp.float32)
    labels = labels.astype(jnp.bfloat16)
    for i, (ref, size) in enumerate(zip(out_refs, sizes)):
        ref[2 * cells // LANES * size :, :] = labels[:, i * LANES : (i + 1) * LANES]

    patches = []
    for h in range(2):
        tile_rows = rows_of[h]
        for copy in copies[4:6] if h == 0 else copies[6:]:
            copy.wait()
        part = slice(h * vis_rows, (h + 1) * vis_rows)
        parts_ref[part] = vis_ref[part].astype(jnp.float32)
        l_col, m_col, d_col = (jnp.broadcast_to(columns[tile_rows, i : i + 1], (half, LANES)) for i in range(3))
        for j in range(groups_of_lanes):
            lane = slice(j * LANES, (j + 1) * LANES)
            u, v, w = (uvw_ref[i, tile_rows, lane].astype(jnp.float32) for i in range(3))
            cosine, sine = cos_sin_turns(l_col * u + m_col * v + d_col * w)
            first = 2 * (h * half * groups_of_lanes + j)
            real = parts_ref[pl.ds(first, half, stride=2 * groups_of_lanes), :]
            imag = parts_ref[pl.ds(first + 1, half, stride=2 * groups_of_lanes), :]
            rot_real = (real * cosine + imag * sine).astype(jnp.bfloat16)
            rot_imag = (imag * cosine - real * sine).astype(jnp.bfloat16)
            right = slice(depth + j * LANES, depth + (j + 1) * LANES)
            rows_ref[h, :half, lane] = rot_real
            rows_ref[h, :half, right] = -rot_imag
            rows_ref[h, half:, lane] = rot_imag
            rows_ref[h, half:, right] = rot_real
    for h in range(2):
        plane_two = jnp.concatenate([columns[rows_of[h], 3:4]] * 2, axis=0)
        total = None
        for p in range(planes):
            mask = (plane_two == float(p)).astype(jnp.float32).astype(jnp.bfloat16)
            product = jnp.dot(
                rows_ref[h] * mask, kern_ref[p].reshape(2 * depth, cells), preferred_element_type=jnp.float32
            )
            total = product if total is None else total + product
        patches.append(jnp.concatenate([total[:half], total[half:]], axis=1).astype(jnp.bfloat16))
    patches = jnp.concatenate(patches, axis=0)
    placed = jnp.dot(placing_ref[...], patches, preferred_element_type=jnp.float32).astype(jnp.bfloat16)
    for i, (ref, size) in enumerate(zip(out_refs, sizes)):
        start = i * LANES
        for j in range(2 * cells // LANES):
            ref[j * size : (j + 1) * size, :] = placed[start : start + size, j * LANES : (j + 1) * LANES]


def padded(sizes):
    return -(-sum(sizes) // LANES) * LANES


def load_patches(in_refs, sizes, patch_buf):
    cells = PSIDE * PSIDE
    half_tiles = cells // LANES
    slots = padded(sizes)
    start = 0
    for ref, size in zip(in_refs, sizes):
        rows = slice(start, start + size)
        below = slice(slots + start, slots + start + size)
        for j in range(half_tiles):
            left = slice(j * LANES, (j + 1) * LANES)
            right = slice(cells + j * LANES, cells + (j + 1) * LANES)
            real = ref[j * size : (j + 1) * size, :]
            imag = ref[(half_tiles + j) * size : (half_tiles + j + 1) * size, :]
            patch_buf[rows, left] = real
            patch_buf[rows, right] = imag
            patch_buf[below, left] = -imag
            patch_buf[below, right] = real
        start += size
    if start < slots:
        for first in (0, slots):
            patch_buf[first + start : first + slots, :] = jnp.zeros((slots - start, 2 * cells), jnp.bfloat16)


def cell_phases(in_refs, sizes, direct):
    slots = padded(sizes)
    labels = [jnp.zeros((SUBLANES, LANES), jnp.float32) for _ in range(slots // LANES)]
    lane = lax.broadcasted_iota(jnp.int32, (SUBLANES, LANES), 1)
    start = 0
    for ref, size in zip(in_refs, sizes):
        here = ref[2 * PSIDE * PSIDE // LANES * size :, :].astype(jnp.float32)
        tile, shift = divmod(start, LANES)
        if shift:
            here = pltpu.roll(here, shift, 1)
            if shift + size > LANES:
                labels[tile + 1] = jnp.where(lane < shift, here, 0.0)
            here = jnp.where(lane >= shift, here, 0.0)
        labels[tile] = labels[tile] + here
        start += size
    labels = jnp.concatenate(labels, axis=1)
    lane = lax.broadcasted_iota(jnp.int32, (1, slots), 1)
    mine = labels[2:3] == lax.axis_index("facet").astype(jnp.float32)
    mine = jnp.where(mine | (lane < sum(sizes[:direct])), 1.0, 0.0)
    index = lax.broadcasted_iota(jnp.int32, (NBLK, slots), 0).astype(jnp.float32) * (1.0 / NBLK)
    cos_u, sin_u = cos_sin_turns(index * labels[0:1])
    return (cos_u * mine, sin_u * mine) + cos_sin_turns(index * labels[1:2])


def fill_phases(buf, rows_of, phases):
    cos_u, sin_u, cos_v, sin_v = phases
    slots = cos_v.shape[1]
    for i, j in enumerate(rows_of):
        cu, su = cos_u[j : j + 1], sin_u[j : j + 1]
        rows = slice(i * NBLK, (i + 1) * NBLK)
        buf[rows, :slots] = (cu * cos_v - su * sin_v).astype(jnp.bfloat16)
        buf[rows, slots:] = (cu * sin_v + su * cos_v).astype(jnp.bfloat16)


PER_CHUNK = 8
IMAGE_PARTS = 2


def add_spectrum(in_refs, sizes, direct, out_ref, phases_buf, patch_buf, start_ref=None):
    load_patches(in_refs, sizes, patch_buf)
    phases = cell_phases(in_refs, sizes, direct)
    width = PER_CHUNK * NBLK
    for chunk in range(NBLK // PER_CHUNK):
        here = slice(chunk * width, (chunk + 1) * width)
        buf = phases_buf.at[chunk % 2]
        fill_phases(buf, range(chunk * PER_CHUNK, (chunk + 1) * PER_CHUNK), phases)
        product = jnp.dot(buf[...], patch_buf[...], preferred_element_type=jnp.float32)
        out_ref[here, :] = product if start_ref is None else start_ref[here, :] + product


def middle_kernel(sizes, direct, start_ref, *rest):
    count = len(sizes)
    out_ref, phases_buf, patch_buf = rest[count:]
    add_spectrum(rest[:count], sizes, direct, out_ref, phases_buf, patch_buf, start_ref)


def spectrum_kernel(sizes, direct, *rest):
    count = len(sizes)
    out_ref, turn_ref, phases_buf, patch_buf = rest[count:]
    add_spectrum(rest[:count], sizes, direct, out_ref, phases_buf, patch_buf)

    cells = PSIDE * PSIDE
    lane = lax.broadcasted_iota(jnp.int32, (NBLK, cells), 1)
    row = lax.broadcasted_iota(jnp.int32, (NBLK, cells), 0)
    cos_u, sin_u = cos_sin_turns((row * (lane // PSIDE)).astype(jnp.float32) * (1.0 / GRID))
    cos_v, sin_v = cos_sin_turns((row * (lane % PSIDE)).astype(jnp.float32) * (1.0 / GRID))
    for j in range(NBLK):
        rows = slice(j * NBLK, (j + 1) * NBLK)
        cu, su = cos_u[j : j + 1], sin_u[j : j + 1]
        turn_ref[rows, :cells] = cu * cos_v - su * sin_v
        turn_ref[rows, cells:] = cu * sin_v + su * cos_v


def image_kernel(sizes, direct, groups, chunks, table_ref, early_ref, turn_ref, *rest):
    count = len(sizes)
    in_refs, out_refs = rest[:count], rest[count : count + groups]
    phases_buf, patch_buf, table_buf = rest[count + groups :]
    cells = PSIDE * PSIDE
    share = cells // groups
    load_patches(in_refs, sizes, patch_buf)
    for s in range(groups):
        start = pl.multiple_of((lax.axis_index("freq") ^ s) * share, share)
        table_buf[s * share : (s + 1) * share, :] = table_ref[pl.ds(start, share), :]
    phases = cell_phases(in_refs, sizes, direct)

    width = PER_CHUNK * NBLK
    for i, chunk in enumerate(chunks):
        buf = phases_buf.at[chunk % 2]
        fill_phases(buf, range(chunk * PER_CHUNK, (chunk + 1) * PER_CHUNK), phases)
        here = slice(chunk * width, (chunk + 1) * width)
        spectrum = early_ref[here, :] + jnp.dot(buf[...], patch_buf[...], preferred_element_type=jnp.float32)
        real, imag = spectrum[:, :cells], spectrum[:, cells:]
        cosine, sine = turn_ref[here, :cells], turn_ref[here, cells:]
        turned = jnp.concatenate([real * cosine - imag * sine, real * sine + imag * cosine], axis=1).astype(jnp.bfloat16)
        image = lax.dot_general(
            table_buf[...], turned, (((1,), (1,)), ((), ())), preferred_element_type=jnp.float32
        ).astype(jnp.bfloat16)
        for s in range(groups):
            out_refs[s][:, i * width : (i + 1) * width] = image[s * share : (s + 1) * share]


def finish_kernel(groups, parts, *refs):
    out_ref = refs[-1]
    columns = PSIDE // groups
    per_tile = LANES // NBLK
    lane = lax.broadcasted_iota(jnp.int32, (PSIDE, LANES), 1) // NBLK
    for tile in range(NBLK // per_tile):
        part, place = divmod(tile, NBLK // per_tile // parts)
        in_refs = refs[part * groups : (part + 1) * groups]
        lanes = slice(place * LANES, (place + 1) * LANES)
        total = in_refs[0][:, lanes].astype(jnp.float32)
        for ref in in_refs[1:]:
            total = total + ref[:, lanes].astype(jnp.float32)
        for i in range(per_tile):
            value = jnp.zeros((PSIDE, LANES), jnp.float32)
            for kq in range(columns):
                piece = total[kq * PSIDE : (kq + 1) * PSIDE]
                shift = (kq - i) * NBLK % LANES
                piece = pltpu.roll(piece, shift, 1) if shift else piece
                value = jnp.where(lane == kq, piece, value)
            out_ref[pl.ds(tile * per_tile + i, PSIDE, stride=NBLK), :] = value


def patch_table():
    index = np.arange(PSIDE)
    kq, jq = (a.reshape(-1, 1) for a in np.meshgrid(index, index, indexing="ij"))
    pu, pv = (a.reshape(1, -1) for a in np.meshgrid(index, index, indexing="ij"))
    angle = 2.0 * np.pi * ((pu * jq + pv * kq) % PSIDE) / PSIDE
    return np.concatenate([np.cos(angle), -np.sin(angle)], axis=1) / GRID


def swap(piece, axis, distance):
    count = lax.axis_size(axis)
    return lax.ppermute(piece, axis, [(i, i ^ distance) for i in range(count)])


def overflow_slots(tiles, capacity, few, facets):
    full = min(facets, tiles // capacity)
    most = full * (capacity - few)
    if full < facets:
        most += max(0, tiles - full * capacity - few)
    return -(-most // 16) * 16


def packed_shards(visibilities, uvw, facet_of, plane_of, cell_of, kernels, centers):
    peers, groups = lax.axis_size("facet"), lax.axis_size("freq")
    tiles = visibilities.shape[1]
    capacity = 4 * tiles // peers
    planes, _, depth, cells = kernels.shape
    near = peers // 2
    few = 5 * capacity // 8
    sizes = [capacity] * near + [few] * near + [overflow_slots(tiles, capacity, few, near)]
    payloads = [jax.ShapeDtypeStruct((2 * cells // LANES * size + SUBLANES, LANES), jnp.bfloat16) for size in sizes]
    lanes = depth // LANES
    vis_rows = visibilities[0].reshape(tiles, 2, lanes, LANES).transpose(0, 2, 1, 3).reshape(-1, LANES)
    operands = (
        centers.T,
        facet_of.reshape(1, tiles),
        plane_of,
        cell_of,
        vis_rows,
        uvw[0].transpose(1, 0, 2),
        kernels,
    )
    pieces = pl.pallas_call(
        functools.partial(gather_kernel, peers, sizes),
        out_shape=payloads,
        in_specs=[HBM] * len(operands),
        out_specs=[VMEM] * len(sizes),
        scratch_shapes=[pltpu.VMEM(operand.shape, operand.dtype) for operand in operands]
        + [
            pltpu.VMEM(vis_rows.shape, jnp.float32),
            pltpu.VMEM((2, tiles, 2 * depth), jnp.bfloat16),
            pltpu.VMEM((LANES * len(sizes), tiles), jnp.bfloat16),
            pltpu.SemaphoreType.DMA((len(operands) + 1 + planes,)),
        ],
        compiler_params=compiler_params(40),
        name="gather",
    )(*(pltpu.with_memory_space_constraint(operand, pltpu.HBM) for operand in operands))
    overflow = [swap(pieces[peers], "facet", near)]
    received = [pieces[0]] + [swap(pieces[s], "facet", s) for s in range(1, peers)]
    overflow += [swap(overflow[0], "facet", s) for s in range(1, near)]
    half = near // 2
    early, early_sizes = received[:near] + overflow[:1], sizes[:near] + sizes[peers:]
    middle, middle_sizes = received[near:-half] + overflow[1:], sizes[near : peers - half] + sizes[peers:] * (near - 1)
    late, late_sizes = received[-half:], sizes[peers - half : peers]
    share = cells // groups
    points = NBLK * NBLK

    def buffers_and_cost(slots):
        buffers = [
            pltpu.VMEM((2, PER_CHUNK * NBLK, 2 * slots), jnp.bfloat16),
            pltpu.VMEM((2 * slots, 2 * cells), jnp.bfloat16),
        ]
        return buffers, pl.CostEstimate(flops=8 * points * slots * cells, bytes_accessed=4 << 20, transcendentals=0)

    buffers, cost = buffers_and_cost(padded(early_sizes))
    spectrum, turns = pl.pallas_call(
        functools.partial(spectrum_kernel, early_sizes, near),
        out_shape=[jax.ShapeDtypeStruct((points, 2 * cells), jnp.float32)] * 2,
        in_specs=[VMEM] * len(early),
        out_specs=[VMEM] * 2,
        scratch_shapes=buffers,
        compiler_params=compiler_params(40),
        cost_estimate=cost,
        name="spectrum",
    )(*early)
    buffers, cost = buffers_and_cost(padded(middle_sizes))
    spectrum = pl.pallas_call(
        functools.partial(middle_kernel, middle_sizes, near - half),
        out_shape=jax.ShapeDtypeStruct((points, 2 * cells), jnp.float32),
        in_specs=[VMEM] * (1 + len(middle)),
        out_specs=VMEM,
        scratch_shapes=buffers,
        compiler_params=compiler_params(40),
        cost_estimate=cost,
        name="middle",
    )(spectrum, *middle)
    buffers, cost = buffers_and_cost(padded(late_sizes))
    parts = IMAGE_PARTS
    chunks = NBLK // PER_CHUNK // parts
    image = jax.ShapeDtypeStruct((share, points // parts), jnp.bfloat16)
    table = jnp.asarray(patch_table(), jnp.bfloat16)
    summed = []
    for part in range(parts):
        images = pl.pallas_call(
            functools.partial(image_kernel, late_sizes, half, groups, range(part * chunks, (part + 1) * chunks)),
            out_shape=[image] * groups,
            in_specs=[VMEM] * (3 + len(late)),
            out_specs=[VMEM] * groups,
            scratch_shapes=buffers + [pltpu.VMEM((cells, 2 * cells), jnp.bfloat16)],
            compiler_params=compiler_params(40),
            cost_estimate=cost,
        )(table, spectrum, turns, *late)
        summed += [images[0]] + [swap(images[s], "freq", s) for s in range(1, groups)]
    facet_image = pl.pallas_call(
        functools.partial(finish_kernel, groups, parts),
        out_shape=jax.ShapeDtypeStruct((GRID, GRID // groups), jnp.float32),
        in_specs=[VMEM] * len(summed),
        out_specs=VMEM,
        compiler_params=compiler_params(16),
        name="finish",
    )(*summed)
    return facet_image[None]


def solution(mesh):
    in_specs = (
        P("freq", "facet", None, None),
        P("freq", "facet", None, None),
        P("freq", "facet", None),
        P("freq", "facet"),
        P("freq", "facet"),
        P(),
        P(),
    )
    out_specs = P("facet", None, "freq")

    def body(*args):
        peers, groups = lax.axis_size("facet"), lax.axis_size("freq")
        capacity = 4 * args[0].shape[1] // peers
        powers = peers & (peers - 1) == 0 and groups & (groups - 1) == 0
        packed = capacity == LANES and powers and GRID // groups == LANES
        return (packed_shards if packed else shards)(*args)

    return jax.shard_map(body, mesh=mesh, in_specs=in_specs, out_specs=out_specs, check_vma=False)
```

```python
import functools

import jax
import jax.numpy as jnp
import numpy as np
from jax import lax
from jax.experimental import pallas as pl
from jax.experimental.pallas import tpu as pltpu
from jax.sharding import PartitionSpec as P


GRID = 512
PSIDE = 16
NBLK = GRID // PSIDE
LANES = 128
SUBLANES = 8

SIN_POLY = (4.442882919124345, -7.30824568650904, 3.6063542184326933, -0.8461116503732697, 0.10982451642490525)
COS_POLY = (1.4142134962552284, -6.978850948563788, 5.73946037690675, -1.8835579059841707, 0.3106880275217573)


def horner(square, coefficients):
    value = coefficients[-1] * square + coefficients[-2]
    for coefficient in coefficients[-3::-1]:
        value = value * square + coefficient
    return value


def cos_sin_turns(turns):
    rest = turns - jnp.round(turns)
    square = rest * rest
    sine = rest * horner(square, SIN_POLY)
    return (1.0 - sine * sine, sine * horner(square, COS_POLY))


def compiler_params(mebibytes):
    return pltpu.CompilerParams(vmem_limit_bytes=mebibytes << 20)


VMEM = pl.BlockSpec(memory_space=pltpu.VMEM)
HBM = pl.BlockSpec(memory_space=pltpu.HBM)


def dft_tables(length):
    indices = jnp.arange(length, dtype=jnp.int32)
    products_mod = indices[:, None] * indices[None, :] % length
    angle_table = products_mod.astype(jnp.float32) * (2.0 * jnp.pi / length)
    norm_scale = 1.0 / jnp.sqrt(jnp.float32(length))
    table_real = (jnp.cos(angle_table) * norm_scale).astype(jnp.bfloat16)
    table_imag = (jnp.sin(angle_table) * norm_scale).astype(jnp.bfloat16)
    return (table_real, table_imag)


def rotate_tiles(vis_pair, coords, sky_pos):
    l_coord = sky_pos[:, 0:1]
    m_coord = sky_pos[:, 1:2]
    w_term = jnp.sqrt(1.0 - l_coord * l_coord - m_coord * m_coord) - 1.0
    coords = coords.astype(jnp.float32)
    phase_angle = (
        2.0 * jnp.pi * (l_coord * coords[:, 0] + m_coord * coords[:, 1] + w_term * coords[:, 2])
    )
    cosine = jnp.cos(phase_angle)
    sine_part = jnp.sin(phase_angle)
    real_part = vis_pair[:, 0].astype(jnp.float32)
    imag_part = vis_pair[:, 1].astype(jnp.float32)
    rot_real = (real_part * cosine + imag_part * sine_part).astype(jnp.bfloat16)
    rot_imag = (imag_part * cosine - real_part * sine_part).astype(jnp.bfloat16)
    return (rot_real, rot_imag)


def stack_kernels(kernels):
    kern_real = kernels[:, 0]
    kern_imag = kernels[:, 1]
    upper_rows = jnp.concatenate([kern_real, kern_imag], axis=2)
    lower_rows = jnp.concatenate([-kern_imag, kern_real], axis=2)
    stacked_rows = jnp.concatenate([upper_rows, lower_rows], axis=0)
    return stacked_rows.reshape(-1, stacked_rows.shape[2])


def grid_tiles(rot_real, rot_imag, planes, stacked, plane_count):
    plane_select = (planes[:, None] == jnp.arange(plane_count)[None, :]).astype(jnp.bfloat16)
    spread = jnp.concatenate(
        [
            rot_real[:, None, :] * plane_select[:, :, None],
            rot_imag[:, None, :] * plane_select[:, :, None],
        ],
        axis=1,
    )
    spread = spread.reshape(spread.shape[0], -1)
    return jnp.dot(spread, stacked, preferred_element_type=jnp.float32).astype(jnp.bfloat16)


def shards(visibilities, uvw, facet_of, plane_of, cell_of, kernels, centers):
    peer_count = lax.axis_size("facet")
    tile_count = visibilities.shape[1]
    capacity = 4 * tile_count // peer_count
    total_slots = peer_count * capacity
    vis_pair = visibilities[0]
    coords = uvw[0]
    target = facet_of[0, :, 0]
    planes = plane_of[0]
    tile_cells = cell_of[0]
    plane_count = kernels.shape[0]
    stacked = stack_kernels(kernels)
    dest_hits = (target[:, None] == jnp.arange(peer_count)[None, :]).astype(jnp.int32)
    before = jnp.cumsum(dest_hits, axis=0) - dest_hits
    within_rank = jnp.sum(before * dest_hits, axis=1)
    slot_index = target * capacity + within_rank
    chosen = (target[:, None] == jnp.arange(centers.shape[0])[None, :]).astype(jnp.float32)
    sky_rows = jnp.sum(chosen[:, :, None] * centers[None, :, :], axis=1)
    rot_real, rot_imag = rotate_tiles(vis_pair, coords, sky_rows)
    own_patches = grid_tiles(rot_real, rot_imag, planes, stacked, plane_count)
    patch_buffer = (
        jnp.zeros((total_slots, own_patches.shape[1]), jnp.bfloat16).at[slot_index].set(own_patches)
    )
    cell_buffer = jnp.zeros((total_slots,), jnp.int32).at[slot_index].set(tile_cells)
    patches, slot_cells = (
        lax.all_to_all(
            patch_buffer.reshape(peer_count, capacity, -1),
            "facet",
            split_axis=0,
            concat_axis=0,
            tiled=True,
        ),
        lax.all_to_all(
            cell_buffer.reshape(peer_count, capacity),
            "facet",
            split_axis=0,
            concat_axis=0,
            tiled=True,
        ),
    )
    patches = patches.reshape(-1, patches.shape[-1])
    slot_cells = slot_cells.reshape(-1)
    nblocks = GRID // PSIDE
    ncells = nblocks * nblocks
    placing = (slot_cells[None, :] == jnp.arange(ncells)[:, None]).astype(jnp.bfloat16)
    blocks = jnp.dot(placing, patches, preferred_element_type=jnp.float32).astype(jnp.bfloat16)
    uv_grid = (
        blocks.reshape(nblocks, nblocks, 2, PSIDE, PSIDE)
        .transpose(2, 0, 3, 1, 4)
        .reshape(2 * GRID, GRID)
    )
    table_real, table_imag = dft_tables(GRID)
    table_both = jnp.concatenate([table_real, table_imag], axis=1)
    product = jnp.dot(uv_grid, table_both, preferred_element_type=jnp.float32)
    half_real = product[:GRID, :GRID] - product[GRID:, GRID:]
    half_imag = product[:GRID, GRID:] + product[GRID:, :GRID]
    partial_value = jnp.stack([half_real, half_imag]).astype(jnp.bfloat16)
    summed = lax.psum_scatter(
        partial_value.astype(jnp.float32).astype(jnp.bfloat16),
        "freq",
        scatter_dimension=2,
        tiled=True,
    )
    right_side = jnp.concatenate([summed[0], -summed[1]], axis=0)
    facet_image = jnp.dot(table_both, right_side, preferred_element_type=jnp.float32)
    return facet_image[None]


def gather_kernel(peers, sizes, centers_hbm, facet_hbm, plane_hbm, cell_hbm, vis_hbm, uvw_hbm, kern_hbm, *rest):
    out_refs = rest[: len(sizes)]
    (centers_ref, facet_ref, plane_ref, cell_ref, vis_ref, uvw_ref, kern_ref, parts_ref, rows_ref, placing_ref, sems) = rest[
        len(sizes) :
    ]
    planes, _, depth, cells = kern_ref.shape
    tiles = facet_ref.shape[1]
    half = tiles // 2
    groups_of_lanes = depth // LANES
    rows_of = [slice(h * half, (h + 1) * half) for h in range(2)]
    vis_rows = vis_ref.shape[0] // 2
    transfers = [(centers_hbm, centers_ref), (facet_hbm, facet_ref), (plane_hbm, plane_ref), (cell_hbm, cell_ref)]
    for h in range(2):
        part = slice(h * vis_rows, (h + 1) * vis_rows)
        transfers += [(vis_hbm.at[part], vis_ref.at[part]), (uvw_hbm.at[:, rows_of[h]], uvw_ref.at[:, rows_of[h]])]
    transfers += [(kern_hbm.at[p], kern_ref.at[p]) for p in range(planes)]
    copies = [pltpu.make_async_copy(source, target, sems.at[i]) for i, (source, target) in enumerate(transfers)]
    for copy in copies:
        copy.start()
    for copy in copies[:4]:
        copy.wait()
    facet = facet_ref[...]
    l_row = jnp.zeros(facet.shape, jnp.float32)
    m_row = jnp.zeros(facet.shape, jnp.float32)
    for f in range(peers):
        hit = facet == f
        l_row = jnp.where(hit, centers_ref[0:1, f : f + 1], l_row)
        m_row = jnp.where(hit, centers_ref[1:2, f : f + 1], m_row)
    d_row = jnp.sqrt(1.0 - l_row * l_row - m_row * m_row) - 1.0
    plane_row = plane_ref[...].astype(jnp.float32)
    zero_row = jnp.zeros_like(l_row)
    columns = jnp.concatenate([l_row, m_row, d_row, plane_row] + [zero_row] * 4, axis=0).T

    near, capacity, few, slots = peers // 2, sizes[0], sizes[peers // 2], LANES * len(sizes)
    relative = facet ^ lax.axis_index("facet")
    lanes = lax.broadcasted_iota(jnp.int32, (tiles, tiles), 1)
    earlier = (lax.broadcasted_iota(jnp.int32, (tiles, tiles), 0) < lanes).astype(jnp.float32).astype(jnp.bfloat16)
    facets = lax.broadcasted_iota(jnp.int32, (peers, tiles), 0)
    hits = facets == relative
    before = jnp.dot(hits.astype(jnp.float32).astype(jnp.bfloat16), earlier, preferred_element_type=jnp.float32)
    rank = jnp.sum(jnp.where(hits, before, 0.0), axis=0, keepdims=True).astype(jnp.int32)
    passed = jnp.where(facets >= near, jnp.maximum(before - few, 0.0), 0.0)
    passed = jnp.sum(passed, axis=0, keepdims=True).astype(jnp.int32)
    slot = jnp.where((relative < near) | (rank < few), relative * capacity + rank, peers * capacity + passed)

    placing = lax.broadcasted_iota(jnp.int32, (slots, tiles), 0) == slot
    placing = placing.astype(jnp.float32).astype(jnp.bfloat16)
    placing_ref[...] = placing
    cell = cell_ref[...].astype(jnp.float32)
    block_u = jnp.floor(cell * (1.0 / NBLK))
    block_v = cell - block_u * NBLK
    labels = [block_u, block_v, facet.astype(jnp.float32)] + [zero_row] * (SUBLANES - 3)
    labels = jnp.concatenate(labels, axis=0).astype(jnp.bfloat16)
    labels = lax.dot_general(labels, placing, (((1,), (1,)), ((), ())), preferred_element_type=jnp.float32)
    labels = labels.astype(jnp.bfloat16)
    for i, (ref, size) in enumerate(zip(out_refs, sizes)):
        ref[2 * cells // LANES * size :, :] = labels[:, i * LANES : (i + 1) * LANES]

    for h in range(2):
        tile_rows = rows_of[h]
        for copy in copies[4 + 2 * h : 6 + 2 * h]:
            copy.wait()
        part = slice(h * vis_rows, (h + 1) * vis_rows)
        parts_ref[part] = vis_ref[part].astype(jnp.float32)
        l_col, m_col, d_col = (jnp.broadcast_to(columns[tile_rows, i : i + 1], (half, LANES)) for i in range(3))
        for j in range(groups_of_lanes):
            lane = slice(j * LANES, (j + 1) * LANES)
            u, v, w = (uvw_ref[i, tile_rows, lane].astype(jnp.float32) for i in range(3))
            cosine, sine = cos_sin_turns(l_col * u + m_col * v + d_col * w)
            first = 2 * (h * half * groups_of_lanes + j)
            real = parts_ref[pl.ds(first, half, stride=2 * groups_of_lanes), :]
            imag = parts_ref[pl.ds(first + 1, half, stride=2 * groups_of_lanes), :]
            rot_real = (real * cosine + imag * sine).astype(jnp.bfloat16)
            rot_imag = (imag * cosine - real * sine).astype(jnp.bfloat16)
            right = slice(depth + j * LANES, depth + (j + 1) * LANES)
            rows_ref[h, :half, lane] = rot_real
            rows_ref[h, :half, right] = -rot_imag
            rows_ref[h, half:, lane] = rot_imag
            rows_ref[h, half:, right] = rot_real
    totals = [None, None]
    for chosen in (range(planes // 2), range(planes // 2, planes)):
        for p in chosen:
            copies[8 + p].wait()
        for h in range(2):
            plane_two = jnp.concatenate([columns[rows_of[h], 3:4]] * 2, axis=0)
            for p in chosen:
                mask = (plane_two == float(p)).astype(jnp.float32).astype(jnp.bfloat16)
                product = jnp.dot(
                    rows_ref[h] * mask, kern_ref[p].reshape(2 * depth, cells), preferred_element_type=jnp.float32
                )
                totals[h] = product if totals[h] is None else totals[h] + product
    patches = [jnp.concatenate([total[:half], total[half:]], axis=1).astype(jnp.bfloat16) for total in totals]
    patches = jnp.concatenate(patches, axis=0)
    placed = jnp.dot(placing_ref[...], patches, preferred_element_type=jnp.float32).astype(jnp.bfloat16)
    for i, (ref, size) in enumerate(zip(out_refs, sizes)):
        start = i * LANES
        for j in range(2 * cells // LANES):
            ref[j * size : (j + 1) * size, :] = placed[start : start + size, j * LANES : (j + 1) * LANES]


def padded(sizes):
    return -(-sum(sizes) // LANES) * LANES


def load_patches(in_refs, sizes, patch_buf):
    cells = PSIDE * PSIDE
    half_tiles = cells // LANES
    slots = padded(sizes)
    start = 0
    for ref, size in zip(in_refs, sizes):
        rows = slice(start, start + size)
        below = slice(slots + start, slots + start + size)
        for j in range(half_tiles):
            left = slice(j * LANES, (j + 1) * LANES)
            right = slice(cells + j * LANES, cells + (j + 1) * LANES)
            real = ref[j * size : (j + 1) * size, :]
            imag = ref[(half_tiles + j) * size : (half_tiles + j + 1) * size, :]
            patch_buf[rows, left] = real
            patch_buf[rows, right] = imag
            patch_buf[below, left] = -imag
            patch_buf[below, right] = real
        start += size
    if start < slots:
        for first in (0, slots):
            patch_buf[first + start : first + slots, :] = jnp.zeros((slots - start, 2 * cells), jnp.bfloat16)


def cell_phases(in_refs, sizes, direct):
    slots = padded(sizes)
    labels = [jnp.zeros((SUBLANES, LANES), jnp.float32) for _ in range(slots // LANES)]
    lane = lax.broadcasted_iota(jnp.int32, (SUBLANES, LANES), 1)
    start = 0
    for ref, size in zip(in_refs, sizes):
        here = ref[2 * PSIDE * PSIDE // LANES * size :, :].astype(jnp.float32)
        tile, shift = divmod(start, LANES)
        if shift:
            here = pltpu.roll(here, shift, 1)
            if shift + size > LANES:
                labels[tile + 1] = jnp.where(lane < shift, here, 0.0)
            here = jnp.where(lane >= shift, here, 0.0)
        labels[tile] = labels[tile] + here
        start += size
    labels = jnp.concatenate(labels, axis=1)
    lane = lax.broadcasted_iota(jnp.int32, (1, slots), 1)
    mine = labels[2:3] == lax.axis_index("facet").astype(jnp.float32)
    mine = jnp.where(mine | (lane < sum(sizes[:direct])), 1.0, 0.0)
    index = lax.broadcasted_iota(jnp.int32, (NBLK, slots), 0).astype(jnp.float32) * (1.0 / NBLK)
    cos_u, sin_u = cos_sin_turns(index * labels[0:1])
    return (cos_u * mine, sin_u * mine) + cos_sin_turns(index * labels[1:2])


def fill_phases(buf, rows_of, phases):
    cos_u, sin_u, cos_v, sin_v = phases
    slots = cos_v.shape[1]
    for i, j in enumerate(rows_of):
        cu, su = cos_u[j : j + 1], sin_u[j : j + 1]
        rows = slice(i * NBLK, (i + 1) * NBLK)
        buf[rows, :slots] = (cu * cos_v - su * sin_v).astype(jnp.bfloat16)
        buf[rows, slots:] = (cu * sin_v + su * cos_v).astype(jnp.bfloat16)


PER_CHUNK = 8
IMAGE_PARTS = 2


def add_spectrum(in_refs, sizes, direct, out_ref, phases_buf, patch_buf, start_ref=None):
    load_patches(in_refs, sizes, patch_buf)
    phases = cell_phases(in_refs, sizes, direct)
    width = PER_CHUNK * NBLK
    for chunk in range(NBLK // PER_CHUNK):
        here = slice(chunk * width, (chunk + 1) * width)
        buf = phases_buf.at[chunk % 2]
        fill_phases(buf, range(chunk * PER_CHUNK, (chunk + 1) * PER_CHUNK), phases)
        product = jnp.dot(buf[...], patch_buf[...], preferred_element_type=jnp.float32)
        out_ref[here, :] = product if start_ref is None else start_ref[here, :] + product


def middle_kernel(sizes, direct, start_ref, *rest):
    count = len(sizes)
    out_ref, phases_buf, patch_buf = rest[count:]
    add_spectrum(rest[:count], sizes, direct, out_ref, phases_buf, patch_buf, start_ref)


def spectrum_kernel(sizes, direct, *rest):
    count = len(sizes)
    out_ref, turn_ref, phases_buf, patch_buf = rest[count:]
    add_spectrum(rest[:count], sizes, direct, out_ref, phases_buf, patch_buf)

    cells = PSIDE * PSIDE
    lane = lax.broadcasted_iota(jnp.int32, (NBLK, cells), 1)
    row = lax.broadcasted_iota(jnp.int32, (NBLK, cells), 0)
    cos_u, sin_u = cos_sin_turns((row * (lane // PSIDE)).astype(jnp.float32) * (1.0 / GRID))
    cos_v, sin_v = cos_sin_turns((row * (lane % PSIDE)).astype(jnp.float32) * (1.0 / GRID))
    for j in range(NBLK):
        rows = slice(j * NBLK, (j + 1) * NBLK)
        cu, su = cos_u[j : j + 1], sin_u[j : j + 1]
        turn_ref[rows, :cells] = cu * cos_v - su * sin_v
        turn_ref[rows, cells:] = cu * sin_v + su * cos_v


def image_kernel(sizes, direct, groups, chunks, table_ref, early_ref, turn_ref, *rest):
    count = len(sizes)
    in_refs, out_refs = rest[:count], rest[count : count + groups]
    phases_buf, patch_buf, table_buf = rest[count + groups :]
    cells = PSIDE * PSIDE
    share = cells // groups
    load_patches(in_refs, sizes, patch_buf)
    for s in range(groups):
        start = pl.multiple_of((lax.axis_index("freq") ^ s) * share, share)
        table_buf[s * share : (s + 1) * share, :] = table_ref[pl.ds(start, share), :]
    phases = cell_phases(in_refs, sizes, direct)

    width = PER_CHUNK * NBLK
    for i, chunk in enumerate(chunks):
        buf = phases_buf.at[chunk % 2]
        fill_phases(buf, range(chunk * PER_CHUNK, (chunk + 1) * PER_CHUNK), phases)
        here = slice(chunk * width, (chunk + 1) * width)
        spectrum = early_ref[here, :] + jnp.dot(buf[...], patch_buf[...], preferred_element_type=jnp.float32)
        real, imag = spectrum[:, :cells], spectrum[:, cells:]
        cosine, sine = turn_ref[here, :cells], turn_ref[here, cells:]
        turned = jnp.concatenate([real * cosine - imag * sine, real * sine + imag * cosine], axis=1).astype(jnp.bfloat16)
        image = lax.dot_general(
            table_buf[...], turned, (((1,), (1,)), ((), ())), preferred_element_type=jnp.float32
        ).astype(jnp.bfloat16)
        for s in range(groups):
            out_refs[s][:, i * width : (i + 1) * width] = image[s * share : (s + 1) * share]


def finish_kernel(groups, parts, *refs):
    out_ref = refs[-1]
    columns = PSIDE // groups
    per_tile = LANES // NBLK
    lane = lax.broadcasted_iota(jnp.int32, (PSIDE, LANES), 1) // NBLK
    for tile in range(NBLK // per_tile):
        part, place = divmod(tile, NBLK // per_tile // parts)
        in_refs = refs[part * groups : (part + 1) * groups]
        lanes = slice(place * LANES, (place + 1) * LANES)
        total = in_refs[0][:, lanes].astype(jnp.float32)
        for ref in in_refs[1:]:
            total = total + ref[:, lanes].astype(jnp.float32)
        for i in range(per_tile):
            value = jnp.zeros((PSIDE, LANES), jnp.float32)
            for kq in range(columns):
                piece = total[kq * PSIDE : (kq + 1) * PSIDE]
                shift = (kq - i) * NBLK % LANES
                piece = pltpu.roll(piece, shift, 1) if shift else piece
                value = jnp.where(lane == kq, piece, value)
            out_ref[pl.ds(tile * per_tile + i, PSIDE, stride=NBLK), :] = value


def patch_table():
    index = np.arange(PSIDE)
    kq, jq = (a.reshape(-1, 1) for a in np.meshgrid(index, index, indexing="ij"))
    pu, pv = (a.reshape(1, -1) for a in np.meshgrid(index, index, indexing="ij"))
    angle = 2.0 * np.pi * ((pu * jq + pv * kq) % PSIDE) / PSIDE
    return np.concatenate([np.cos(angle), -np.sin(angle)], axis=1) / GRID


def swap(piece, axis, distance):
    count = lax.axis_size(axis)
    return lax.ppermute(piece, axis, [(i, i ^ distance) for i in range(count)])


def overflow_slots(tiles, capacity, few, facets):
    full = min(facets, tiles // capacity)
    most = full * (capacity - few)
    if full < facets:
        most += max(0, tiles - full * capacity - few)
    return -(-most // 16) * 16


def packed_shards(visibilities, uvw, facet_of, plane_of, cell_of, kernels, centers):
    peers, groups = lax.axis_size("facet"), lax.axis_size("freq")
    tiles = visibilities.shape[1]
    capacity = 4 * tiles // peers
    planes, _, depth, cells = kernels.shape
    near = peers // 2
    few = 5 * capacity // 8
    sizes = [capacity] * near + [few] * near + [overflow_slots(tiles, capacity, few, near)]
    payloads = [jax.ShapeDtypeStruct((2 * cells // LANES * size + SUBLANES, LANES), jnp.bfloat16) for size in sizes]
    lanes = depth // LANES
    vis_rows = visibilities[0].reshape(tiles, 2, lanes, LANES).transpose(0, 2, 1, 3).reshape(-1, LANES)
    operands = (
        centers.T,
        facet_of.reshape(1, tiles),
        plane_of,
        cell_of,
        vis_rows,
        uvw[0].transpose(1, 0, 2),
        kernels,
    )
    pieces = pl.pallas_call(
        functools.partial(gather_kernel, peers, sizes),
        out_shape=payloads,
        in_specs=[HBM] * len(operands),
        out_specs=[VMEM] * len(sizes),
        scratch_shapes=[pltpu.VMEM(operand.shape, operand.dtype) for operand in operands]
        + [
            pltpu.VMEM(vis_rows.shape, jnp.float32),
            pltpu.VMEM((2, tiles, 2 * depth), jnp.bfloat16),
            pltpu.VMEM((LANES * len(sizes), tiles), jnp.bfloat16),
            pltpu.SemaphoreType.DMA((len(operands) + 1 + planes,)),
        ],
        compiler_params=compiler_params(40),
        name="gather",
    )(*(pltpu.with_memory_space_constraint(operand, pltpu.HBM) for operand in operands))
    overflow = [swap(pieces[peers], "facet", near)]
    received = [pieces[0]] + [swap(pieces[s], "facet", s) for s in range(1, peers)]
    overflow += [swap(overflow[0], "facet", s) for s in range(1, near)]
    early, early_sizes = received[:near] + overflow[:1], sizes[:near] + sizes[peers:]
    middle, middle_sizes = received[near:-1], sizes[near : peers - 1]
    late, late_sizes = received[-1:] + overflow[1:], sizes[peers - 1 : peers] + sizes[peers:] * (near - 1)
    share = cells // groups
    points = NBLK * NBLK

    def buffers_and_cost(slots):
        buffers = [
            pltpu.VMEM((2, PER_CHUNK * NBLK, 2 * slots), jnp.bfloat16),
            pltpu.VMEM((2 * slots, 2 * cells), jnp.bfloat16),
        ]
        return buffers, pl.CostEstimate(flops=8 * points * slots * cells, bytes_accessed=4 << 20, transcendentals=0)

    buffers, cost = buffers_and_cost(padded(early_sizes))
    spectrum, turns = pl.pallas_call(
        functools.partial(spectrum_kernel, early_sizes, near),
        out_shape=[jax.ShapeDtypeStruct((points, 2 * cells), jnp.float32)] * 2,
        in_specs=[VMEM] * len(early),
        out_specs=[VMEM] * 2,
        scratch_shapes=buffers,
        compiler_params=compiler_params(40),
        cost_estimate=cost,
        name="spectrum",
    )(*early)
    buffers, cost = buffers_and_cost(padded(middle_sizes))
    spectrum = pl.pallas_call(
        functools.partial(middle_kernel, middle_sizes, near - 1),
        out_shape=jax.ShapeDtypeStruct((points, 2 * cells), jnp.float32),
        in_specs=[VMEM] * (1 + len(middle)),
        out_specs=VMEM,
        scratch_shapes=buffers,
        compiler_params=compiler_params(40),
        cost_estimate=cost,
        name="middle",
    )(spectrum, *middle)
    buffers, cost = buffers_and_cost(padded(late_sizes))
    parts = IMAGE_PARTS
    chunks = NBLK // PER_CHUNK // parts
    image = jax.ShapeDtypeStruct((share, points // parts), jnp.bfloat16)
    table = jnp.asarray(patch_table(), jnp.bfloat16)
    summed = []
    for part in range(parts):
        images = pl.pallas_call(
            functools.partial(image_kernel, late_sizes, 1, groups, range(part * chunks, (part + 1) * chunks)),
            out_shape=[image] * groups,
            in_specs=[VMEM] * (3 + len(late)),
            out_specs=[VMEM] * groups,
            scratch_shapes=buffers + [pltpu.VMEM((cells, 2 * cells), jnp.bfloat16)],
            compiler_params=compiler_params(40),
            cost_estimate=cost,
        )(table, spectrum, turns, *late)
        summed += [images[0]] + [swap(images[s], "freq", s) for s in range(1, groups)]
    facet_image = pl.pallas_call(
        functools.partial(finish_kernel, groups, parts),
        out_shape=jax.ShapeDtypeStruct((GRID, GRID // groups), jnp.float32),
        in_specs=[VMEM] * len(summed),
        out_specs=VMEM,
        compiler_params=compiler_params(16),
        name="finish",
    )(*summed)
    return facet_image[None]


def solution(mesh):
    in_specs = (
        P("freq", "facet", None, None),
        P("freq", "facet", None, None),
        P("freq", "facet", None),
        P("freq", "facet"),
        P("freq", "facet"),
        P(),
        P(),
    )
    out_specs = P("facet", None, "freq")

    def body(*args):
        peers, groups = lax.axis_size("facet"), lax.axis_size("freq")
        capacity = 4 * args[0].shape[1] // peers
        powers = peers & (peers - 1) == 0 and groups & (groups - 1) == 0
        packed = capacity == LANES and powers and GRID // groups == LANES
        return (packed_shards if packed else shards)(*args)

    return jax.shard_map(body, mesh=mesh, in_specs=in_specs, out_specs=out_specs, check_vma=False)
```
